256 devices in a mesh: dp: 128 (over z, x, y), mp: 2 (over core).
Axes of the slice: x: 4, y: 4, z: 8, core: 2. Of those that a mesh axis runs over, the one named last changes fastest.
Arguments:
- embeddings: float32 [98304, 1024], P('dp', 'mp')
- cluster_id: int32 [98304], P('dp'), may hold values from 0 to 32767, as said below
- centroids: float32 [32768, 1024], P('dp', 'mp'), may hold values from -6 to 6
- cluster_mass: float32 [32768], P('dp'), may hold values from 1 to 16
Outputs:
- max_similarity: float32 [98304], P('dp')
- new_centroids: float32 [32768, 1024], P('dp', 'mp')
The draws below stay inside these ranges and needn't reach their ends.
Inputs may be any that keep to these rules, and one draw needn't show every extreme that they name: `cluster_id`: cluster k belongs to owner k // 256. Among the 768 rows of one index of dp, at most 12 have clusters of any one owner, and for some owner exactly 12.
All inputs are finite; a program needn't handle non-finite values.
Results may differ from the reference program's by a relative error of at most 0.0011.
Values may be sent and summed in bfloat16 or wider, within the bound.
A program may use at most 64 MiB of HBM per device.

```python
import math
import jax
import jax.numpy as jnp
from jax import lax

D = 1024
CL_DEV = 256
ROW_DEV = 768
CLUSTERS = 32768
ROWS = 98304
CAP = 12


def cluster_helper(key):
    owners = ROWS // ROW_DEV
    base = jax.random.fold_in(key, 3)

    def one_block(block_key):
        first, second, third, fourth = jax.random.split(block_key, 4)
        full_owner = jax.random.randint(first, (), 0, owners)
        others = (full_owner + 1 + jnp.arange((owners - 1) * CAP) // CAP) % owners
        order = jax.random.permutation(second, (owners - 1) * CAP)
        picks = others[order[:ROW_DEV - CAP]]
        chosen = jnp.concatenate([jnp.full((CAP,), full_owner), picks])
        chosen = chosen[jax.random.permutation(third, ROW_DEV)]
        local = jax.random.randint(fourth, (ROW_DEV,), 0, CL_DEV)
        return (chosen * CL_DEV + local).astype(jnp.int32)
    keys = jax.random.split(base, owners)
    return jax.vmap(one_block)(keys).reshape(ROWS)


def draw_cluster_id(key, part):
    return cluster_helper(key)


def draw_embeddings(key, part):
    ids = cluster_helper(key)
    centre_key = jax.random.fold_in(key, 7)
    centres = jax.vmap(lambda ident: jax.random.normal(jax.random.fold_in(centre_key, ident), (D,), jnp.float32))(ids)
    noise_key = jax.random.fold_in(key, 11)
    noise = jax.random.normal(noise_key, (ROWS, D), jnp.float32)
    values = 0.8 * centres + 0.6 * noise
    return values.astype(jnp.float32)


def level_of(rng, dims, pieces, smallest, top_value):
    level, own = 1.0, jax.random.fold_in(rng, 6)
    for dim, blocks in pieces:
        heights = jnp.exp(jax.random.uniform(jax.random.fold_in(own, dim), (blocks,), jnp.float32, smallest / len(pieces), top_value / len(pieces)))
        level = level * jnp.repeat(heights, dims[dim] // blocks).reshape([-1 if axis == dim else 1 for axis in range(len(dims))])
    return level


def scatter_about(stream_key, dims, scale, bound, shards=(), kind=jnp.bfloat16):
    gain = level_of(stream_key, dims, shards, -0.22, 0.18) if shards else 1.0
    values = jax.random.normal(stream_key, dims, jnp.float32) * scale * gain
    return jnp.minimum(jnp.maximum(values, -bound), bound).astype(kind)


def setup_inputs(seed: int = 0) -> dict:
    key_of = jax.random.split(jax.random.key(seed), 5)
    embeddings = draw_embeddings(jax.random.fold_in(key_of[4], 71), 0)
    cluster_id = draw_cluster_id(jax.random.fold_in(key_of[4], 71), 0)
    centroids = scatter_about(key_of[2], (CLUSTERS, D), 1.0, 6.0, ((0, 128), (1, 2)), jnp.float32)
    cluster_mass = jnp.clip(jnp.exp(math.log(16.0) - 2.7725887 * jax.random.uniform(key_of[3], (CLUSTERS,), jnp.float32) ** level_of(key_of[3], (CLUSTERS,), ((0, 128),), -0.2, 0.2)), 1.0, 16.0)
    return dict(embeddings=embeddings, cluster_id=cluster_id, centroids=centroids, cluster_mass=cluster_mass)


def reference(embeddings, cluster_id, centroids, cluster_mass):
    owners = ROWS // ROW_DEV
    slots = 2 * ROW_DEV
    cap = slots // owners
    squares = lax.optimization_barrier(jnp.sum(embeddings * embeddings, axis=1))
    unit = (embeddings * lax.rsqrt(squares / D + 1e-06)[:, None]).astype(jnp.bfloat16)
    owner = (cluster_id // CL_DEV).astype(jnp.int32)
    local = (cluster_id - owner * CL_DEV).astype(jnp.int32)
    sums = jnp.zeros((CLUSTERS, D), jnp.float32).at[cluster_id].add(unit.astype(jnp.float32))
    counts = jnp.zeros((CLUSTERS,), jnp.float32).at[cluster_id].add(jnp.ones((ROWS,), jnp.float32))
    new_centroids = (cluster_mass[:, None] * centroids + sums) / (cluster_mass + counts)[:, None]
    blocked = owner.reshape(owners, ROW_DEV)
    hot = (blocked[:, :, None] == jnp.arange(owners, dtype=jnp.int32)[None, None, :]).astype(jnp.int32)
    running = jnp.cumsum(hot, axis=1)
    rank = jnp.take_along_axis(running, blocked[:, :, None], axis=2)[:, :, 0] - 1
    source = (jnp.arange(ROWS, dtype=jnp.int32) // ROW_DEV).astype(jnp.int32)
    position = (source * cap + rank.reshape(ROWS)).astype(jnp.int32)
    buffer = jnp.zeros((owners, slots, D), jnp.bfloat16).at[owner, position].set(unit)
    bids = jnp.full((owners, slots), -1, jnp.int32).at[owner, position].set(local)

    def one_owner(pair):
        rows, ids = pair
        wide = rows.astype(jnp.float32)
        scores = jnp.dot(wide, wide.T, precision=lax.Precision.HIGHEST) / D
        index = jnp.arange(slots, dtype=jnp.int32)
        same = (ids[:, None] == ids[None, :]) & (ids[:, None] >= 0) & (index[:, None] != index[None, :])
        return lax.optimization_barrier(jnp.max(jnp.where(same, scores, -1.0), axis=1))
    best = lax.map(one_owner, (buffer, bids))
    max_similarity = best[owner, position]
    return (max_similarity, new_centroids)
```

```python
import functools

import jax
import jax.numpy as jnp
from jax import lax
from jax.experimental import pallas as pl
from jax.experimental.pallas import tpu as pltpu
from jax.sharding import PartitionSpec as P

D = 1024
HALF = 512
ROWS = 768
CLUSTERS = 256
CAP = 12
ROOM = 128
NZ = 8
NXY = 16
GROUPS = (
    ((0, 1, 7), 16, 40),
    ((2, 6), 64, 24),
    ((3, 5), 96, 24),
    ((4,), 0, 16),
)
LANE = {k: base + CAP * m for members, base, _ in GROUPS for m, k in enumerate(members)}
KEYS = 128
MESH = pl.DeviceIdType.MESH
NT = (((1,), (1,)), ((), ()))
NEAR = (1, 7, 2, 6, 3, 5, 4)


def neg(d):
    return ((4 - d // 4) % 4) * 4 + (4 - d % 4) % 4


def hot(mask):
    return jnp.where(mask, 1.0, 0.0).astype(jnp.bfloat16)


def exchange_kernel(
    emb_ref, cid_ref, cent_ref, mass_ref,
    best_ref, nc_ref, flag_ref,
    emb, unit, sq_mine, sq_peer, zout, zin, mout, min_, xo0, xo1, xo2, xo3, idout,
    rows, rows_p, idin, idcol, tiles_i, best_out, ret1, ret2, cent, out_v,
    local_sem, sq_sem, zs, zr, ms, mr, xs, xr, ids_s, ids_r, ps, pr, bs, br, es, fs, fr,
):
    xout = (xo0, xo1, xo2, xo3)
    me = lax.axis_index("dp")
    c = lax.axis_index("mp")
    z, x, y = me // 16, (me // 4) % 4, me % 4

    def at_z(k):
        return (((z + k) % NZ) * 16 + x * 4 + y, c)

    def at_xy(d):
        return (z * 16 + ((x + d // 4) % 4) * 4 + (y + d % 4) % 4, c)

    partner = (me, 1 - c)

    load = pltpu.make_async_copy(emb_ref, emb, local_sem.at[0])
    load.start()
    cent_load = pltpu.make_async_copy(cent_ref, cent, local_sem.at[1])
    cent_load.start()
    blank = jnp.zeros((NXY, 16, HALF), jnp.bfloat16)
    rows[:, 48:64, :] = blank
    rows[:, 80:96, :] = blank
    rows[:, 112:128, :] = blank

    barrier = pltpu.get_barrier_semaphore()
    for k in range(1, NZ):
        pl.semaphore_signal(barrier, inc=1, device_id=at_z(k), device_id_type=MESH)
    for d in range(1, NXY):
        pl.semaphore_signal(barrier, inc=1, device_id=at_xy(d), device_id_type=MESH)
    pl.semaphore_signal(barrier, inc=1, device_id=partner, device_id_type=MESH)

    cid = cid_ref[...]
    owner = cid >> 8
    dz = ((owner >> 4) - z) & 7
    dxy = ((((owner >> 2) & 3) - x) & 3) * 4 + (((owner & 3) - y) & 3)
    target = dz * 16 + dxy
    lane128 = lax.broadcasted_iota(jnp.int32, (128, 128), 1)
    sub128 = lax.broadcasted_iota(jnp.int32, (128, 128), 0)
    upto = hot(sub128 <= lane128)
    sub8 = lax.broadcasted_iota(jnp.int32, (8, 128), 0)
    base_t = jnp.zeros((128, 128), jnp.float32)
    base_z = jnp.zeros((8, 128), jnp.float32)
    ranks, places = [], []
    for b in range(ROWS // 128):
        cut = slice(128 * b, 128 * b + 128)
        is_t = sub128 == target[:, cut]
        is_z = sub8 == dz[:, cut]
        run_t = base_t + jnp.dot(hot(is_t), upto, preferred_element_type=jnp.float32)
        run_z = base_z + jnp.dot(hot(is_z), upto, preferred_element_type=jnp.float32)
        ranks.append(jnp.sum(jnp.where(is_t, run_t, 0.0), axis=0, keepdims=True) - 1.0)
        places.append(jnp.sum(jnp.where(is_z, run_z, 0.0), axis=0, keepdims=True) - 1.0)
        base_t = jnp.broadcast_to(run_t[:, 127:128], (128, 128))
        base_z = jnp.broadcast_to(run_z[:, 127:128], (8, 128))
    most = jnp.max(base_z, axis=0, keepdims=True)
    over = jnp.where(most > float(ROOM), 1.0, 0.0)
    rank = jnp.concatenate(ranks, axis=1)
    place = jnp.concatenate(places, axis=1).astype(jnp.int32)
    slot = jnp.where(place < ROOM, dz * ROOM + place, -1)
    tile_of = dz * 16 + ((4 - (dxy >> 2)) & 3) * 4 + ((4 - (dxy & 3)) & 3)
    lane_of = rank.astype(jnp.int32)
    for k in range(NZ):
        lane_of = jnp.where(dz == k, lane_of + LANE[(NZ - k) % NZ], lane_of)
    tiles_i[...] = jnp.zeros_like(tiles_i)
    for b in range(ROWS // 128):
        cut = slice(128 * b, 128 * b + 128)
        tiles_i[0, b:b + 1, :] = tile_of[:, cut]
        tiles_i[1, b:b + 1, :] = lane_of[:, cut]
    row8 = lax.broadcasted_iota(jnp.int32, (8, ROWS), 0)
    values = jnp.where(
        row8 == 0, ((cid & 255) + 1).astype(jnp.float32),
        jnp.where(row8 == 1, dxy.astype(jnp.float32), jnp.where(row8 == 2, rank, 0.0)),
    ).astype(jnp.bfloat16)

    load.wait()
    squares = jnp.zeros((ROWS, 128), jnp.float32)
    for f in range(HALF // 128):
        part = emb[:, 128 * f:128 * f + 128]
        squares = squares + part * part
    mine = jnp.sum(squares.T, axis=0, keepdims=True)
    sq_mine[...] = mine
    pl.semaphore_wait(barrier, NZ - 1 + NXY - 1 + 1)
    sq_copy = pltpu.make_async_remote_copy(
        sq_mine, sq_peer, sq_sem.at[0], sq_sem.at[1], device_id=partner, device_id_type=MESH)
    sq_copy.start()

    place_hot = []
    for k in range(NZ):
        want = lax.broadcasted_iota(jnp.int32, (ROOM, ROWS), 0) + k * ROOM
        place_hot.append(hot(want == slot))
    meta_copies = []
    for k in (0,) + NEAR:
        meta = lax.dot_general(values, place_hot[k], NT, preferred_element_type=jnp.float32)
        meta = jnp.where(sub8 == 3, over, meta)
        if k == 0:
            min_[0] = meta
        else:
            mout[k] = meta
            copy = pltpu.make_async_remote_copy(
                mout.at[k], min_.at[NZ - k], ms.at[k], mr.at[NZ - k], device_id=at_z(k), device_id_type=MESH)
            copy.start()
            meta_copies.append((NZ - k, copy))

    sq_copy.wait()
    scale = lax.rsqrt((sq_mine[...] + sq_peer[...]) / D + 1e-06)
    scale = jnp.broadcast_to(scale, (128, ROWS)).T
    for f in range(HALF // 128):
        unit[:, 128 * f:128 * f + 128] = (emb[:, 128 * f:128 * f + 128] * scale).astype(jnp.bfloat16)

    z_copies = {}
    for k in NEAR + (0,):
        packed = jnp.dot(place_hot[k], unit[...], preferred_element_type=jnp.float32).astype(jnp.bfloat16)
        if k == 0:
            zin[0] = packed
        else:
            zout[k] = packed
            copy = pltpu.make_async_remote_copy(
                zout.at[k], zin.at[NZ - k], zs.at[k], zr.at[NZ - k], device_id=at_z(k), device_id_type=MESH)
            copy.start()
            z_copies[NZ - k] = copy
    meta_by = dict(meta_copies)

    def wait_meta(k):
        if k:
            meta_by[k].wait_recv()

    x_copies = {}

    def forward(g):
        members, base, count = GROUPS[g]
        total = None
        for m, k in enumerate(members):
            meta = min_[k]
            valid = meta[0:1, :] > 0.5
            there = jnp.where(valid, meta[1:2, :] * float(count) + meta[2:3, :] + float(CAP * m), -1.0)
            there = there.astype(jnp.int32)
            want = lax.broadcasted_iota(jnp.int32, (NXY * count, ROOM), 0)
            if k:
                z_copies[k].wait_recv()
            part = jnp.dot(hot(want == there), zin[k], preferred_element_type=jnp.float32)
            total = part if total is None else total + part
        for d in range(NXY):
            block = total[count * d:count * d + count, :].astype(jnp.bfloat16)
            if d == 0:
                rows[0, base:base + count, :] = block
            else:
                xout[g][d] = block
                copy = pltpu.make_async_remote_copy(
                    xout[g].at[d], rows.at[neg(d), pl.ds(base, count)], xs.at[g, d], xr.at[g, neg(d)],
                    device_id=at_xy(d), device_id_type=MESH)
                copy.start()
                x_copies[g, neg(d)] = copy

    p_copies = {}

    def share(g):
        _, base, count = GROUPS[g]
        for j in range(NXY):
            if j:
                x_copies[g, j].wait_recv()
            copy = pltpu.make_async_remote_copy(
                rows.at[j, pl.ds(base, count)], rows_p.at[j, pl.ds(base, count)], ps.at[g, j], pr.at[g, j],
                device_id=partner, device_id_type=MESH)
            copy.start()
            p_copies[g, j] = copy

    for k in GROUPS[0][0]:
        wait_meta(k)
    forward(0)

    for k in range(NZ):
        if k not in GROUPS[0][0]:
            wait_meta(k)
    ids = jnp.zeros((NXY, 128), jnp.float32)
    flag = jnp.zeros((1, 128), jnp.float32)
    sub16 = lax.broadcasted_iota(jnp.int32, (NXY, 128), 0)
    for k in range(NZ):
        meta = min_[k]
        valid = meta[0:1, :] > 0.5
        to = jnp.where(valid, meta[1:2, :], -1.0).astype(jnp.int32)
        place_k = meta[2:3, :].astype(jnp.int32) + LANE[k]
        left = jnp.where(sub16 == to, meta[0:1, :], 0.0).astype(jnp.bfloat16)
        ids = ids + lax.dot_general(left, hot(sub128 == place_k), NT, preferred_element_type=jnp.float32)
        flag = jnp.maximum(flag, meta[3:4, :])
    ids = jnp.where(lax.broadcasted_iota(jnp.int32, (NXY, 128), 1) == 127, flag, ids)
    id_copies = {}
    for d in range(NXY):
        if d == 0:
            idin[0] = ids[0:1, :]
        else:
            idout[d] = ids[d:d + 1, :]
            copy = pltpu.make_async_remote_copy(
                idout.at[d], idin.at[neg(d)], ids_s.at[d], ids_r.at[neg(d)], device_id=at_xy(d), device_id_type=MESH)
            copy.start()
            id_copies[neg(d)] = copy

    forward(1)
    share(0)
    for j in range(1, NXY):
        id_copies[j].wait_recv()
    flag = jnp.zeros((1, 128), jnp.float32)
    last = lax.broadcasted_iota(jnp.int32, (1, 128), 1) == 127
    for j in range(NXY):
        line = idin[j]
        flag = jnp.maximum(flag, jnp.where(last, line, 0.0))
        line = jnp.where(last | (line < 0.5), -1.0, line)
        idcol[j] = jnp.broadcast_to(line, (128, 128)).T
    flag_ref[...] = flag
    forward(2)
    share(1)
    forward(3)
    share(2)
    share(3)

    for g in range(4):
        for j in range(NXY):
            p_copies[g, j].wait_recv()

    for q in range(4):
        first = 8 * c + 2 * q
        query = rows[pl.ds(first, 2)].reshape(256, HALF)
        query_p = rows_p[pl.ds(first, 2)].reshape(256, HALF)
        id_q = [idin[first], idin[first + 1]]
        top = [jnp.full((8, 128), -float(D), jnp.float32) for _ in range(2)]

        def keys_step(t, top, first=first, q=q, query=query, query_p=query_p, id_q=id_q):
            j = (8 * c + t) % NXY
            scores = lax.dot_general(rows[j], query, NT, preferred_element_type=jnp.float32)
            scores = scores + lax.dot_general(rows_p[j], query_p, NT, preferred_element_type=jnp.float32)
            id_k = idcol[j]
            out = []
            for h in range(2):
                same = (id_k == id_q[h]) & ((sub128 != lane128) | (t != 2 * q + h))
                kept = jnp.where(same, scores[:, 128 * h:128 * h + 128], -float(D))
                out.append(jnp.maximum(top[h], jnp.max(kept.reshape(16, 8, 128), axis=0)))
            return tuple(out)

        top = lax.fori_loop(0, NXY, keys_step, tuple(top))
        for h in range(2):
            best_out[2 * q + h] = jnp.max(top[h], axis=0, keepdims=True) * (1.0 / D)

    def best_copy(i):
        jx, jy = 2 * c + i // 4, i % 4
        there = (z * 16 + ((x + jx) % 4) * 4 + (y + jy) % 4, c)
        return pltpu.make_async_remote_copy(
            best_out.at[i], ret1.at[8 * c + i], bs.at[i], br.at[i], device_id=there, device_id_type=MESH)

    @pl.when(c == 0)
    def _():
        ret1[0] = best_out[0]

    @pl.when(c == 1)
    def _():
        best_copy(0).start()

    for i in range(1, 8):
        best_copy(i).start()

    sub256 = lax.broadcasted_iota(jnp.int32, (CLUSTERS, 128), 0).astype(jnp.float32) + 1.0
    counts = jnp.zeros((CLUSTERS, 128), jnp.float32)
    sums = jnp.zeros((CLUSTERS, HALF), jnp.float32)
    for j in range(NXY):
        line = jnp.where(last, 0.0, idin[j])
        member = jnp.where(sub256 == line, 1.0, 0.0)
        counts = counts + member
        sums = sums + jnp.dot(member.astype(jnp.bfloat16), rows[j], preferred_element_type=jnp.float32)
    cent_load.wait()
    total = jnp.sum(counts, axis=1, keepdims=True)
    mass = jnp.broadcast_to(mass_ref[...], (128, CLUSTERS)).T[:, 0:1]
    cent[...] = (mass * cent[...] + sums) / (mass + total)
    nc_copy = pltpu.make_async_copy(cent, nc_ref, local_sem.at[2])
    nc_copy.start()

    @pl.when(c == 1)
    def _():
        best_copy(0).wait()

    for i in range(1, 8):
        best_copy(i).wait()
    half = pltpu.make_async_remote_copy(
        ret1.at[pl.ds(8 * c, 8)], ret1.at[pl.ds(8 * c, 8)], es.at[0], es.at[1], device_id=partner, device_id_type=MESH)
    half.start()
    half.wait()
    back = []
    for k in NEAR[::-1]:
        copy = pltpu.make_async_remote_copy(
            ret1, ret2.at[NZ - k], fs.at[k], fr.at[NZ - k], device_id=at_z(k), device_id_type=MESH)
        copy.start()
        back.append((NZ - k, copy))
    tile_t = tiles_i[0]
    lane_t = tiles_i[1]
    result = jnp.zeros((8, 128), jnp.float32)

    def pick(k, result):
        for j in range(NXY):
            line = ret1[j] if k == 0 else ret2[k, j]
            got = jnp.take_along_axis(
                jnp.broadcast_to(line, (8, 128)), lane_t, axis=1, mode="promise_in_bounds")
            result = jnp.where(tile_t == k * 16 + j, got, result)
        return result

    result = pick(0, result)
    for k, copy in back[::-1]:
        copy.wait_recv()
        result = pick(k, result)
    for b in range(ROWS // 128):
        best_ref[:, 128 * b:128 * b + 128] = result[b:b + 1, :]

    for _, copy in back:
        copy.wait_send()
    for _, copy in meta_copies:
        copy.wait_send()
    for copy in z_copies.values():
        copy.wait_send()
    for copy in x_copies.values():
        copy.wait_send()
    for copy in id_copies.values():
        copy.wait_send()
    for copy in p_copies.values():
        copy.wait_send()
    nc_copy.wait()


def compact(embeddings, cluster_id, centroids, cluster_mass):
    vmem = pl.BlockSpec(memory_space=pltpu.VMEM)
    anywhere = pl.BlockSpec(memory_space=pl.ANY)
    f32, bf16, i32 = jnp.float32, jnp.bfloat16, jnp.int32
    dma = pltpu.SemaphoreType.DMA
    return pl.pallas_call(
        exchange_kernel,
        out_shape=(
            jax.ShapeDtypeStruct((1, ROWS), f32),
            jax.ShapeDtypeStruct((CLUSTERS, HALF), f32),
            jax.ShapeDtypeStruct((1, 128), f32),
        ),
        in_specs=[anywhere, vmem, anywhere, vmem],
        out_specs=(vmem, anywhere, vmem),
        scratch_shapes=[
            pltpu.VMEM((ROWS, HALF), f32),
            pltpu.VMEM((ROWS, HALF), bf16),
            pltpu.VMEM((1, ROWS), f32),
            pltpu.VMEM((1, ROWS), f32),
            pltpu.VMEM((NZ, ROOM, HALF), bf16),
            pltpu.VMEM((NZ, ROOM, HALF), bf16),
            pltpu.VMEM((NZ, 8, 128), f32),
            pltpu.VMEM((NZ, 8, 128), f32),
            *[pltpu.VMEM((NXY, count, HALF), bf16) for _, _, count in GROUPS],
            pltpu.VMEM((NXY, 1, 128), f32),
            pltpu.VMEM((NXY, KEYS, HALF), bf16),
            pltpu.VMEM((NXY, KEYS, HALF), bf16),
            pltpu.VMEM((NXY, 1, 128), f32),
            pltpu.VMEM((NXY, 128, 128), f32),
            pltpu.VMEM((2, 8, 128), i32),
            pltpu.VMEM((8, 1, 128), f32),
            pltpu.VMEM((NXY, 1, 128), f32),
            pltpu.VMEM((NZ, NXY, 1, 128), f32),
            pltpu.VMEM((CLUSTERS, HALF), f32),
            pltpu.VMEM((8, 128), f32),
            dma((3,)), dma((2,)), dma((NZ,)), dma((NZ,)), dma((NZ,)), dma((NZ,)),
            dma((4, NXY)), dma((4, NXY)), dma((NXY,)), dma((NXY,)), dma((4, NXY)), dma((4, NXY)),
            dma((8,)), dma((8,)), dma((2,)), dma((NZ,)), dma((NZ,)),
        ],
        compiler_params=pltpu.CompilerParams(
            collective_id=0, has_side_effects=True, vmem_limit_bytes=48 * 2**20),
    )(embeddings, cluster_id.reshape(1, ROWS), centroids, cluster_mass.reshape(1, CLUSTERS))


def from_partner(value):
    return lax.ppermute(value, "mp", [(0, 1), (1, 0)])


def general(embeddings, cluster_id, centroids, cluster_mass):
    owners = lax.axis_size("dp")
    row_count = embeddings.shape[0]
    slot_count = 2 * row_count
    capacity = slot_count // owners
    cluster_count = centroids.shape[0]
    core = lax.axis_index("mp")
    squares = jnp.sum(embeddings * embeddings, axis=1)
    squares = squares + from_partner(squares)
    unit = (embeddings * lax.rsqrt(squares / D + 1e-06)[:, None]).astype(jnp.bfloat16)
    owner = cluster_id // cluster_count
    local = cluster_id - owner * cluster_count
    owner_hot = (owner[:, None] == jnp.arange(owners, dtype=jnp.int32)[None, :]).astype(jnp.bfloat16)
    row_index = jnp.arange(row_count, dtype=jnp.int32)
    lower = (row_index[:, None] >= row_index[None, :]).astype(jnp.bfloat16)
    running = jnp.dot(lower, owner_hot, preferred_element_type=jnp.float32)
    rank = jnp.sum(running * owner_hot.astype(jnp.float32), axis=1).astype(jnp.int32) - 1
    slot = owner * capacity + rank
    slot_index = jnp.arange(slot_count, dtype=jnp.int32)
    placed = slot_index[:, None] == slot[None, :]
    outgoing = jnp.dot(
        placed.astype(jnp.bfloat16), unit, preferred_element_type=jnp.float32
    ).astype(jnp.bfloat16)
    out_ids = jnp.max(jnp.where(placed, local[None, :] + 1, 0), axis=1) - 1
    incoming = lax.all_to_all(outgoing, "dp", split_axis=0, concat_axis=0, tiled=True)
    in_ids = lax.all_to_all(out_ids, "dp", split_axis=0, concat_axis=0, tiled=True)
    member = (jnp.arange(cluster_count, dtype=jnp.int32)[:, None] == in_ids[None, :]).astype(jnp.bfloat16)
    sums = jnp.dot(member, incoming, preferred_element_type=jnp.float32)
    counts = jnp.sum(member.astype(jnp.float32), axis=1)
    new_centroids = (cluster_mass[:, None] * centroids + sums) / (cluster_mass + counts)[:, None]
    half = slot_count // 2
    start = core * half
    contract = (((1,), (1,)), ((), ()))
    other = from_partner(incoming)
    scores = lax.dot_general(
        lax.dynamic_slice_in_dim(incoming, start, half, 0), incoming, contract, preferred_element_type=jnp.float32)
    scores = scores + lax.dot_general(
        lax.dynamic_slice_in_dim(other, start, half, 0), other, contract, preferred_element_type=jnp.float32)
    scores = scores / D
    query_ids = lax.dynamic_slice_in_dim(in_ids, start, half, 0)
    query_pos = start + jnp.arange(half, dtype=jnp.int32)
    same = (
        (query_ids[:, None] == in_ids[None, :])
        & (query_ids[:, None] >= 0)
        & (query_pos[:, None] != slot_index[None, :])
    )
    best = jnp.max(jnp.where(same, scores, -1.0), axis=1)
    best_p = from_partner(best)
    low, high = jnp.where(core == 0, best, best_p), jnp.where(core == 0, best_p, best)
    returned = lax.all_to_all(
        jnp.concatenate([low, high]), "dp", split_axis=0, concat_axis=0, tiled=True)
    return jnp.take(returned, slot), new_centroids


def shards(embeddings, cluster_id, centroids, cluster_mass):
    best, new_centroids, flag = compact(embeddings, cluster_id, centroids, cluster_mass)
    return lax.cond(
        flag[0, 127] > 0.5,
        lambda *args: general(*args),
        lambda *args: (best.reshape(ROWS), new_centroids),
        embeddings, cluster_id, centroids, cluster_mass,
    )


def solution(mesh):
    in_specs = (P("dp", "mp"), P("dp"), P("dp", "mp"), P("dp"))
    out_specs = (P("dp"), P("dp", "mp"))
    return jax.shard_map(shards, mesh=mesh, in_specs=in_specs, out_specs=out_specs, check_vma=False)
```

```python
import functools

import jax
import jax.numpy as jnp
from jax import lax
from jax.experimental import pallas as pl
from jax.experimental.pallas import tpu as pltpu
from jax.sharding import PartitionSpec as P

D = 1024
HALF = 512
ROWS = 768
CLUSTERS = 256
CAP = 12
ROOM = 128
NZ = 8
NXY = 16
GROUPS = (
    ((0, 1, 7), 16, 40),
    ((2, 6), 56, 24),
    ((3, 5), 80, 24),
    ((4,), 0, 16),
)
LANE = {k: base + CAP * m for members, base, _ in GROUPS for m, k in enumerate(members)}
MESH = pl.DeviceIdType.MESH
NT = (((1,), (1,)), ((), ()))
NEAR = (1, 7, 2, 6, 3, 5, 4)


def neg(d):
    return ((4 - d // 4) % 4) * 4 + (4 - d % 4) % 4


def hot(mask):
    return jnp.where(mask, 1.0, 0.0).astype(jnp.bfloat16)


def exchange_kernel(
    emb_ref, cid_ref, cent_ref, mass_ref,
    best_ref, nc_ref, flag_ref,
    emb, unit, sq_mine, sq_peer, zout, zin, mout, min_, xo0, xo1, xo2, xo3, idout,
    r0, r1, r2, r3, p0, p1, p2, p3, idin, ik0, ik1, ik2, ik3, top0, top1, top2, top3, idq, sums,
    tiles_i, column, best_out, ret1, ret2, cent,
    local_sem, sq_sem, zs, zr, ms, mr, xs, xr, ids_s, ids_r, ps, pr, bs, br, es, fs, fr,
):
    xout = (xo0, xo1, xo2, xo3)
    rows, rows_p, idkey, top = (r0, r1, r2, r3), (p0, p1, p2, p3), (ik0, ik1, ik2, ik3), (top0, top1, top2, top3)
    me = lax.axis_index("dp")
    c = lax.axis_index("mp")
    z, x, y = me // 16, (me // 4) % 4, me % 4

    def at_z(k):
        return (((z + k) % NZ) * 16 + x * 4 + y, c)

    def at_xy(d):
        return (z * 16 + ((x + d // 4) % 4) * 4 + (y + d % 4) % 4, c)

    partner = (me, 1 - c)

    load = pltpu.make_async_copy(emb_ref, emb, local_sem.at[0])
    load.start()
    cent_load = pltpu.make_async_copy(cent_ref, cent, local_sem.at[1])
    cent_load.start()

    barrier = pltpu.get_barrier_semaphore()
    for k in range(1, NZ):
        pl.semaphore_signal(barrier, inc=1, device_id=at_z(k), device_id_type=MESH)
    for d in range(1, NXY):
        pl.semaphore_signal(barrier, inc=1, device_id=at_xy(d), device_id_type=MESH)
    pl.semaphore_signal(barrier, inc=1, device_id=partner, device_id_type=MESH)

    cid = cid_ref[...]
    owner = cid >> 8
    dz = ((owner >> 4) - z) & 7
    dxy = ((((owner >> 2) & 3) - x) & 3) * 4 + (((owner & 3) - y) & 3)
    target = dz * 16 + dxy
    lane128 = lax.broadcasted_iota(jnp.int32, (128, 128), 1)
    sub128 = lax.broadcasted_iota(jnp.int32, (128, 128), 0)
    upto = hot(sub128 <= lane128)
    sub8 = lax.broadcasted_iota(jnp.int32, (8, 128), 0)
    base_t = jnp.zeros((128, 128), jnp.float32)
    base_z = jnp.zeros((8, 128), jnp.float32)
    ranks, places = [], []
    for b in range(ROWS // 128):
        cut = slice(128 * b, 128 * b + 128)
        is_t = sub128 == target[:, cut]
        is_z = sub8 == dz[:, cut]
        run_t = base_t + jnp.dot(hot(is_t), upto, preferred_element_type=jnp.float32)
        run_z = base_z + jnp.dot(hot(is_z), upto, preferred_element_type=jnp.float32)
        ranks.append(jnp.sum(jnp.where(is_t, run_t, 0.0), axis=0, keepdims=True) - 1.0)
        places.append(jnp.sum(jnp.where(is_z, run_z, 0.0), axis=0, keepdims=True) - 1.0)
        base_t = jnp.broadcast_to(run_t[:, 127:128], (128, 128))
        base_z = jnp.broadcast_to(run_z[:, 127:128], (8, 128))
    most = jnp.max(base_z, axis=0, keepdims=True)
    over = jnp.where(most > float(ROOM), 1.0, 0.0)
    rank = jnp.concatenate(ranks, axis=1)
    place = jnp.concatenate(places, axis=1).astype(jnp.int32)
    slot = jnp.where(place < ROOM, dz * ROOM + place, -1)
    tile_of = dz * 16 + ((4 - (dxy >> 2)) & 3) * 4 + ((4 - (dxy & 3)) & 3)
    lane_of = rank.astype(jnp.int32)
    for k in range(NZ):
        lane_of = jnp.where(dz == k, lane_of + LANE[(NZ - k) % NZ], lane_of)
    tiles_i[...] = jnp.zeros_like(tiles_i)
    for b in range(ROWS // 128):
        cut = slice(128 * b, 128 * b + 128)
        tiles_i[0, b:b + 1, :] = tile_of[:, cut]
        tiles_i[1, b:b + 1, :] = lane_of[:, cut]
    row8 = lax.broadcasted_iota(jnp.int32, (8, ROWS), 0)
    values = jnp.where(
        row8 == 0, ((cid & 255) + 1).astype(jnp.float32),
        jnp.where(row8 == 1, dxy.astype(jnp.float32), jnp.where(row8 == 2, rank, 0.0)),
    ).astype(jnp.bfloat16)

    load.wait()
    squares = jnp.zeros((ROWS, 128), jnp.float32)
    for f in range(HALF // 128):
        part = emb[:, 128 * f:128 * f + 128]
        squares = squares + part * part
    mine = jnp.sum(squares.T, axis=0, keepdims=True)
    sq_mine[...] = mine
    pl.semaphore_wait(barrier, NZ - 1 + NXY - 1 + 1)
    sq_copy = pltpu.make_async_remote_copy(
        sq_mine, sq_peer, sq_sem.at[0], sq_sem.at[1], device_id=partner, device_id_type=MESH)
    sq_copy.start()

    place_hot = []
    for k in range(NZ):
        want = lax.broadcasted_iota(jnp.int32, (ROOM, ROWS), 0) + k * ROOM
        place_hot.append(hot(want == slot))
    meta_copies = []
    for k in (0,) + NEAR:
        meta = lax.dot_general(values, place_hot[k], NT, preferred_element_type=jnp.float32)
        meta = jnp.where(sub8 == 3, over, meta)
        if k == 0:
            min_[0] = meta
        else:
            mout[k] = meta
            copy = pltpu.make_async_remote_copy(
                mout.at[k], min_.at[NZ - k], ms.at[k], mr.at[NZ - k], device_id=at_z(k), device_id_type=MESH)
            copy.start()
            meta_copies.append((NZ - k, copy))

    sq_copy.wait()
    scale = lax.rsqrt((sq_mine[...] + sq_peer[...]) / D + 1e-06)
    scale = jnp.broadcast_to(scale, (128, ROWS)).T
    for f in range(HALF // 128):
        unit[:, 128 * f:128 * f + 128] = (emb[:, 128 * f:128 * f + 128] * scale).astype(jnp.bfloat16)

    z_copies = {}
    for k in NEAR + (0,):
        packed = jnp.dot(place_hot[k], unit[...], preferred_element_type=jnp.float32).astype(jnp.bfloat16)
        if k == 0:
            zin[0] = packed
        else:
            zout[k] = packed
            copy = pltpu.make_async_remote_copy(
                zout.at[k], zin.at[NZ - k], zs.at[k], zr.at[NZ - k], device_id=at_z(k), device_id_type=MESH)
            copy.start()
            z_copies[NZ - k] = copy
    meta_by = dict(meta_copies)

    def wait_meta(k):
        if k:
            meta_by[k].wait_recv()

    x_copies = {}

    def forward(g):
        members, _, count = GROUPS[g]
        total = None
        for m, k in enumerate(members):
            meta = min_[k]
            valid = meta[0:1, :] > 0.5
            there = jnp.where(valid, meta[1:2, :] * float(count) + meta[2:3, :] + float(CAP * m), -1.0)
            there = there.astype(jnp.int32)
            want = lax.broadcasted_iota(jnp.int32, (NXY * count, ROOM), 0)
            if k:
                z_copies[k].wait_recv()
            part = jnp.dot(hot(want == there), zin[k], preferred_element_type=jnp.float32)
            total = part if total is None else total + part
        for d in range(NXY):
            block = total[count * d:count * d + count, :].astype(jnp.bfloat16)
            if d == 0:
                rows[g][0] = block
            else:
                xout[g][d] = block
                copy = pltpu.make_async_remote_copy(
                    xout[g].at[d], rows[g].at[neg(d)], xs.at[g, d], xr.at[g, neg(d)],
                    device_id=at_xy(d), device_id_type=MESH)
                copy.start()
                x_copies[g, neg(d)] = copy

    p_copies = {}

    def share(g):
        for j in range(NXY):
            if j:
                x_copies[g, j].wait_recv()
            copy = pltpu.make_async_remote_copy(
                rows[g].at[j], rows_p[g].at[j], ps.at[g, j], pr.at[g, j],
                device_id=partner, device_id_type=MESH)
            copy.start()
            p_copies[g, j] = copy

    for k in GROUPS[0][0]:
        wait_meta(k)
    forward(0)

    for k in range(NZ):
        if k not in GROUPS[0][0]:
            wait_meta(k)
    ids = jnp.zeros((NXY, 128), jnp.float32)
    flag = jnp.zeros((1, 128), jnp.float32)
    sub16 = lax.broadcasted_iota(jnp.int32, (NXY, 128), 0)
    for k in range(NZ):
        meta = min_[k]
        valid = meta[0:1, :] > 0.5
        to = jnp.where(valid, meta[1:2, :], -1.0).astype(jnp.int32)
        place_k = meta[2:3, :].astype(jnp.int32) + LANE[k]
        left = jnp.where(sub16 == to, meta[0:1, :], 0.0).astype(jnp.bfloat16)
        ids = ids + lax.dot_general(left, hot(sub128 == place_k), NT, preferred_element_type=jnp.float32)
        flag = jnp.maximum(flag, meta[3:4, :])
    ids = jnp.where(lax.broadcasted_iota(jnp.int32, (NXY, 128), 1) == 127, flag, ids)
    id_copies = {}
    for d in range(NXY):
        if d == 0:
            idin[0] = ids[0:1, :]
        else:
            idout[d] = ids[d:d + 1, :]
            copy = pltpu.make_async_remote_copy(
                idout.at[d], idin.at[neg(d)], ids_s.at[d], ids_r.at[neg(d)], device_id=at_xy(d), device_id_type=MESH)
            copy.start()
            id_copies[neg(d)] = copy

    forward(1)
    share(0)
    for j in range(1, NXY):
        id_copies[j].wait_recv()
    flag = jnp.zeros((1, 128), jnp.float32)
    last = lax.broadcasted_iota(jnp.int32, (1, 128), 1) == 127
    for j in range(NXY):
        line = idin[j]
        flag = jnp.maximum(flag, jnp.where(last, line, 0.0))
        line = jnp.where(last | (line < 0.5), -1.0, line)
        turned = jnp.broadcast_to(line, (128, 128)).T
        for g, (_, base, count) in enumerate(GROUPS):
            idkey[g][count * j:count * j + count, :] = turned[base:base + count, :]
    flag_ref[...] = flag
    for g, (_, _, count) in enumerate(GROUPS):
        half = count * NXY // 2
        for h in range(-(-half // 128)):
            size = min(128, half - 128 * h)
            block = idkey[g][pl.ds(pl.multiple_of(half * c + 128 * h, 8), size), :]
            idq[g, :, 128 * h:128 * h + size] = block.T[0:8, :]
        top[g][...] = jnp.full(top[g].shape, -float(D), jnp.float32)
    sub256 = lax.broadcasted_iota(jnp.int32, (CLUSTERS, 128), 0).astype(jnp.float32) + 1.0

    def member_sums(g):
        count = GROUPS[g][2]
        width = count * NXY
        seen = jnp.zeros((CLUSTERS, 128), jnp.float32)
        parts = []
        for h in range(width // 128):
            line = idkey[g][128 * h:128 * h + 128, :].T[0:1, :]
            member = jnp.where(sub256 == line, 1.0, 0.0)
            seen = seen + member
            parts.append(member.astype(jnp.bfloat16))
        return seen, jnp.dot(
            jnp.concatenate(parts, axis=1), rows[g][...].reshape(width, HALF), preferred_element_type=jnp.float32)

    def await_partner(g):
        for j in range(NXY):
            p_copies[g, j].wait_recv()

    def score(kg, qg):
        nk, nq = GROUPS[kg][2] * NXY, GROUPS[qg][2] * NXY // 2
        first = pl.multiple_of((NXY // 2) * c, 8)
        query = rows[qg][pl.ds(first, NXY // 2)].reshape(nq, HALF)
        query_p = rows_p[qg][pl.ds(first, NXY // 2)].reshape(nq, HALF)
        scores = lax.dot_general(rows[kg][...].reshape(nk, HALF), query, NT, preferred_element_type=jnp.float32)
        scores = scores + lax.dot_general(
            rows_p[kg][...].reshape(nk, HALF), query_p, NT, preferred_element_type=jnp.float32)
        for h in range(-(-nq // 128)):
            size = min(128, nq - 128 * h)
            same = idkey[kg][...][:, :size] == idq[qg, 0:1, 128 * h:128 * h + size]
            if kg == qg:
                apart = lax.broadcasted_iota(jnp.int32, (nk, size), 0) - lax.broadcasted_iota(jnp.int32, (nk, size), 1)
                same = same & (apart != nq * c + 128 * h)
            kept = jnp.where(same, scores[:, 128 * h:128 * h + size], -float(D))
            kept = jnp.max(kept.reshape(nk // 8, 8, size), axis=0)
            old = top[qg][:, 128 * h:128 * h + size]
            top[qg][:, 128 * h:128 * h + size] = jnp.maximum(old, kept)

    counts, total = member_sums(0)
    sums[...] = total
    await_partner(0)
    score(0, 0)
    forward(2)
    share(1)
    more, total = member_sums(1)
    counts = counts + more
    sums[...] += total
    await_partner(1)
    score(0, 1)
    score(1, 0)
    score(1, 1)
    forward(3)
    share(2)
    more, total = member_sums(2)
    counts = counts + more
    sums[...] += total
    await_partner(2)
    for g in range(2):
        score(g, 2)
        score(2, g)
    score(2, 2)
    share(3)
    await_partner(3)
    for g in range(3):
        score(g, 3)
        score(3, g)
    score(3, 3)
    for g, (_, base, count) in enumerate(GROUPS):
        half = count * NXY // 2
        pieces = []
        for h in range(-(-half // 128)):
            size = min(128, half - 128 * h)
            best = jnp.max(top[g][:, 128 * h:128 * h + size], axis=0, keepdims=True) * (1.0 / D)
            pieces.append(jnp.broadcast_to(best, (128, size)).T)
        best = jnp.concatenate(pieces, axis=0) if len(pieces) > 1 else pieces[0]
        for i in range(NXY // 2):
            column[i, base:base + count, :] = best[count * i:count * i + count, :]
    for i in range(NXY // 2):
        best_out[i] = column[i].T[0:1, :]

    def best_copy(i):
        jx, jy = 2 * c + i // 4, i % 4
        there = (z * 16 + ((x + jx) % 4) * 4 + (y + jy) % 4, c)
        return pltpu.make_async_remote_copy(
            best_out.at[i], ret1.at[8 * c + i], bs.at[i], br.at[i], device_id=there, device_id_type=MESH)

    @pl.when(c == 0)
    def _():
        ret1[0] = best_out[0]

    @pl.when(c == 1)
    def _():
        best_copy(0).start()

    for i in range(1, 8):
        best_copy(i).start()

    more, total = member_sums(3)
    counts = counts + more
    cent_load.wait()
    number = jnp.sum(counts, axis=1, keepdims=True)
    mass = jnp.broadcast_to(mass_ref[...], (128, CLUSTERS)).T[:, 0:1]
    cent[...] = (mass * cent[...] + (sums[...] + total)) / (mass + number)
    nc_copy = pltpu.make_async_copy(cent, nc_ref, local_sem.at[2])
    nc_copy.start()

    @pl.when(c == 1)
    def _():
        best_copy(0).wait()

    for i in range(1, 8):
        best_copy(i).wait()
    half = pltpu.make_async_remote_copy(
        ret1.at[pl.ds(8 * c, 8)], ret1.at[pl.ds(8 * c, 8)], es.at[0], es.at[1], device_id=partner, device_id_type=MESH)
    half.start()
    half.wait()
    back = []
    for k in NEAR[::-1]:
        copy = pltpu.make_async_remote_copy(
            ret1, ret2.at[NZ - k], fs.at[k], fr.at[NZ - k], device_id=at_z(k), device_id_type=MESH)
        copy.start()
        back.append((NZ - k, copy))
    tile_t = tiles_i[0]
    lane_t = tiles_i[1]
    result = jnp.zeros((8, 128), jnp.float32)

    def pick(k, result):
        for j in range(NXY):
            line = ret1[j] if k == 0 else ret2[k, j]
            got = jnp.take_along_axis(
                jnp.broadcast_to(line, (8, 128)), lane_t, axis=1, mode="promise_in_bounds")
            result = jnp.where(tile_t == k * 16 + j, got, result)
        return result

    result = pick(0, result)
    for k, copy in back[::-1]:
        copy.wait_recv()
        result = pick(k, result)
    for b in range(ROWS // 128):
        best_ref[:, 128 * b:128 * b + 128] = result[b:b + 1, :]

    for _, copy in back:
        copy.wait_send()
    for _, copy in meta_copies:
        copy.wait_send()
    for copy in z_copies.values():
        copy.wait_send()
    for copy in x_copies.values():
        copy.wait_send()
    for copy in id_copies.values():
        copy.wait_send()
    for copy in p_copies.values():
        copy.wait_send()
    nc_copy.wait()


def compact(embeddings, cluster_id, centroids, cluster_mass):
    vmem = pl.BlockSpec(memory_space=pltpu.VMEM)
    anywhere = pl.BlockSpec(memory_space=pl.ANY)
    f32, bf16, i32 = jnp.float32, jnp.bfloat16, jnp.int32
    dma = pltpu.SemaphoreType.DMA
    return pl.pallas_call(
        exchange_kernel,
        out_shape=(
            jax.ShapeDtypeStruct((1, ROWS), f32),
            jax.ShapeDtypeStruct((CLUSTERS, HALF), f32),
            jax.ShapeDtypeStruct((1, 128), f32),
        ),
        in_specs=[anywhere, vmem, anywhere, vmem],
        out_specs=(vmem, anywhere, vmem),
        scratch_shapes=[
            pltpu.VMEM((ROWS, HALF), f32),
            pltpu.VMEM((ROWS, HALF), bf16),
            pltpu.VMEM((1, ROWS), f32),
            pltpu.VMEM((1, ROWS), f32),
            pltpu.VMEM((NZ, ROOM, HALF), bf16),
            pltpu.VMEM((NZ, ROOM, HALF), bf16),
            pltpu.VMEM((NZ, 8, 128), f32),
            pltpu.VMEM((NZ, 8, 128), f32),
            *[pltpu.VMEM((NXY, count, HALF), bf16) for _, _, count in GROUPS],
            pltpu.VMEM((NXY, 1, 128), f32),
            *[pltpu.VMEM((NXY, count, HALF), bf16) for _, _, count in GROUPS],
            *[pltpu.VMEM((NXY, count, HALF), bf16) for _, _, count in GROUPS],
            pltpu.VMEM((NXY, 1, 128), f32),
            *[pltpu.VMEM((NXY * count, 128), f32) for _, _, count in GROUPS],
            *[pltpu.VMEM((8, NXY // 2 * count), f32) for _, _, count in GROUPS],
            pltpu.VMEM((4, 8, 384), f32),
            pltpu.VMEM((CLUSTERS, HALF), f32),
            pltpu.VMEM((2, 8, 128), i32),
            pltpu.VMEM((8, 128, 128), f32),
            pltpu.VMEM((8, 1, 128), f32),
            pltpu.VMEM((NXY, 1, 128), f32),
            pltpu.VMEM((NZ, NXY, 1, 128), f32),
            pltpu.VMEM((CLUSTERS, HALF), f32),
            dma((3,)), dma((2,)), dma((NZ,)), dma((NZ,)), dma((NZ,)), dma((NZ,)),
            dma((4, NXY)), dma((4, NXY)), dma((NXY,)), dma((NXY,)), dma((4, NXY)), dma((4, NXY)),
            dma((8,)), dma((8,)), dma((2,)), dma((NZ,)), dma((NZ,)),
        ],
        compiler_params=pltpu.CompilerParams(
            collective_id=0, has_side_effects=True, vmem_limit_bytes=48 * 2**20),
    )(embeddings, cluster_id.reshape(1, ROWS), centroids, cluster_mass.reshape(1, CLUSTERS))


def from_partner(value):
    return lax.ppermute(value, "mp", [(0, 1), (1, 0)])


def general(embeddings, cluster_id, centroids, cluster_mass):
    owners = lax.axis_size("dp")
    row_count = embeddings.shape[0]
    slot_count = 2 * row_count
    capacity = slot_count // owners
    cluster_count = centroids.shape[0]
    core = lax.axis_index("mp")
    squares = jnp.sum(embeddings * embeddings, axis=1)
    squares = squares + from_partner(squares)
    unit = (embeddings * lax.rsqrt(squares / D + 1e-06)[:, None]).astype(jnp.bfloat16)
    owner = cluster_id // cluster_count
    local = cluster_id - owner * cluster_count
    owner_hot = (owner[:, None] == jnp.arange(owners, dtype=jnp.int32)[None, :]).astype(jnp.bfloat16)
    row_index = jnp.arange(row_count, dtype=jnp.int32)
    lower = (row_index[:, None] >= row_index[None, :]).astype(jnp.bfloat16)
    running = jnp.dot(lower, owner_hot, preferred_element_type=jnp.float32)
    rank = jnp.sum(running * owner_hot.astype(jnp.float32), axis=1).astype(jnp.int32) - 1
    slot = owner * capacity + rank
    slot_index = jnp.arange(slot_count, dtype=jnp.int32)
    placed = slot_index[:, None] == slot[None, :]
    outgoing = jnp.dot(
        placed.astype(jnp.bfloat16), unit, preferred_element_type=jnp.float32
    ).astype(jnp.bfloat16)
    out_ids = jnp.max(jnp.where(placed, local[None, :] + 1, 0), axis=1) - 1
    incoming = lax.all_to_all(outgoing, "dp", split_axis=0, concat_axis=0, tiled=True)
    in_ids = lax.all_to_all(out_ids, "dp", split_axis=0, concat_axis=0, tiled=True)
    member = (jnp.arange(cluster_count, dtype=jnp.int32)[:, None] == in_ids[None, :]).astype(jnp.bfloat16)
    sums = jnp.dot(member, incoming, preferred_element_type=jnp.float32)
    counts = jnp.sum(member.astype(jnp.float32), axis=1)
    new_centroids = (cluster_mass[:, None] * centroids + sums) / (cluster_mass + counts)[:, None]
    half = slot_count // 2
    start = core * half
    contract = (((1,), (1,)), ((), ()))
    other = from_partner(incoming)
    scores = lax.dot_general(
        lax.dynamic_slice_in_dim(incoming, start, half, 0), incoming, contract, preferred_element_type=jnp.float32)
    scores = scores + lax.dot_general(
        lax.dynamic_slice_in_dim(other, start, half, 0), other, contract, preferred_element_type=jnp.float32)
    scores = scores / D
    query_ids = lax.dynamic_slice_in_dim(in_ids, start, half, 0)
    query_pos = start + jnp.arange(half, dtype=jnp.int32)
    same = (
        (query_ids[:, None] == in_ids[None, :])
        & (query_ids[:, None] >= 0)
        & (query_pos[:, None] != slot_index[None, :])
    )
    best = jnp.max(jnp.where(same, scores, -1.0), axis=1)
    best_p = from_partner(best)
    low, high = jnp.where(core == 0, best, best_p), jnp.where(core == 0, best_p, best)
    returned = lax.all_to_all(
        jnp.concatenate([low, high]), "dp", split_axis=0, concat_axis=0, tiled=True)
    return jnp.take(returned, slot), new_centroids


def shards(embeddings, cluster_id, centroids, cluster_mass):
    best, new_centroids, flag = compact(embeddings, cluster_id, centroids, cluster_mass)
    return lax.cond(
        flag[0, 127] > 0.5,
        lambda *args: general(*args),
        lambda *args: (best.reshape(ROWS), new_centroids),
        embeddings, cluster_id, centroids, cluster_mass,
    )


def solution(mesh):
    in_specs = (P("dp", "mp"), P("dp"), P("dp", "mp"), P("dp"))
    out_specs = (P("dp"), P("dp", "mp"))
    return jax.shard_map(shards, mesh=mesh, in_specs=in_specs, out_specs=out_specs, check_vma=False)
```

```python
import functools

import jax
import jax.numpy as jnp
from jax import lax
from jax.experimental import pallas as pl
from jax.experimental.pallas import tpu as pltpu
from jax.sharding import PartitionSpec as P

D = 1024
HALF = 512
ROWS = 768
CLUSTERS = 256
CAP = 12
ROOM = 128
NZ = 8
NXY = 16
GROUPS = (((0, 1, 7), 0, 40), ((2, 6), 40, 24))
LANE = {k: base + CAP * m for members, base, _ in GROUPS for m, k in enumerate(members)}
FAR = (3, 5, 4)
FAR_SETS = (((3, 5), 0, 24, 2731, 16), ((4,), 2, 16, 1, 4))
WIDTH = tuple(count * NXY for _, _, count in GROUPS)
MESH = pl.DeviceIdType.MESH
NT = (((1,), (1,)), ((), ()))
NEAR = (1, 7, 2, 6)


def neg(d):
    return ((4 - d // 4) % 4) * 4 + (4 - d % 4) % 4


def hot(mask):
    return jnp.where(mask, 1.0, 0.0).astype(jnp.bfloat16)


def exchange_kernel(
    emb_ref, cid_ref, cent_ref, mass_ref,
    best_ref, nc_ref, flag_ref,
    emb, unit, sq_mine, sq_peer, zout, zin, z_far, z_far_p, mout, min_, xo0, xo1, idout, fo0, fo1, fi0, fi1, fid_out, fid_in,
    r0, r1, p0, p1, idin, ik0, ik1, ik_far, top, idq, acc0, acc1, acc_far, top_far, sums,
    tiles_i, column, best_out, far_out, ret1, ret2, far_z, back_out, far_ret, cent, cid_v, mass_v,
    local_sem, sq_sem, zs, zr, ms, mr, xs, xr, ids_s, ids_r, ps, pr, bs, br, fs, fr,
    ws, wr, vs, vr, us, ur, ts, tr,
):
    xout, rows, rows_p, idkey = (xo0, xo1), (r0, r1), (p0, p1), (ik0, ik1)
    fout, fin, acc = (fo0, fo1), (fi0, fi1), (acc0, acc1)
    me = lax.axis_index("dp")
    c = lax.axis_index("mp")
    z, x, y = me // 16, (me // 4) % 4, me % 4

    def at_z(k):
        return (((z + k) % NZ) * 16 + x * 4 + y, c)

    def at_xy(d):
        return (z * 16 + ((x + d // 4) % 4) * 4 + (y + d % 4) % 4, c)

    partner = (me, 1 - c)

    def send(src, dst, send_sem, recv_sem, to):
        copy = pltpu.make_async_remote_copy(src, dst, send_sem, recv_sem, device_id=to, device_id_type=MESH)
        copy.start()
        return copy

    cid_load = pltpu.make_async_copy(cid_ref, cid_v, local_sem.at[3])
    cid_load.start()
    mass_load = pltpu.make_async_copy(mass_ref, mass_v, local_sem.at[4])
    mass_load.start()
    load = pltpu.make_async_copy(emb_ref, emb, local_sem.at[0])
    load.start()
    cent_load = pltpu.make_async_copy(cent_ref, cent, local_sem.at[1])
    cent_load.start()
    barrier = pltpu.get_barrier_semaphore()
    for k in range(1, NZ):
        pl.semaphore_signal(barrier, inc=1, device_id=at_z(k), device_id_type=MESH)
    for d in range(1, NXY):
        pl.semaphore_signal(barrier, inc=1, device_id=at_xy(d), device_id_type=MESH)
        pl.semaphore_signal(barrier, inc=1, device_id=(at_xy(d)[0], 1 - c), device_id_type=MESH)
    for k in FAR:
        pl.semaphore_signal(barrier, inc=1, device_id=(at_z(k)[0], 1 - c), device_id_type=MESH)
    pl.semaphore_signal(barrier, inc=1, device_id=partner, device_id_type=MESH)

    cid_load.wait()
    cid = cid_v[...].reshape(1, ROWS)
    owner = cid >> 8
    dz = ((owner >> 4) - z) & 7
    dxy = ((((owner >> 2) & 3) - x) & 3) * 4 + (((owner & 3) - y) & 3)
    target = dz * 16 + dxy
    lane128 = lax.broadcasted_iota(jnp.int32, (128, 128), 1)
    sub128 = lax.broadcasted_iota(jnp.int32, (128, 128), 0)
    upto = hot(sub128 <= lane128)
    sub8 = lax.broadcasted_iota(jnp.int32, (8, 128), 0)
    sub16 = lax.broadcasted_iota(jnp.int32, (NXY, 128), 0)
    last = lax.broadcasted_iota(jnp.int32, (1, 128), 1) == 127
    base_t = jnp.zeros((128, 128), jnp.float32)
    base_z = jnp.zeros((8, 128), jnp.float32)
    ranks, places = [], []
    for b in range(ROWS // 128):
        cut = slice(128 * b, 128 * b + 128)
        is_t = sub128 == target[:, cut]
        is_z = sub8 == dz[:, cut]
        run_t = base_t + jnp.dot(hot(is_t), upto, preferred_element_type=jnp.float32)
        run_z = base_z + jnp.dot(hot(is_z), upto, preferred_element_type=jnp.float32)
        ranks.append(jnp.sum(jnp.where(is_t, run_t, 0.0), axis=0, keepdims=True) - 1.0)
        places.append(jnp.sum(jnp.where(is_z, run_z, 0.0), axis=0, keepdims=True) - 1.0)
        base_t = jnp.broadcast_to(run_t[:, 127:128], (128, 128))
        base_z = jnp.broadcast_to(run_z[:, 127:128], (8, 128))
    near_most = jnp.where((sub8 < 3) | (sub8 > 5), base_z, 0.0)
    over = jnp.where(jnp.max(near_most, axis=0, keepdims=True) > float(ROOM), 1.0, 0.0)
    rank_f = jnp.concatenate(ranks, axis=1)
    rank = rank_f.astype(jnp.int32)
    place = jnp.concatenate(places, axis=1).astype(jnp.int32)
    slot = jnp.where(place < ROOM, dz * ROOM + place, -1)
    far_row = (dz >= 3) & (dz <= 5)
    far_lane = jnp.where(dz == 3, rank, jnp.where(dz == 5, rank + CAP, rank + 2 * CAP))
    far_lane = jnp.where(far_row, far_lane, -1)
    far_slot = (
        jnp.where((dz == 3) | (dz == 5), dxy * FAR_SETS[0][2] + far_lane, -1),
        jnp.where(dz == 4, dxy * FAR_SETS[1][2] + rank, -1),
    )
    turned = ((4 - (dxy >> 2)) & 3) * 4 + ((4 - (dxy & 3)) & 3)
    tile_of = jnp.where(far_row, NZ * NXY + dxy, dz * NXY + turned)
    lane_of = jnp.where(far_row, far_lane, rank)
    for k in (0,) + NEAR:
        lane_of = jnp.where(dz == k, rank + LANE[(NZ - k) % NZ], lane_of)
    tiles_i[...] = jnp.zeros_like(tiles_i)
    for b in range(ROWS // 128):
        cut = slice(128 * b, 128 * b + 128)
        tiles_i[0, b:b + 1, :] = tile_of[:, cut]
        tiles_i[1, b:b + 1, :] = lane_of[:, cut]
    row8 = lax.broadcasted_iota(jnp.int32, (8, ROWS), 0)
    local = ((cid & 255) + 1).astype(jnp.float32)
    values = jnp.where(
        row8 == 0, local,
        jnp.where(row8 == 1, dxy.astype(jnp.float32), jnp.where(row8 == 2, rank_f, 0.0)),
    ).astype(jnp.bfloat16)

    load.wait()
    squares = jnp.zeros((ROWS, 128), jnp.float32)
    for f in range(HALF // 128):
        part = emb[:, 128 * f:128 * f + 128]
        squares = squares + part * part
    mine = jnp.sum(squares.T, axis=0, keepdims=True)
    sq_mine[...] = mine
    pl.semaphore_wait(barrier, NZ - 1 + 2 * (NXY - 1) + len(FAR) + 1)
    sq_copy = send(sq_mine, sq_peer, sq_sem.at[0], sq_sem.at[1], partner)

    place_hot = {}
    for k in (0,) + NEAR:
        want = lax.broadcasted_iota(jnp.int32, (ROOM, ROWS), 0) + k * ROOM
        place_hot[k] = hot(want == slot)
    far_hot = [
        hot(lax.broadcasted_iota(jnp.int32, (NXY * count, ROWS), 0) == far_slot[e])
        for e, (_, _, count, _, _) in enumerate(FAR_SETS)
    ]

    sq_copy.wait()
    scale = lax.rsqrt((sq_mine[...] + sq_peer[...]) / D + 1e-06)
    scale = jnp.broadcast_to(scale, (128, ROWS)).T
    for f in range(HALF // 128):
        unit[:, 128 * f:128 * f + 128] = (emb[:, 128 * f:128 * f + 128] * scale).astype(jnp.bfloat16)

    z_copies, meta_copies, f_copies, fid_copies = {}, {}, {}, {}

    def pack(k):
        packed = jnp.dot(place_hot[k], unit[...], preferred_element_type=jnp.float32).astype(jnp.bfloat16)
        if k == 0:
            zin[0] = packed
        else:
            zout[k] = packed
            z_copies[NZ - k] = send(zout.at[k], zin.at[NZ - k], zs.at[k], zr.at[NZ - k], at_z(k))

    pack(1)
    pack(7)
    left = jnp.where(
        far_row & (lax.broadcasted_iota(jnp.int32, (NXY, ROWS), 0) == dxy), local, 0.0).astype(jnp.bfloat16)
    right = hot(lax.broadcasted_iota(jnp.int32, (128, ROWS), 0) == far_lane)
    ids = lax.dot_general(left, right, NT, preferred_element_type=jnp.float32)
    for d in range(NXY):
        if d == 0:
            fid_in[0] = ids[0:1, :]
        else:
            fid_out[d] = ids[d:d + 1, :]
            fid_copies[neg(d)] = send(fid_out.at[d], fid_in.at[neg(d)], vs.at[d], vr.at[neg(d)], at_xy(d))

    def pack_far(e):
        count = FAR_SETS[e][2]
        packed = jnp.dot(far_hot[e], unit[...], preferred_element_type=jnp.float32)
        for d in range(NXY):
            block = packed[count * d:count * d + count, :].astype(jnp.bfloat16)
            if d == 0:
                fin[e][0] = block
            else:
                fout[e][d] = block
                f_copies[e, neg(d)] = send(
                    fout[e].at[d], fin[e].at[neg(d)], ws.at[e, d], wr.at[e, neg(d)], at_xy(d))

    pack_far(0)
    pack_far(1)
    for k in NEAR + (0,):
        meta = lax.dot_general(values, place_hot[k], NT, preferred_element_type=jnp.float32)
        if k == 0:
            min_[0] = meta
        else:
            mout[k] = meta
            meta_copies[NZ - k] = send(mout.at[k], min_.at[NZ - k], ms.at[k], mr.at[NZ - k], at_z(k))
    pack(2)
    pack(6)
    pack(0)

    x_copies, p_copies = {}, {}

    def forward(g):
        members, _, count = GROUPS[g]
        total = None
        for m, k in enumerate(members):
            if g == 0 and k:
                meta_copies[k].wait_recv()
            meta = min_[k]
            valid = meta[0:1, :] > 0.5
            there = jnp.where(valid, meta[1:2, :] * float(count) + meta[2:3, :] + float(CAP * m), -1.0)
            there = there.astype(jnp.int32)
            want = lax.broadcasted_iota(jnp.int32, (NXY * count, ROOM), 0)
            if k:
                z_copies[k].wait_recv()
            part = jnp.dot(hot(want == there), zin[k], preferred_element_type=jnp.float32)
            total = part if total is None else total + part
        for d in range(NXY):
            block = total[count * d:count * d + count, :].astype(jnp.bfloat16)
            if d == 0:
                rows[g][0] = block
            else:
                xout[g][d] = block
                x_copies[g, neg(d)] = send(
                    xout[g].at[d], rows[g].at[neg(d)], xs.at[g, d], xr.at[g, neg(d)], at_xy(d))

    def share(g):
        for j in range(NXY):
            if j:
                x_copies[g, j].wait_recv()
            p_copies[g, j] = send(rows[g].at[j], rows_p[g].at[j], ps.at[g, j], pr.at[g, j], partner)

    def share_far(kk):
        z_copies[FAR[kk]].wait_recv()
        p_copies[2 + kk, 0] = send(z_far.at[kk], z_far_p.at[kk], ps.at[2 + kk, 0], pr.at[2 + kk, 0], partner)

    for j in range(1, NXY):
        fid_copies[j].wait_recv()
    known = jnp.concatenate([fid_in[j] for j in range(NXY)], axis=0).astype(jnp.bfloat16)
    back_at = jnp.zeros((NXY, 128), jnp.float32)
    far_values, far_places = [], []
    for planes, first, count, factor, shift in FAR_SETS:
        width = NXY * count
        flat = lax.broadcasted_iota(jnp.int32, (1, width), 1)
        holder = (flat * factor) >> shift
        within = flat - holder * count
        lane = jnp.where(within < CAP * len(planes), within + CAP * first, -1)
        spread = hot(lax.broadcasted_iota(jnp.int32, (128, width), 0) == lane)
        mine16 = lax.broadcasted_iota(jnp.int32, (NXY, width), 0) == holder
        far_ids = jnp.dot(known, spread, preferred_element_type=jnp.float32)
        far_ids = jnp.sum(jnp.where(mine16, far_ids, 0.0), axis=0, keepdims=True)
        low = lax.broadcasted_iota(jnp.int32, (8, width), 0) * CAP
        inside = (within >= low) & (within < low + CAP) & (low < CAP * len(planes)) & (far_ids > 0.5)
        base_f = jnp.zeros((8, 128), jnp.float32)
        runs = []
        for b in range(width // 128):
            run = base_f + jnp.dot(hot(inside[:, 128 * b:128 * b + 128]), upto, preferred_element_type=jnp.float32)
            runs.append(run)
            base_f = jnp.broadcast_to(run[:, 127:128], (8, 128))
        over = jnp.maximum(over, jnp.where(jnp.max(base_f, axis=0, keepdims=True) > float(ROOM), 1.0, 0.0))
        far_place = jnp.where(inside, jnp.concatenate(runs, axis=1) - 1.0, -1.0)
        far_place = jnp.where(far_place < float(ROOM), far_place, -1.0)
        any_place = jnp.maximum(jnp.max(far_place, axis=0, keepdims=True), 0.0)
        back_at = back_at + lax.dot_general(
            jnp.where(mine16, any_place, 0.0).astype(jnp.bfloat16), spread, NT, preferred_element_type=jnp.float32)
        far_values.append(jnp.broadcast_to(far_ids, (8, width)).astype(jnp.bfloat16))
        far_places.append(far_place)
    back_at = back_at.astype(jnp.int32)

    def relay_far(e):
        planes, _, count, _, _ = FAR_SETS[e]
        width = NXY * count
        chosen = []
        for m, k in enumerate(planes):
            want = lax.broadcasted_iota(jnp.int32, (ROOM, width), 0).astype(jnp.float32)
            chosen.append(hot(want == far_places[e][m:m + 1, :]))
            mout[k] = lax.dot_general(far_values[e], chosen[m], NT, preferred_element_type=jnp.float32)
            meta_copies[NZ - k] = send(mout.at[k], min_.at[NZ - k], ms.at[k], mr.at[NZ - k], at_z(k))
        for j in range(1, NXY):
            f_copies[e, j].wait_recv()
        for m, k in enumerate(planes):
            zout[k] = jnp.dot(
                chosen[m], fin[e][...].reshape(width, HALF), preferred_element_type=jnp.float32).astype(jnp.bfloat16)
            z_copies[NZ - k] = send(
                zout.at[k], z_far.at[FAR.index(NZ - k)], zs.at[k], zr.at[NZ - k], at_z(k))

    forward(0)
    relay_far(0)

    for k in (2, 6):
        meta_copies[k].wait_recv()
    ids = jnp.zeros((NXY, 128), jnp.float32)
    for k in (0,) + NEAR:
        meta = min_[k]
        valid = meta[0:1, :] > 0.5
        to = jnp.where(valid, meta[1:2, :], -1.0).astype(jnp.int32)
        place_k = meta[2:3, :].astype(jnp.int32) + LANE[k]
        left = jnp.where(sub16 == to, meta[0:1, :], 0.0).astype(jnp.bfloat16)
        ids = ids + lax.dot_general(left, hot(sub128 == place_k), NT, preferred_element_type=jnp.float32)
    id_copies = {}
    for d in range(NXY):
        if d == 0:
            idin[0] = ids[0:1, :]
        else:
            idout[d] = ids[d:d + 1, :]
            id_copies[neg(d)] = send(idout.at[d], idin.at[neg(d)], ids_s.at[d], ids_r.at[neg(d)], at_xy(d))

    forward(1)
    relay_far(1)

    share(0)
    for j in range(1, NXY):
        id_copies[j].wait_recv()
    for j in range(NXY):
        line = idin[j]
        line = jnp.where(line < 0.5, -1.0, line)
        turned = jnp.broadcast_to(line, (128, 128)).T
        for g, (_, base, count) in enumerate(GROUPS):
            idkey[g][count * j:count * j + count, :] = turned[base:base + count, :]

    for g in range(2):
        half = WIDTH[g] // 2
        for h in range(-(-half // 128)):
            size = min(128, half - 128 * h)
            block = idkey[g][pl.ds(pl.multiple_of(half * c + 128 * h, 8), size), :]
            idq[g, :, 128 * h:128 * h + size] = block.T[0:8, :]
    for ref in (top, top_far, acc0, acc1, acc_far):
        ref[...] = jnp.full(ref.shape, -float(D), jnp.float32)
    sub256 = lax.broadcasted_iota(jnp.int32, (CLUSTERS, 128), 0).astype(jnp.float32) + 1.0

    def member_sums(source, key):
        seen = jnp.zeros((CLUSTERS, 128), jnp.float32)
        parts = []
        for h in range(key.shape[0] // 128):
            line = source[128 * h:128 * h + 128, :].T[0:1, :]
            member = jnp.where(sub256 == line, 1.0, 0.0)
            seen = seen + member
            parts.append(member.astype(jnp.bfloat16))
        member = jnp.concatenate(parts, axis=1) if len(parts) > 1 else parts[0]
        return seen, jnp.dot(member, key, preferred_element_type=jnp.float32)

    def near_sums(g):
        return member_sums(idkey[g], rows[g][...].reshape(WIDTH[g], HALF))

    def keys_of(g):
        return rows[g][...].reshape(WIDTH[g], HALF), rows_p[g][...].reshape(WIDTH[g], HALF)

    def own_half(g):
        half = WIDTH[g] // 2
        first = pl.ds(pl.multiple_of(NXY // 2 * c, 8), NXY // 2)
        return rows[g][first].reshape(half, HALF), rows_p[g][first].reshape(half, HALF)

    def nt(a, b):
        return lax.dot_general(a, b, NT, preferred_element_type=jnp.float32)

    def score_near(e):
        pairs = [(e, e)] + [pair for g in range(e) for pair in ((g, e), (e, g))]
        own = [nt(keys_of(kg)[0], own_half(qg)[0]) for kg, qg in pairs]
        for j in range(NXY):
            p_copies[e, j].wait_recv()
        for (kg, qg), part in zip(pairs, own):
            nk, nq = WIDTH[kg], WIDTH[qg] // 2
            scores = part + nt(keys_of(kg)[1], own_half(qg)[1])
            for h in range(-(-nq // 128)):
                cut = slice(128 * h, min(128 * h + 128, nq))
                size = cut.stop - cut.start
                same = idkey[kg][...][:, :size] == idq[qg, 0:1, cut]
                if kg == qg:
                    apart = (lax.broadcasted_iota(jnp.int32, (nk, size), 0)
                             - lax.broadcasted_iota(jnp.int32, (nk, size), 1))
                    same = same & (apart != nq * c + 128 * h)
                kept = jnp.where(same, scores[:, cut], -float(D))
                top[qg, :, cut] = jnp.maximum(top[qg, :, cut], jnp.max(kept.reshape(nk // 8, 8, size), axis=0))

    half_far = pl.ds(pl.multiple_of(ROOM // 2 * c, ROOM // 2), ROOM // 2)

    def score_far(planes):
        first, width = planes[0], ROOM * len(planes)
        cut = slice(first, first + len(planes))
        groups = [0, 1] + [2 + kk for kk in range(first + len(planes))]

        def side(g):
            if g < 2:
                return own_half(g)
            return z_far[g - 2, half_far, :], z_far_p[g - 2, half_far, :]

        columns = z_far[cut].reshape(width, HALF)
        own = [nt(side(g)[0], columns) for g in groups]
        for kk in planes:
            p_copies[2 + kk, 0].wait_recv()
        columns = z_far_p[cut].reshape(width, HALF)
        for g, part in zip(groups, own):
            scores = part + nt(side(g)[1], columns)
            n = scores.shape[0]
            if g < 2:
                mine = idkey[g][pl.ds(pl.multiple_of(n * c, 8), n), :]
            else:
                mine = ik_far[g - 2, half_far, :]
            for kk in planes:
                line = min_[FAR[kk]][0:1, :]
                same = mine == line
                if g == 2 + kk:
                    apart = (lax.broadcasted_iota(jnp.int32, (n, ROOM), 1)
                             - lax.broadcasted_iota(jnp.int32, (n, ROOM), 0))
                    same = same & (apart != n * c)
                kept = jnp.where(same, scores[:, ROOM * (kk - first):ROOM * (kk - first) + ROOM], -float(D))
                top_far[kk] = jnp.maximum(top_far[kk], jnp.max(kept.reshape(n // 8, 8, ROOM), axis=0))
                if g < 2:
                    acc[g][...] = jnp.maximum(acc[g][...], kept)
                elif g - 2 < first:
                    acc_far[g - 2] = jnp.maximum(acc_far[g - 2], kept)

    def take_far(kk):
        meta_copies[FAR[kk]].wait_recv()
        line = min_[FAR[kk]][0:1, :]
        ik_far[kk] = jnp.broadcast_to(jnp.where(line < 0.5, -1.0, line), (128, 128)).T
        share_far(kk)

    counts, total = near_sums(0)
    sums[...] = total
    score_near(0)
    share(1)
    take_far(0)
    take_far(1)
    more, total = near_sums(1)
    counts = counts + more
    sums[...] += total
    score_near(1)
    take_far(2)
    score_far((0, 1))
    score_far((2,))
    for g, (_, base, count) in enumerate(GROUPS):
        half = WIDTH[g] // 2
        pieces = []
        for h in range(-(-half // 128)):
            size = min(128, half - 128 * h)
            best = jnp.max(top[g, :, 128 * h:128 * h + size], axis=0, keepdims=True)
            pieces.append(jnp.broadcast_to(best, (128, size)).T)
        best = jnp.concatenate(pieces, axis=0)
        best = jnp.maximum(best, jnp.max(acc[g][...], axis=1, keepdims=True)) * (1.0 / D)
        for i in range(NXY // 2):
            column[i, base:base + count, :] = best[count * i:count * i + count, :]
    for kk in range(3):
        best = jnp.max(top_far[kk], axis=0, keepdims=True)
        if kk < 2:
            mine = jnp.broadcast_to(jnp.max(acc_far[kk], axis=1, keepdims=True), (ROOM // 2, 128))
            mine = jnp.concatenate([jnp.where(c == h, mine, -float(D)) for h in range(2)], axis=0)
            best = jnp.maximum(best, mine.T[0:1, :])
        far_out[kk, :, 0:128] = best * (1.0 / D)
        far_out[kk, :, 128:256] = over
    far_back = []
    for kk, k in enumerate(FAR):
        there = FAR.index(NZ - k)
        for core in range(2):
            far_back.append(send(
                far_out.at[kk], far_z.at[c, there], us.at[core, kk], ur.at[c, there], (at_z(k)[0], core)))
    for i in range(NXY // 2):
        best_out[i] = jnp.where(last, over, column[i].T[0:1, :])

    def best_copy(i, other):
        jx, jy = 2 * c + i // 4, i % 4
        there = (z * 16 + ((x + jx) % 4) * 4 + (y + jy) % 4, 1 - c if other else c)
        return pltpu.make_async_remote_copy(
            best_out.at[i], ret1.at[8 * c + i], bs.at[int(other), i], br.at[8 * c + i],
            device_id=there, device_id_type=MESH)

    @pl.when(c == 0)
    def _():
        ret1[0] = best_out[0]

    @pl.when(c == 1)
    def _():
        best_copy(0, False).start()

    best_copy(0, True).start()
    for i in range(1, 8):
        best_copy(i, False).start()
        best_copy(i, True).start()

    for kk in range(3):
        more, part = member_sums(ik_far[kk], z_far[kk])
        counts = counts + more
        total = part if kk == 0 else total + part
    cent_load.wait()
    mass_load.wait()
    number = jnp.sum(counts, axis=1, keepdims=True)
    mass = jnp.broadcast_to(mass_v[...], (128, CLUSTERS)).T[:, 0:1]
    cent[...] = (mass * cent[...] + (sums[...] + total)) / (mass + number)
    nc_copy = pltpu.make_async_copy(cent, nc_ref, local_sem.at[2])
    nc_copy.start()

    @pl.when(c == 1)
    def _():
        best_copy(0, False).wait_send()

    best_copy(0, True).wait_send()
    for i in range(1, 8):
        best_copy(i, False).wait_send()
        best_copy(i, True).wait_send()

    def best_arrived(j):
        pltpu.make_async_remote_copy(
            best_out.at[0], ret1.at[j], bs.at[0, 0], br.at[j], device_id=partner, device_id_type=MESH).wait_recv()

    @pl.when(c == 1)
    def _():
        best_arrived(0)

    for j in range(1, NXY):
        best_arrived(j)
    back = {}
    for k in (2, 6, 1, 7):
        back[NZ - k] = send(ret1, ret2.at[NZ - k], fs.at[k], fr.at[NZ - k], at_z(k))
    for h in range(2):
        for kk in range(3):
            pltpu.make_async_remote_copy(
                far_out.at[kk], far_z.at[h, kk], us.at[0, kk], ur.at[h, kk],
                device_id=partner, device_id_type=MESH).wait_recv()
    lane16 = lax.broadcasted_iota(jnp.int32, (NXY, 128), 1)
    got = jnp.zeros((NXY, 128), jnp.float32)
    for kk in range(3):
        line = jnp.maximum(far_z[0, kk][:, 0:128], far_z[1, kk][:, 0:128])
        line = jnp.broadcast_to(line, (8, 128))
        found = jnp.concatenate(
            [jnp.take_along_axis(line, back_at[8 * h:8 * h + 8, :], axis=1, mode="promise_in_bounds") for h in range(2)],
            axis=0)
        got = jnp.where(lane16 >= kk * CAP, found, got)
    far_over = far_z[0, 0][:, 128:256]
    for h in range(2):
        for kk in range(3):
            far_over = jnp.maximum(far_over, far_z[h, kk][:, 128:256])
    got = jnp.where(lane16 == 127, far_over, got)
    far_home = {}
    for j in range(NXY):
        if j == 0:
            far_ret[0] = got[0:1, :]
        else:
            back_out[j] = got[j:j + 1, :]
            far_home[neg(j)] = send(back_out.at[j], far_ret.at[neg(j)], ts.at[j], tr.at[neg(j)], at_xy(j))
    tile_t = tiles_i[0]
    lane_t = tiles_i[1]
    result = jnp.zeros((8, 128), jnp.float32)
    flag = jnp.zeros((1, 128), jnp.float32)

    def pick(line, tile, result, flag):
        got = jnp.take_along_axis(jnp.broadcast_to(line, (8, 128)), lane_t, axis=1, mode="promise_in_bounds")
        return jnp.where(tile_t == tile, got, result), jnp.maximum(flag, jnp.where(last, line, 0.0))

    for j in range(NXY):
        result, flag = pick(ret1[j], j, result, flag)
    for k in NEAR:
        back[k].wait_recv()
        for j in range(NXY):
            result, flag = pick(ret2[k, j], k * NXY + j, result, flag)
    for d in range(NXY):
        if d:
            far_home[d].wait_recv()
        result, flag = pick(far_ret[d], NZ * NXY + d, result, flag)
    for b in range(ROWS // 128):
        best_ref[:, 128 * b:128 * b + 128] = result[b:b + 1, :]
    flag_ref[0, 0] = jnp.max(flag).astype(jnp.int32)

    for group in (back, meta_copies, z_copies, x_copies, id_copies, p_copies, f_copies, fid_copies, far_home):
        for copy in group.values():
            copy.wait_send()
    for copy in far_back:
        copy.wait_send()
    nc_copy.wait()


def compact(embeddings, cluster_id, centroids, cluster_mass):
    vmem = pl.BlockSpec(memory_space=pltpu.VMEM)
    anywhere = pl.BlockSpec(memory_space=pl.ANY)
    f32, bf16, i32 = jnp.float32, jnp.bfloat16, jnp.int32
    dma = pltpu.SemaphoreType.DMA
    line = (1, 128)
    return pl.pallas_call(
        exchange_kernel,
        out_shape=(
            jax.ShapeDtypeStruct((1, ROWS), f32),
            jax.ShapeDtypeStruct((CLUSTERS, HALF), f32),
            jax.ShapeDtypeStruct((1, 1), i32),
        ),
        in_specs=[anywhere, anywhere, anywhere, anywhere],
        out_specs=(vmem, anywhere, pl.BlockSpec(memory_space=pltpu.SMEM)),
        scratch_shapes=[
            pltpu.VMEM((ROWS, HALF), f32),
            pltpu.VMEM((ROWS, HALF), bf16),
            pltpu.VMEM((1, ROWS), f32),
            pltpu.VMEM((1, ROWS), f32),
            pltpu.VMEM((NZ, ROOM, HALF), bf16),
            pltpu.VMEM((NZ, ROOM, HALF), bf16),
            pltpu.VMEM((3, ROOM, HALF), bf16),
            pltpu.VMEM((3, ROOM, HALF), bf16),
            pltpu.VMEM((NZ, 8, 128), f32),
            pltpu.VMEM((NZ, 8, 128), f32),
            *[pltpu.VMEM((NXY, count, HALF), bf16) for _, _, count in GROUPS],
            pltpu.VMEM((NXY, *line), f32),
            *[pltpu.VMEM((NXY, far[2], HALF), bf16) for far in FAR_SETS],
            *[pltpu.VMEM((NXY, far[2], HALF), bf16) for far in FAR_SETS],
            pltpu.VMEM((NXY, *line), f32),
            pltpu.VMEM((NXY, *line), f32),
            *[pltpu.VMEM((NXY, count, HALF), bf16) for _, _, count in GROUPS],
            *[pltpu.VMEM((NXY, count, HALF), bf16) for _, _, count in GROUPS],
            pltpu.VMEM((NXY, *line), f32),
            *[pltpu.VMEM((NXY * count, 128), f32) for _, _, count in GROUPS],
            pltpu.VMEM((3, 128, 128), f32),
            pltpu.VMEM((2, 8, 384), f32),
            pltpu.VMEM((2, 8, 384), f32),
            *[pltpu.VMEM((width // 2, 128), f32) for width in WIDTH],
            pltpu.VMEM((2, ROOM // 2, 128), f32),
            pltpu.VMEM((3, 8, 128), f32),
            pltpu.VMEM((CLUSTERS, HALF), f32),
            pltpu.VMEM((2, 8, 128), i32),
            pltpu.VMEM((8, 128, 128), f32),
            pltpu.VMEM((8, *line), f32),
            pltpu.VMEM((3, 1, 256), f32),
            pltpu.VMEM((NXY, *line), f32),
            pltpu.VMEM((NZ, NXY, *line), f32),
            pltpu.VMEM((2, 3, 1, 256), f32),
            pltpu.VMEM((NXY, *line), f32),
            pltpu.VMEM((NXY, *line), f32),
            pltpu.VMEM((CLUSTERS, HALF), f32),
            pltpu.VMEM((ROWS,), i32),
            pltpu.VMEM((1, CLUSTERS), f32),
            dma((5,)), dma((2,)), dma((NZ,)), dma((NZ,)), dma((NZ,)), dma((NZ,)),
            dma((2, NXY)), dma((2, NXY)), dma((NXY,)), dma((NXY,)), dma((5, NXY)), dma((5, NXY)),
            dma((2, 8)), dma((NXY,)), dma((NZ,)), dma((NZ,)),
            dma((2, NXY)), dma((2, NXY)), dma((NXY,)), dma((NXY,)), dma((2, 3)), dma((2, 3)), dma((NXY,)), dma((NXY,)),
        ],
        compiler_params=pltpu.CompilerParams(
            collective_id=0, has_side_effects=True, vmem_limit_bytes=48 * 2**20),
    )(embeddings, cluster_id, centroids, cluster_mass.reshape(1, CLUSTERS))


def from_partner(value):
    return lax.ppermute(value, "mp", [(0, 1), (1, 0)])


def general(embeddings, cluster_id, centroids, cluster_mass):
    owners = lax.axis_size("dp")
    row_count = embeddings.shape[0]
    slot_count = 2 * row_count
    capacity = slot_count // owners
    cluster_count = centroids.shape[0]
    core = lax.axis_index("mp")
    squares = jnp.sum(embeddings * embeddings, axis=1)
    squares = squares + from_partner(squares)
    unit = (embeddings * lax.rsqrt(squares / D + 1e-06)[:, None]).astype(jnp.bfloat16)
    owner = cluster_id // cluster_count
    local = cluster_id - owner * cluster_count
    owner_hot = (owner[:, None] == jnp.arange(owners, dtype=jnp.int32)[None, :]).astype(jnp.bfloat16)
    row_index = jnp.arange(row_count, dtype=jnp.int32)
    lower = (row_index[:, None] >= row_index[None, :]).astype(jnp.bfloat16)
    running = jnp.dot(lower, owner_hot, preferred_element_type=jnp.float32)
    rank = jnp.sum(running * owner_hot.astype(jnp.float32), axis=1).astype(jnp.int32) - 1
    slot = owner * capacity + rank
    slot_index = jnp.arange(slot_count, dtype=jnp.int32)
    placed = slot_index[:, None] == slot[None, :]
    outgoing = jnp.dot(
        placed.astype(jnp.bfloat16), unit, preferred_element_type=jnp.float32
    ).astype(jnp.bfloat16)
    out_ids = jnp.max(jnp.where(placed, local[None, :] + 1, 0), axis=1) - 1
    incoming = lax.all_to_all(outgoing, "dp", split_axis=0, concat_axis=0, tiled=True)
    in_ids = lax.all_to_all(out_ids, "dp", split_axis=0, concat_axis=0, tiled=True)
    member = (jnp.arange(cluster_count, dtype=jnp.int32)[:, None] == in_ids[None, :]).astype(jnp.bfloat16)
    sums = jnp.dot(member, incoming, preferred_element_type=jnp.float32)
    counts = jnp.sum(member.astype(jnp.float32), axis=1)
    new_centroids = (cluster_mass[:, None] * centroids + sums) / (cluster_mass + counts)[:, None]
    half = slot_count // 2
    start = core * half
    contract = (((1,), (1,)), ((), ()))
    other = from_partner(incoming)
    scores = lax.dot_general(
        lax.dynamic_slice_in_dim(incoming, start, half, 0), incoming, contract, preferred_element_type=jnp.float32)
    scores = scores + lax.dot_general(
        lax.dynamic_slice_in_dim(other, start, half, 0), other, contract, preferred_element_type=jnp.float32)
    scores = scores / D
    query_ids = lax.dynamic_slice_in_dim(in_ids, start, half, 0)
    query_pos = start + jnp.arange(half, dtype=jnp.int32)
    same = (
        (query_ids[:, None] == in_ids[None, :])
        & (query_ids[:, None] >= 0)
        & (query_pos[:, None] != slot_index[None, :])
    )
    best = jnp.max(jnp.where(same, scores, -1.0), axis=1)
    best_p = from_partner(best)
    low, high = jnp.where(core == 0, best, best_p), jnp.where(core == 0, best_p, best)
    returned = lax.all_to_all(
        jnp.concatenate([low, high]), "dp", split_axis=0, concat_axis=0, tiled=True)
    return jnp.take(returned, slot), new_centroids


def shards(embeddings, cluster_id, centroids, cluster_mass):
    best, new_centroids, flag = compact(embeddings, cluster_id, centroids, cluster_mass)
    return lax.cond(
        flag[0, 0] > 0,
        lambda *args: general(*args),
        lambda *args: (best.reshape(ROWS), new_centroids),
        embeddings, cluster_id, centroids, cluster_mass,
    )


def solution(mesh):
    in_specs = (P("dp", "mp"), P("dp"), P("dp", "mp"), P("dp"))
    out_specs = (P("dp"), P("dp", "mp"))
    return jax.shard_map(shards, mesh=mesh, in_specs=in_specs, out_specs=out_specs, check_vma=False)
```

```python
import functools

import jax
import jax.numpy as jnp
from jax import lax
from jax.experimental import pallas as pl
from jax.experimental.pallas import tpu as pltpu
from jax.sharding import PartitionSpec as P

D = 1024
HALF = 512
ROWS = 768
CLUSTERS = 256
CAP = 12
ROOM = 128
NZ = 8
NXY = 16
GROUPS = (((0, 1, 7), 0, 40), ((2, 6), 40, 24))
LANE = {k: base + CAP * m for members, base, _ in GROUPS for m, k in enumerate(members)}
FAR = (3, 5, 4)
FAR_SETS = (((3, 5), 0, 24, 2731, 16), ((4,), 2, 16, 1, 4))
WIDTH = tuple(count * NXY for _, _, count in GROUPS)
MESH = pl.DeviceIdType.MESH
NT = (((1,), (1,)), ((), ()))
NEAR = (1, 7, 2, 6)
POS = {k: i for i, k in enumerate((0,) + NEAR + FAR)}


def neg(d):
    return ((4 - d // 4) % 4) * 4 + (4 - d % 4) % 4


def hot(mask):
    return jnp.where(mask, 1.0, 0.0).astype(jnp.bfloat16)


def exchange_kernel(
    emb_ref, cid_ref, cent_ref, mass_ref,
    best_ref, nc_ref, flag_ref,
    emb, unit, sq_mine, sq_peer, zout, zin, z_far, z_far_p, mout, min_, xo0, xo1, idout, fo0, fo1, fi0, fi1, fid_out, fid_in,
    r0, r1, p0, p1, idin, ik0, ik1, ik_far, top, idq, acc0, acc1, acc_far, top_far, sums,
    tiles_i, column, best_out, far_out, ret1, ret2, far_z, back_out, far_ret, cent, cid_v, mass_v,
    local_sem, sq_sem, zs, zr, ms, mr, xs, xr, ids_s, ids_r, ps, pr, bs, br, fs, fr,
    ws, wr, vs, vr, us, ur, ts, tr,
):
    xout, rows, rows_p, idkey = (xo0, xo1), (r0, r1), (p0, p1), (ik0, ik1)
    fout, fin, acc = (fo0, fo1), (fi0, fi1), (acc0, acc1)
    me = lax.axis_index("dp")
    c = lax.axis_index("mp")
    z, x, y = me // 16, (me // 4) % 4, me % 4

    def at_z(k):
        return (((z + k) % NZ) * 16 + x * 4 + y, c)

    def at_xy(d):
        return (z * 16 + ((x + d // 4) % 4) * 4 + (y + d % 4) % 4, c)

    partner = (me, 1 - c)

    def send(src, dst, send_sem, recv_sem, to):
        copy = pltpu.make_async_remote_copy(src, dst, send_sem, recv_sem, device_id=to, device_id_type=MESH)
        copy.start()
        return copy

    def sent(ref, sem):
        pltpu.make_async_remote_copy(ref, ref, sem, sem, device_id=partner, device_id_type=MESH).wait_send()

    def arrived(ref, sem):
        pltpu.make_async_remote_copy(ref, ref, sem, sem, device_id=partner, device_id_type=MESH).wait_recv()

    others = pl.ds(1, NXY - 1)

    cid_load = pltpu.make_async_copy(cid_ref, cid_v, local_sem.at[3])
    cid_load.start()
    mass_load = pltpu.make_async_copy(mass_ref, mass_v, local_sem.at[4])
    mass_load.start()
    load = pltpu.make_async_copy(emb_ref, emb, local_sem.at[0])
    load.start()
    cent_load = pltpu.make_async_copy(cent_ref, cent, local_sem.at[1])
    cent_load.start()
    barrier = pltpu.get_barrier_semaphore()
    for k in range(1, NZ):
        pl.semaphore_signal(barrier, inc=1, device_id=at_z(k), device_id_type=MESH)
    for d in range(1, NXY):
        pl.semaphore_signal(barrier, inc=1, device_id=at_xy(d), device_id_type=MESH)
        pl.semaphore_signal(barrier, inc=1, device_id=(at_xy(d)[0], 1 - c), device_id_type=MESH)
    for k in FAR:
        pl.semaphore_signal(barrier, inc=1, device_id=(at_z(k)[0], 1 - c), device_id_type=MESH)
    pl.semaphore_signal(barrier, inc=1, device_id=partner, device_id_type=MESH)

    cid_load.wait()
    cid = cid_v[...].reshape(1, ROWS)
    owner = cid >> 8
    dz = ((owner >> 4) - z) & 7
    dxy = ((((owner >> 2) & 3) - x) & 3) * 4 + (((owner & 3) - y) & 3)
    target = dz * 16 + dxy
    lane128 = lax.broadcasted_iota(jnp.int32, (128, 128), 1)
    sub128 = lax.broadcasted_iota(jnp.int32, (128, 128), 0)
    upto = hot(sub128 <= lane128)
    sub8 = lax.broadcasted_iota(jnp.int32, (8, 128), 0)
    sub16 = lax.broadcasted_iota(jnp.int32, (NXY, 128), 0)
    last = lax.broadcasted_iota(jnp.int32, (1, 128), 1) == 127
    base_t = jnp.zeros((128, 128), jnp.float32)
    base_z = jnp.zeros((8, 128), jnp.float32)
    ranks, places = [], []
    for b in range(ROWS // 128):
        cut = slice(128 * b, 128 * b + 128)
        is_t = sub128 == target[:, cut]
        is_z = sub8 == dz[:, cut]
        run_t = base_t + jnp.dot(hot(is_t), upto, preferred_element_type=jnp.float32)
        run_z = base_z + jnp.dot(hot(is_z), upto, preferred_element_type=jnp.float32)
        ranks.append(jnp.sum(jnp.where(is_t, run_t, 0.0), axis=0, keepdims=True) - 1.0)
        places.append(jnp.sum(jnp.where(is_z, run_z, 0.0), axis=0, keepdims=True) - 1.0)
        base_t = jnp.broadcast_to(run_t[:, 127:128], (128, 128))
        base_z = jnp.broadcast_to(run_z[:, 127:128], (8, 128))
    near_most = jnp.where((sub8 < 3) | (sub8 > 5), base_z, 0.0)
    over = jnp.where(jnp.max(near_most, axis=0, keepdims=True) > float(ROOM), 1.0, 0.0)
    rank_f = jnp.concatenate(ranks, axis=1)
    rank = rank_f.astype(jnp.int32)
    place = jnp.concatenate(places, axis=1).astype(jnp.int32)
    slot = jnp.where(place < ROOM, dz * ROOM + place, -1)
    far_row = (dz >= 3) & (dz <= 5)
    far_lane = jnp.where(dz == 3, rank, jnp.where(dz == 5, rank + CAP, rank + 2 * CAP))
    far_lane = jnp.where(far_row, far_lane, -1)
    far_slot = (
        jnp.where((dz == 3) | (dz == 5), dxy * FAR_SETS[0][2] + far_lane, -1),
        jnp.where(dz == 4, dxy * FAR_SETS[1][2] + rank, -1),
    )
    turned = ((4 - (dxy >> 2)) & 3) * 4 + ((4 - (dxy & 3)) & 3)
    tile_of = jnp.where(far_row, NZ * NXY + dxy, dz * NXY + turned)
    lane_of = jnp.where(far_row, far_lane, rank)
    for k in (0,) + NEAR:
        lane_of = jnp.where(dz == k, rank + LANE[(NZ - k) % NZ], lane_of)
    tiles_i[...] = jnp.zeros_like(tiles_i)
    for b in range(ROWS // 128):
        cut = slice(128 * b, 128 * b + 128)
        tiles_i[0, b:b + 1, :] = tile_of[:, cut]
        tiles_i[1, b:b + 1, :] = lane_of[:, cut]
    row8 = lax.broadcasted_iota(jnp.int32, (8, ROWS), 0)
    local = ((cid & 255) + 1).astype(jnp.float32)
    values = jnp.where(
        row8 == 0, local,
        jnp.where(row8 == 1, dxy.astype(jnp.float32), jnp.where(row8 == 2, rank_f, 0.0)),
    ).astype(jnp.bfloat16)

    load.wait()
    squares = jnp.zeros((ROWS, 128), jnp.float32)
    for f in range(HALF // 128):
        part = emb[:, 128 * f:128 * f + 128]
        squares = squares + part * part
    mine = jnp.sum(squares.T, axis=0, keepdims=True)
    sq_mine[...] = mine
    pl.semaphore_wait(barrier, NZ - 1 + 2 * (NXY - 1) + len(FAR) + 1)
    sq_copy = send(sq_mine, sq_peer, sq_sem.at[0], sq_sem.at[1], partner)

    place_hot = {}
    for k in (0,) + NEAR:
        want = lax.broadcasted_iota(jnp.int32, (ROOM, ROWS), 0) + k * ROOM
        place_hot[k] = hot(want == slot)
    far_hot = [
        hot(lax.broadcasted_iota(jnp.int32, (NXY * count, ROWS), 0) == far_slot[e])
        for e, (_, _, count, _, _) in enumerate(FAR_SETS)
    ]

    sq_copy.wait()
    scale = lax.rsqrt((sq_mine[...] + sq_peer[...]) / D + 1e-06)
    scale = jnp.broadcast_to(scale, (128, ROWS)).T
    for f in range(HALF // 128):
        unit[:, 128 * f:128 * f + 128] = (emb[:, 128 * f:128 * f + 128] * scale).astype(jnp.bfloat16)

    def pack(k):
        packed = jnp.dot(place_hot[k], unit[...], preferred_element_type=jnp.float32).astype(jnp.bfloat16)
        if k == 0:
            zin[0] = packed
        else:
            zout[POS[k]] = packed
            send(zout.at[POS[k]], zin.at[POS[NZ - k]], zs.at[0], zr.at[0 if k in (1, 7) else 1], at_z(k))

    pack(1)
    pack(7)
    left = jnp.where(
        far_row & (lax.broadcasted_iota(jnp.int32, (NXY, ROWS), 0) == dxy), local, 0.0).astype(jnp.bfloat16)
    right = hot(lax.broadcasted_iota(jnp.int32, (128, ROWS), 0) == far_lane)
    ids = lax.dot_general(left, right, NT, preferred_element_type=jnp.float32)
    for d in range(NXY):
        if d == 0:
            fid_in[0] = ids[0:1, :]
        else:
            fid_out[d] = ids[d:d + 1, :]
            send(fid_out.at[d], fid_in.at[neg(d)], vs.at[0], vr.at[0], at_xy(d))

    def pack_far(e):
        count = FAR_SETS[e][2]
        packed = jnp.dot(far_hot[e], unit[...], preferred_element_type=jnp.float32)
        for d in range(NXY):
            block = packed[count * d:count * d + count, :].astype(jnp.bfloat16)
            if d == 0:
                fin[e][0] = block
            else:
                fout[e][d] = block
                send(fout[e].at[d], fin[e].at[neg(d)], ws.at[e], wr.at[e], at_xy(d))

    pack_far(0)
    pack_far(1)
    for k in NEAR + (0,):
        meta = lax.dot_general(values, place_hot[k], NT, preferred_element_type=jnp.float32)
        if k == 0:
            min_[0] = meta
        else:
            mout[POS[k]] = meta
            send(mout.at[POS[k]], min_.at[POS[NZ - k]], ms.at[0], mr.at[0 if k in (1, 7) else 1], at_z(k))
    pack(2)
    pack(6)
    pack(0)

    p_copies = {}

    def forward(g):
        members, _, count = GROUPS[g]
        total = None
        if g == 0:
            arrived(min_.at[pl.ds(1, 2)], mr.at[0])
        for m, k in enumerate(members):
            meta = min_[POS[k]]
            valid = meta[0:1, :] > 0.5
            there = jnp.where(valid, meta[1:2, :] * float(count) + meta[2:3, :] + float(CAP * m), -1.0)
            there = there.astype(jnp.int32)
            want = lax.broadcasted_iota(jnp.int32, (NXY * count, ROOM), 0)
            if m == g ^ 1:
                arrived(zin.at[pl.ds(1 + 2 * g, 2)], zr.at[g])
            part = jnp.dot(hot(want == there), zin[POS[k]], preferred_element_type=jnp.float32)
            total = part if total is None else total + part
        for d in range(NXY):
            block = total[count * d:count * d + count, :].astype(jnp.bfloat16)
            if d == 0:
                rows[g][0] = block
            else:
                xout[g][d] = block
                send(xout[g].at[d], rows[g].at[neg(d)], xs.at[g], xr.at[g], at_xy(d))

    def share(g):
        arrived(rows[g].at[others], xr.at[g])
        p_copies[g] = send(rows[g], rows_p[g], ps.at[g], pr.at[g], partner)

    def share_far(kk):
        arrived(z_far.at[kk], zr.at[2 + kk])
        p_copies[2 + kk] = send(z_far.at[kk], z_far_p.at[kk], ps.at[2 + kk], pr.at[2 + kk], partner)

    arrived(fid_in.at[others], vr.at[0])
    known = jnp.concatenate([fid_in[j] for j in range(NXY)], axis=0).astype(jnp.bfloat16)
    back_at = jnp.zeros((NXY, 128), jnp.float32)
    far_values, far_places = [], []
    for planes, first, count, factor, shift in FAR_SETS:
        width = NXY * count
        flat = lax.broadcasted_iota(jnp.int32, (1, width), 1)
        holder = (flat * factor) >> shift
        within = flat - holder * count
        lane = jnp.where(within < CAP * len(planes), within + CAP * first, -1)
        spread = hot(lax.broadcasted_iota(jnp.int32, (128, width), 0) == lane)
        mine16 = lax.broadcasted_iota(jnp.int32, (NXY, width), 0) == holder
        far_ids = jnp.dot(known, spread, preferred_element_type=jnp.float32)
        far_ids = jnp.sum(jnp.where(mine16, far_ids, 0.0), axis=0, keepdims=True)
        low = lax.broadcasted_iota(jnp.int32, (8, width), 0) * CAP
        inside = (within >= low) & (within < low + CAP) & (low < CAP * len(planes)) & (far_ids > 0.5)
        base_f = jnp.zeros((8, 128), jnp.float32)
        runs = []
        for b in range(width // 128):
            run = base_f + jnp.dot(hot(inside[:, 128 * b:128 * b + 128]), upto, preferred_element_type=jnp.float32)
            runs.append(run)
            base_f = jnp.broadcast_to(run[:, 127:128], (8, 128))
        over = jnp.maximum(over, jnp.where(jnp.max(base_f, axis=0, keepdims=True) > float(ROOM), 1.0, 0.0))
        far_place = jnp.where(inside, jnp.concatenate(runs, axis=1) - 1.0, -1.0)
        far_place = jnp.where(far_place < float(ROOM), far_place, -1.0)
        any_place = jnp.maximum(jnp.max(far_place, axis=0, keepdims=True), 0.0)
        back_at = back_at + lax.dot_general(
            jnp.where(mine16, any_place, 0.0).astype(jnp.bfloat16), spread, NT, preferred_element_type=jnp.float32)
        far_values.append(jnp.broadcast_to(far_ids, (8, width)).astype(jnp.bfloat16))
        far_places.append(far_place)
    back_at = back_at.astype(jnp.int32)

    def relay_far(e):
        planes, _, count, _, _ = FAR_SETS[e]
        width = NXY * count
        chosen = []
        for m, k in enumerate(planes):
            want = lax.broadcasted_iota(jnp.int32, (ROOM, width), 0).astype(jnp.float32)
            chosen.append(hot(want == far_places[e][m:m + 1, :]))
            mout[POS[k]] = lax.dot_general(far_values[e], chosen[m], NT, preferred_element_type=jnp.float32)
            there = FAR.index(NZ - k)
            send(mout.at[POS[k]], min_.at[POS[NZ - k]], ms.at[0], mr.at[2 + there], at_z(k))
        arrived(fin[e].at[others], wr.at[e])
        for m, k in enumerate(planes):
            zout[POS[k]] = jnp.dot(
                chosen[m], fin[e][...].reshape(width, HALF), preferred_element_type=jnp.float32).astype(jnp.bfloat16)
            there = FAR.index(NZ - k)
            send(zout.at[POS[k]], z_far.at[there], zs.at[0], zr.at[2 + there], at_z(k))

    forward(0)
    relay_far(0)

    arrived(min_.at[pl.ds(3, 2)], mr.at[1])
    ids = jnp.zeros((NXY, 128), jnp.float32)
    for k in (0,) + NEAR:
        meta = min_[POS[k]]
        valid = meta[0:1, :] > 0.5
        to = jnp.where(valid, meta[1:2, :], -1.0).astype(jnp.int32)
        place_k = meta[2:3, :].astype(jnp.int32) + LANE[k]
        left = jnp.where(sub16 == to, meta[0:1, :], 0.0).astype(jnp.bfloat16)
        ids = ids + lax.dot_general(left, hot(sub128 == place_k), NT, preferred_element_type=jnp.float32)
    for d in range(NXY):
        if d == 0:
            idin[0] = ids[0:1, :]
        else:
            idout[d] = ids[d:d + 1, :]
            send(idout.at[d], idin.at[neg(d)], ids_s.at[0], ids_r.at[0], at_xy(d))

    forward(1)
    relay_far(1)

    share(0)
    arrived(idin.at[others], ids_r.at[0])
    for j in range(NXY):
        line = idin[j]
        line = jnp.where(line < 0.5, -1.0, line)
        turned = jnp.broadcast_to(line, (128, 128)).T
        for g, (_, base, count) in enumerate(GROUPS):
            idkey[g][count * j:count * j + count, :] = turned[base:base + count, :]

    for g in range(2):
        half = WIDTH[g] // 2
        for h in range(-(-half // 128)):
            size = min(128, half - 128 * h)
            block = idkey[g][pl.ds(pl.multiple_of(half * c + 128 * h, 8), size), :]
            idq[g, :, 128 * h:128 * h + size] = block.T[0:8, :]
    for ref in (top, top_far, acc0, acc1, acc_far):
        ref[...] = jnp.full(ref.shape, -float(D), jnp.float32)
    sub256 = lax.broadcasted_iota(jnp.int32, (CLUSTERS, 128), 0).astype(jnp.float32) + 1.0

    def member_sums(source, key):
        seen = jnp.zeros((CLUSTERS, 128), jnp.float32)
        parts = []
        for h in range(key.shape[0] // 128):
            line = source[128 * h:128 * h + 128, :].T[0:1, :]
            member = jnp.where(sub256 == line, 1.0, 0.0)
            seen = seen + member
            parts.append(member.astype(jnp.bfloat16))
        member = jnp.concatenate(parts, axis=1) if len(parts) > 1 else parts[0]
        return seen, jnp.dot(member, key, preferred_element_type=jnp.float32)

    def near_sums(g):
        return member_sums(idkey[g], rows[g][...].reshape(WIDTH[g], HALF))

    def keys_of(g):
        return rows[g][...].reshape(WIDTH[g], HALF), rows_p[g][...].reshape(WIDTH[g], HALF)

    def own_half(g):
        half = WIDTH[g] // 2
        first = pl.ds(pl.multiple_of(NXY // 2 * c, 8), NXY // 2)
        return rows[g][first].reshape(half, HALF), rows_p[g][first].reshape(half, HALF)

    def nt(a, b):
        return lax.dot_general(a, b, NT, preferred_element_type=jnp.float32)

    def score_near(e):
        pairs = [(e, e)] + [pair for g in range(e) for pair in ((g, e), (e, g))]
        own = [nt(keys_of(kg)[0], own_half(qg)[0]) for kg, qg in pairs]
        p_copies[e].wait_recv()
        for (kg, qg), part in zip(pairs, own):
            nk, nq = WIDTH[kg], WIDTH[qg] // 2
            scores = part + nt(keys_of(kg)[1], own_half(qg)[1])
            for h in range(-(-nq // 128)):
                cut = slice(128 * h, min(128 * h + 128, nq))
                size = cut.stop - cut.start
                same = idkey[kg][...][:, :size] == idq[qg, 0:1, cut]
                if kg == qg:
                    apart = (lax.broadcasted_iota(jnp.int32, (nk, size), 0)
                             - lax.broadcasted_iota(jnp.int32, (nk, size), 1))
                    same = same & (apart != nq * c + 128 * h)
                kept = jnp.where(same, scores[:, cut], -float(D))
                top[qg, :, cut] = jnp.maximum(top[qg, :, cut], jnp.max(kept.reshape(nk // 8, 8, size), axis=0))

    half_far = pl.ds(pl.multiple_of(ROOM // 2 * c, ROOM // 2), ROOM // 2)

    def score_far(planes):
        first, width = planes[0], ROOM * len(planes)
        cut = slice(first, first + len(planes))
        groups = [0, 1] + [2 + kk for kk in range(first + len(planes))]

        def side(g):
            if g < 2:
                return own_half(g)
            return z_far[g - 2, half_far, :], z_far_p[g - 2, half_far, :]

        columns = z_far[cut].reshape(width, HALF)
        own = [nt(side(g)[0], columns) for g in groups]
        for kk in planes:
            p_copies[2 + kk].wait_recv()
        columns = z_far_p[cut].reshape(width, HALF)
        for g, part in zip(groups, own):
            scores = part + nt(side(g)[1], columns)
            n = scores.shape[0]
            if g < 2:
                mine = idkey[g][pl.ds(pl.multiple_of(n * c, 8), n), :]
            else:
                mine = ik_far[g - 2, half_far, :]
            for kk in planes:
                line = min_[POS[FAR[kk]]][0:1, :]
                same = mine == line
                if g == 2 + kk:
                    apart = (lax.broadcasted_iota(jnp.int32, (n, ROOM), 1)
                             - lax.broadcasted_iota(jnp.int32, (n, ROOM), 0))
                    same = same & (apart != n * c)
                kept = jnp.where(same, scores[:, ROOM * (kk - first):ROOM * (kk - first) + ROOM], -float(D))
                top_far[kk] = jnp.maximum(top_far[kk], jnp.max(kept.reshape(n // 8, 8, ROOM), axis=0))
                if g < 2:
                    acc[g][...] = jnp.maximum(acc[g][...], kept)
                elif g - 2 < first:
                    acc_far[g - 2] = jnp.maximum(acc_far[g - 2], kept)

    def take_far(kk):
        arrived(min_.at[POS[FAR[kk]]], mr.at[2 + kk])
        line = min_[POS[FAR[kk]]][0:1, :]
        ik_far[kk] = jnp.broadcast_to(jnp.where(line < 0.5, -1.0, line), (128, 128)).T
        share_far(kk)

    counts, total = near_sums(0)
    sums[...] = total
    score_near(0)
    share(1)
    take_far(0)
    take_far(1)
    more, total = near_sums(1)
    counts = counts + more
    sums[...] += total
    score_near(1)
    score_far((0, 1))
    take_far(2)
    score_far((2,))
    for g, (_, base, count) in enumerate(GROUPS):
        half = WIDTH[g] // 2
        pieces = []
        for h in range(-(-half // 128)):
            size = min(128, half - 128 * h)
            best = jnp.max(top[g, :, 128 * h:128 * h + size], axis=0, keepdims=True)
            pieces.append(jnp.broadcast_to(best, (128, size)).T)
        best = jnp.concatenate(pieces, axis=0)
        best = jnp.maximum(best, jnp.max(acc[g][...], axis=1, keepdims=True)) * (1.0 / D)
        for i in range(NXY // 2):
            column[i, base:base + count, :] = best[count * i:count * i + count, :]
    for kk in range(3):
        best = jnp.max(top_far[kk], axis=0, keepdims=True)
        if kk < 2:
            mine = jnp.broadcast_to(jnp.max(acc_far[kk], axis=1, keepdims=True), (ROOM // 2, 128))
            mine = jnp.concatenate([jnp.where(c == h, mine, -float(D)) for h in range(2)], axis=0)
            best = jnp.maximum(best, mine.T[0:1, :])
        far_out[kk, :, 0:128] = best * (1.0 / D)
        far_out[kk, :, 128:256] = over
    for kk, k in enumerate(FAR):
        there = FAR.index(NZ - k)
        for core in range(2):
            send(far_out.at[kk], far_z.at[c, there], us.at[core], ur.at[0], (at_z(k)[0], core))
    for i in range(NXY // 2):
        best_out[i] = jnp.where(last, over, column[i].T[0:1, :])

    def best_copy(i, other):
        jx, jy = 2 * c + i // 4, i % 4
        there = (z * 16 + ((x + jx) % 4) * 4 + (y + jy) % 4, 1 - c if other else c)
        return pltpu.make_async_remote_copy(
            best_out.at[i], ret1.at[8 * c + i], bs.at[int(other)], br.at[0],
            device_id=there, device_id_type=MESH)

    @pl.when(c == 0)
    def _():
        ret1[0] = best_out[0]

    @pl.when(c == 1)
    def _():
        best_copy(0, False).start()

    best_copy(0, True).start()
    for i in range(1, 8):
        best_copy(i, False).start()
        best_copy(i, True).start()

    for kk in range(3):
        more, part = member_sums(ik_far[kk], z_far[kk])
        counts = counts + more
        total = part if kk == 0 else total + part
    cent_load.wait()
    mass_load.wait()
    number = jnp.sum(counts, axis=1, keepdims=True)
    mass = jnp.broadcast_to(mass_v[...], (128, CLUSTERS)).T[:, 0:1]
    cent[...] = (mass * cent[...] + (sums[...] + total)) / (mass + number)
    nc_copy = pltpu.make_async_copy(cent, nc_ref, local_sem.at[2])
    nc_copy.start()

    @pl.when(c == 0)
    def _():
        arrived(ret1.at[others], br.at[0])

    @pl.when(c == 1)
    def _():
        arrived(ret1, br.at[0])

    back = {}
    for k in (2, 6, 1, 7):
        back[NZ - k] = send(
            ret1, ret2.at[POS[NZ - k] - 1], fs.at[POS[k] - 1], fr.at[POS[NZ - k] - 1], at_z(k))
    arrived(far_z, ur.at[0])
    lane16 = lax.broadcasted_iota(jnp.int32, (NXY, 128), 1)
    got = jnp.zeros((NXY, 128), jnp.float32)
    for kk in range(3):
        line = jnp.maximum(far_z[0, kk][:, 0:128], far_z[1, kk][:, 0:128])
        line = jnp.broadcast_to(line, (8, 128))
        found = jnp.concatenate(
            [jnp.take_along_axis(line, back_at[8 * h:8 * h + 8, :], axis=1, mode="promise_in_bounds") for h in range(2)],
            axis=0)
        got = jnp.where(lane16 >= kk * CAP, found, got)
    far_over = far_z[0, 0][:, 128:256]
    for h in range(2):
        for kk in range(3):
            far_over = jnp.maximum(far_over, far_z[h, kk][:, 128:256])
    got = jnp.where(lane16 == 127, far_over, got)
    for j in range(NXY):
        if j == 0:
            far_ret[0] = got[0:1, :]
        else:
            back_out[j] = got[j:j + 1, :]
            send(back_out.at[j], far_ret.at[neg(j)], ts.at[0], tr.at[0], at_xy(j))
    tile_t = tiles_i[0]
    lane_t = tiles_i[1]
    result = jnp.zeros((8, 128), jnp.float32)
    flag = jnp.zeros((1, 128), jnp.float32)

    def pick(line, tile, result, flag):
        got = jnp.take_along_axis(jnp.broadcast_to(line, (8, 128)), lane_t, axis=1, mode="promise_in_bounds")
        return jnp.where(tile_t == tile, got, result), jnp.maximum(flag, jnp.where(last, line, 0.0))

    for j in range(NXY):
        result, flag = pick(ret1[j], j, result, flag)
    for k in NEAR:
        back[k].wait_recv()
        for j in range(NXY):
            result, flag = pick(ret2[POS[k] - 1, j], k * NXY + j, result, flag)
    arrived(far_ret.at[others], tr.at[0])
    for d in range(NXY):
        result, flag = pick(far_ret[d], NZ * NXY + d, result, flag)
    for b in range(ROWS // 128):
        best_ref[:, 128 * b:128 * b + 128] = result[b:b + 1, :]
    flag_ref[0, 0] = jnp.max(flag).astype(jnp.int32)

    @pl.when(c == 0)
    def _():
        sent(best_out.at[pl.ds(1, 7)], bs.at[0])

    @pl.when(c == 1)
    def _():
        sent(best_out, bs.at[0])

    sent(best_out, bs.at[1])
    for copy in list(back.values()) + list(p_copies.values()):
        copy.wait_send()
    sent(zout.at[pl.ds(1, NZ - 1)], zs.at[0])
    sent(mout.at[pl.ds(1, NZ - 1)], ms.at[0])
    for e in range(2):
        sent(xout[e].at[others], xs.at[e])
        sent(fout[e].at[others], ws.at[e])
        sent(far_out, us.at[e])
    sent(fid_out.at[others], vs.at[0])
    sent(idout.at[others], ids_s.at[0])
    sent(back_out.at[others], ts.at[0])
    nc_copy.wait()


def compact(embeddings, cluster_id, centroids, cluster_mass):
    vmem = pl.BlockSpec(memory_space=pltpu.VMEM)
    anywhere = pl.BlockSpec(memory_space=pl.ANY)
    f32, bf16, i32 = jnp.float32, jnp.bfloat16, jnp.int32
    dma = pltpu.SemaphoreType.DMA
    line = (1, 128)
    return pl.pallas_call(
        exchange_kernel,
        out_shape=(
            jax.ShapeDtypeStruct((1, ROWS), f32),
            jax.ShapeDtypeStruct((CLUSTERS, HALF), f32),
            jax.ShapeDtypeStruct((1, 1), i32),
        ),
        in_specs=[anywhere, anywhere, anywhere, anywhere],
        out_specs=(vmem, anywhere, pl.BlockSpec(memory_space=pltpu.SMEM)),
        scratch_shapes=[
            pltpu.VMEM((ROWS, HALF), f32),
            pltpu.VMEM((ROWS, HALF), bf16),
            pltpu.VMEM((1, ROWS), f32),
            pltpu.VMEM((1, ROWS), f32),
            pltpu.VMEM((NZ, ROOM, HALF), bf16),
            pltpu.VMEM((1 + len(NEAR), ROOM, HALF), bf16),
            pltpu.VMEM((3, ROOM, HALF), bf16),
            pltpu.VMEM((3, ROOM, HALF), bf16),
            pltpu.VMEM((NZ, 8, 128), f32),
            pltpu.VMEM((NZ, 8, 128), f32),
            *[pltpu.VMEM((NXY, count, HALF), bf16) for _, _, count in GROUPS],
            pltpu.VMEM((NXY, *line), f32),
            *[pltpu.VMEM((NXY, far[2], HALF), bf16) for far in FAR_SETS],
            *[pltpu.VMEM((NXY, far[2], HALF), bf16) for far in FAR_SETS],
            pltpu.VMEM((NXY, *line), f32),
            pltpu.VMEM((NXY, *line), f32),
            *[pltpu.VMEM((NXY, count, HALF), bf16) for _, _, count in GROUPS],
            *[pltpu.VMEM((NXY, count, HALF), bf16) for _, _, count in GROUPS],
            pltpu.VMEM((NXY, *line), f32),
            *[pltpu.VMEM((NXY * count, 128), f32) for _, _, count in GROUPS],
            pltpu.VMEM((3, 128, 128), f32),
            pltpu.VMEM((2, 8, 384), f32),
            pltpu.VMEM((2, 8, 384), f32),
            *[pltpu.VMEM((width // 2, 128), f32) for width in WIDTH],
            pltpu.VMEM((2, ROOM // 2, 128), f32),
            pltpu.VMEM((3, 8, 128), f32),
            pltpu.VMEM((CLUSTERS, HALF), f32),
            pltpu.VMEM((2, 8, 128), i32),
            pltpu.VMEM((8, 128, 128), f32),
            pltpu.VMEM((8, *line), f32),
            pltpu.VMEM((3, 1, 256), f32),
            pltpu.VMEM((NXY, *line), f32),
            pltpu.VMEM((len(NEAR), NXY, *line), f32),
            pltpu.VMEM((2, 3, 1, 256), f32),
            pltpu.VMEM((NXY, *line), f32),
            pltpu.VMEM((NXY, *line), f32),
            pltpu.VMEM((CLUSTERS, HALF), f32),
            pltpu.VMEM((ROWS,), i32),
            pltpu.VMEM((1, CLUSTERS), f32),
            dma((5,)), dma((2,)), dma((1,)), dma((5,)), dma((1,)), dma((5,)), dma((2,)), dma((2,)),
            dma((1,)), dma((1,)), dma((5,)), dma((5,)), dma((2,)), dma((1,)), dma((4,)), dma((4,)),
            dma((2,)), dma((2,)), dma((1,)), dma((1,)), dma((2,)), dma((1,)), dma((1,)), dma((1,)),
        ],
        compiler_params=pltpu.CompilerParams(
            collective_id=0, has_side_effects=True, vmem_limit_bytes=48 * 2**20),
    )(embeddings, cluster_id, centroids, cluster_mass.reshape(1, CLUSTERS))


def from_partner(value):
    return lax.ppermute(value, "mp", [(0, 1), (1, 0)])


def general(embeddings, cluster_id, centroids, cluster_mass):
    owners = lax.axis_size("dp")
    row_count = embeddings.shape[0]
    slot_count = 2 * row_count
    capacity = slot_count // owners
    cluster_count = centroids.shape[0]
    core = lax.axis_index("mp")
    squares = jnp.sum(embeddings * embeddings, axis=1)
    squares = squares + from_partner(squares)
    unit = (embeddings * lax.rsqrt(squares / D + 1e-06)[:, None]).astype(jnp.bfloat16)
    owner = cluster_id // cluster_count
    local = cluster_id - owner * cluster_count
    owner_hot = (owner[:, None] == jnp.arange(owners, dtype=jnp.int32)[None, :]).astype(jnp.bfloat16)
    row_index = jnp.arange(row_count, dtype=jnp.int32)
    lower = (row_index[:, None] >= row_index[None, :]).astype(jnp.bfloat16)
    running = jnp.dot(lower, owner_hot, preferred_element_type=jnp.float32)
    rank = jnp.sum(running * owner_hot.astype(jnp.float32), axis=1).astype(jnp.int32) - 1
    slot = owner * capacity + rank
    slot_index = jnp.arange(slot_count, dtype=jnp.int32)
    placed = slot_index[:, None] == slot[None, :]
    outgoing = jnp.dot(
        placed.astype(jnp.bfloat16), unit, preferred_element_type=jnp.float32
    ).astype(jnp.bfloat16)
    out_ids = jnp.max(jnp.where(placed, local[None, :] + 1, 0), axis=1) - 1
    incoming = lax.all_to_all(outgoing, "dp", split_axis=0, concat_axis=0, tiled=True)
    in_ids = lax.all_to_all(out_ids, "dp", split_axis=0, concat_axis=0, tiled=True)
    member = (jnp.arange(cluster_count, dtype=jnp.int32)[:, None] == in_ids[None, :]).astype(jnp.bfloat16)
    sums = jnp.dot(member, incoming, preferred_element_type=jnp.float32)
    counts = jnp.sum(member.astype(jnp.float32), axis=1)
    new_centroids = (cluster_mass[:, None] * centroids + sums) / (cluster_mass + counts)[:, None]
    half = slot_count // 2
    start = core * half
    contract = (((1,), (1,)), ((), ()))
    other = from_partner(incoming)
    scores = lax.dot_general(
        lax.dynamic_slice_in_dim(incoming, start, half, 0), incoming, contract, preferred_element_type=jnp.float32)
    scores = scores + lax.dot_general(
        lax.dynamic_slice_in_dim(other, start, half, 0), other, contract, preferred_element_type=jnp.float32)
    scores = scores / D
    query_ids = lax.dynamic_slice_in_dim(in_ids, start, half, 0)
    query_pos = start + jnp.arange(half, dtype=jnp.int32)
    same = (
        (query_ids[:, None] == in_ids[None, :])
        & (query_ids[:, None] >= 0)
        & (query_pos[:, None] != slot_index[None, :])
    )
    best = jnp.max(jnp.where(same, scores, -1.0), axis=1)
    best_p = from_partner(best)
    low, high = jnp.where(core == 0, best, best_p), jnp.where(core == 0, best_p, best)
    returned = lax.all_to_all(
        jnp.concatenate([low, high]), "dp", split_axis=0, concat_axis=0, tiled=True)
    return jnp.take(returned, slot), new_centroids


def shards(embeddings, cluster_id, centroids, cluster_mass):
    best, new_centroids, flag = compact(embeddings, cluster_id, centroids, cluster_mass)
    return lax.cond(
        flag[0, 0] > 0,
        lambda *args: general(*args),
        lambda *args: (best.reshape(ROWS), new_centroids),
        embeddings, cluster_id, centroids, cluster_mass,
    )


def solution(mesh):
    in_specs = (P("dp", "mp"), P("dp"), P("dp", "mp"), P("dp"))
    out_specs = (P("dp"), P("dp", "mp"))
    return jax.shard_map(shards, mesh=mesh, in_specs=in_specs, out_specs=out_specs, check_vma=False)
```

```python
import functools

import jax
import jax.numpy as jnp
from jax import lax
from jax.experimental import pallas as pl
from jax.experimental.pallas import tpu as pltpu
from jax.sharding import PartitionSpec as P

D = 1024
HALF = 512
ROWS = 768
CLUSTERS = 256
CAP = 12
ROOM = 128
NZ = 8
NXY = 16
GROUPS = (((1, 7), 0, 24), ((2, 6), 24, 24), ((None, 0), 48, 24))
LANE = {k: base + CAP * m for members, base, _ in GROUPS for m, k in enumerate(members) if k is not None}
OWN = 2
FAR = (3, 5, 4)
FAR_SETS = (((3, 5), 0, 24), ((4,), 2, 24))
WIDTH = tuple(count * NXY for _, _, count in GROUPS)
MESH = pl.DeviceIdType.MESH
NT = (((1,), (1,)), ((), ()))
NEAR = (1, 7, 2, 6)
AROUND = (10, 9, 11, 6, 14, 2, 8, 5, 7, 13, 15, 1, 3, 4, 12, 0)
POS = {k: i for i, k in enumerate(NEAR + FAR)}


def neg(d):
    return ((4 - d // 4) % 4) * 4 + (4 - d % 4) % 4


def hot(mask):
    return jnp.where(mask, 1.0, 0.0).astype(jnp.bfloat16)


def exchange_kernel(
    emb_ref, cid_ref, cent_ref, mass_ref,
    best_ref, nc_ref, flag_ref,
    emb, unit, sq_mine, sq_peer, zout, zin, z_far, z_far_p, mout, min_, xo0, xo1, idout, fo0, fo1, fi0, fi1, fi1_p, fid_out, fid_in,
    r0, r1, p0, p1, idin, ik0, ik1, ik2, ik_far, top, idq, acc0, acc1, acc2, acc_far, top_far, sums,
    tiles_i, column, best_out, far_out, ret1, ret2, far_z, back_out, far_ret, cent, cid_v, mass_v,
    local_sem, sq_sem, zs, zr, ms, mr, xs, xr, ids_s, ids_r, ps, pr, bs, br, fs, fr,
    ws, wr, vs, vr, us, ur, ts, tr,
):
    xout, rows, rows_p, idkey = (xo0, xo1), (r0, r1, fi1), (p0, p1, fi1_p), (ik0, ik1, ik2)
    fout, fin, acc = (fo0, fo1), (fi0, fi1), (acc0, acc1, acc2)
    me = lax.axis_index("dp")
    c = lax.axis_index("mp")
    z, x, y = me // 16, (me // 4) % 4, me % 4

    def at_z(k):
        return (((z + k) % NZ) * 16 + x * 4 + y, c)

    def at_xy(d):
        return (z * 16 + ((x + d // 4) % 4) * 4 + (y + d % 4) % 4, c)

    partner = (me, 1 - c)

    def send(src, dst, send_sem, recv_sem, to):
        copy = pltpu.make_async_remote_copy(src, dst, send_sem, recv_sem, device_id=to, device_id_type=MESH)
        copy.start()
        return copy

    def sent(ref, sem):
        pltpu.make_async_remote_copy(ref, ref, sem, sem, device_id=partner, device_id_type=MESH).wait_send()

    def arrived(ref, sem):
        pltpu.make_async_remote_copy(ref, ref, sem, sem, device_id=partner, device_id_type=MESH).wait_recv()

    others = pl.ds(1, NXY - 1)

    cid_load = pltpu.make_async_copy(cid_ref, cid_v, local_sem.at[3])
    cid_load.start()
    mass_load = pltpu.make_async_copy(mass_ref, mass_v, local_sem.at[4])
    mass_load.start()
    load = pltpu.make_async_copy(emb_ref, emb, local_sem.at[0])
    load.start()
    cent_load = pltpu.make_async_copy(cent_ref, cent, local_sem.at[1])
    cent_load.start()
    barrier = pltpu.get_barrier_semaphore()
    for k in FAR[::-1]:
        pl.semaphore_signal(barrier, inc=1, device_id=at_z(k), device_id_type=MESH)
        pl.semaphore_signal(barrier, inc=1, device_id=(at_z(k)[0], 1 - c), device_id_type=MESH)
    for d in AROUND[:-1]:
        pl.semaphore_signal(barrier, inc=1, device_id=at_xy(d), device_id_type=MESH)
        pl.semaphore_signal(barrier, inc=1, device_id=(at_xy(d)[0], 1 - c), device_id_type=MESH)
    for k in NEAR:
        pl.semaphore_signal(barrier, inc=1, device_id=at_z(k), device_id_type=MESH)
    pl.semaphore_signal(barrier, inc=1, device_id=partner, device_id_type=MESH)

    cid_load.wait()
    cid = cid_v[...].reshape(1, ROWS)
    owner = cid >> 8
    dz = ((owner >> 4) - z) & 7
    dxy = ((((owner >> 2) & 3) - x) & 3) * 4 + (((owner & 3) - y) & 3)
    target = dz * 16 + dxy
    lane128 = lax.broadcasted_iota(jnp.int32, (128, 128), 1)
    sub128 = lax.broadcasted_iota(jnp.int32, (128, 128), 0)
    upto = hot(sub128 <= lane128)
    sub8 = lax.broadcasted_iota(jnp.int32, (8, 128), 0)
    sub16 = lax.broadcasted_iota(jnp.int32, (NXY, 128), 0)
    last = lax.broadcasted_iota(jnp.int32, (1, 128), 1) == 127
    base_t = jnp.zeros((128, 128), jnp.float32)
    base_z = jnp.zeros((8, 128), jnp.float32)
    ranks, places = [], []
    for b in range(ROWS // 128):
        cut = slice(128 * b, 128 * b + 128)
        is_t = sub128 == target[:, cut]
        is_z = sub8 == dz[:, cut]
        run_t = base_t + jnp.dot(hot(is_t), upto, preferred_element_type=jnp.float32)
        run_z = base_z + jnp.dot(hot(is_z), upto, preferred_element_type=jnp.float32)
        ranks.append(jnp.sum(jnp.where(is_t, run_t, 0.0), axis=0, keepdims=True) - 1.0)
        places.append(jnp.sum(jnp.where(is_z, run_z, 0.0), axis=0, keepdims=True) - 1.0)
        base_t = jnp.broadcast_to(run_t[:, 127:128], (128, 128))
        base_z = jnp.broadcast_to(run_z[:, 127:128], (8, 128))
    near_most = jnp.where((sub8 == 1) | (sub8 == 2) | (sub8 > 5), base_z, 0.0)
    over = jnp.where(jnp.max(near_most, axis=0, keepdims=True) > float(ROOM), 1.0, 0.0)
    rank_f = jnp.concatenate(ranks, axis=1)
    rank = rank_f.astype(jnp.int32)
    place = jnp.concatenate(places, axis=1).astype(jnp.int32)
    slot = jnp.where(place < ROOM, dz * ROOM + place, -1)
    far_row = (dz >= 3) & (dz <= 5)
    far_lane = jnp.where(dz == 3, rank, jnp.where(dz == 5, rank + CAP, rank + 2 * CAP))
    far_lane = jnp.where(far_row, far_lane, jnp.where(dz == 0, rank + 3 * CAP, -1))
    far_slot = (
        jnp.where((dz == 3) | (dz == 5), dxy * FAR_SETS[0][2] + far_lane, -1),
        jnp.where((dz == 4) | (dz == 0), dxy * FAR_SETS[1][2] + far_lane - 2 * CAP, -1),
    )
    turned = ((4 - (dxy >> 2)) & 3) * 4 + ((4 - (dxy & 3)) & 3)
    tile_of = jnp.where(far_row, NZ * NXY + dxy, dz * NXY + turned)
    lane_of = jnp.where(far_row, far_lane, rank)
    for k in (0,) + NEAR:
        lane_of = jnp.where(dz == k, rank + LANE[(NZ - k) % NZ], lane_of)
    tiles_i[...] = jnp.zeros_like(tiles_i)
    for b in range(ROWS // 128):
        cut = slice(128 * b, 128 * b + 128)
        tiles_i[0, b:b + 1, :] = tile_of[:, cut]
        tiles_i[1, b:b + 1, :] = lane_of[:, cut]
    row8 = lax.broadcasted_iota(jnp.int32, (8, ROWS), 0)
    local = ((cid & 255) + 1).astype(jnp.float32)
    values = jnp.where(
        row8 == 0, local,
        jnp.where(row8 == 1, dxy.astype(jnp.float32), jnp.where(row8 == 2, rank_f, 0.0)),
    ).astype(jnp.bfloat16)

    load.wait()
    squares = jnp.zeros((ROWS, 128), jnp.float32)
    for f in range(HALF // 128):
        part = emb[:, 128 * f:128 * f + 128]
        squares = squares + part * part
    mine = jnp.sum(squares.T, axis=0, keepdims=True)
    sq_mine[...] = mine
    pl.semaphore_wait(barrier, NZ - 1 + 2 * (NXY - 1) + len(FAR) + 1)
    sq_copy = send(sq_mine, sq_peer, sq_sem.at[0], sq_sem.at[1], partner)

    place_hot = {}
    for k in NEAR:
        want = lax.broadcasted_iota(jnp.int32, (ROOM, ROWS), 0) + k * ROOM
        place_hot[k] = hot(want == slot)
    far_hot = [
        hot(lax.broadcasted_iota(jnp.int32, (NXY * count, ROWS), 0) == far_slot[e])
        for e, (_, _, count) in enumerate(FAR_SETS)
    ]

    sq_copy.wait()
    scale = lax.rsqrt((sq_mine[...] + sq_peer[...]) / D + 1e-06)
    scale = jnp.broadcast_to(scale, (128, ROWS)).T
    for f in range(HALF // 128):
        unit[:, 128 * f:128 * f + 128] = (emb[:, 128 * f:128 * f + 128] * scale).astype(jnp.bfloat16)

    def pack(k):
        packed = jnp.dot(place_hot[k], unit[...], preferred_element_type=jnp.float32).astype(jnp.bfloat16)
        zout[POS[k]] = packed
        send(zout.at[POS[k]], zin.at[POS[NZ - k]], zs.at[0], zr.at[0 if k in (1, 7) else 1], at_z(k))

    pack(1)
    pack(7)
    left = jnp.where(
        (far_row | (dz == 0)) & (lax.broadcasted_iota(jnp.int32, (NXY, ROWS), 0) == dxy), local, 0.0).astype(jnp.bfloat16)
    right = hot(lax.broadcasted_iota(jnp.int32, (128, ROWS), 0) == far_lane)
    ids = lax.dot_general(left, right, NT, preferred_element_type=jnp.float32)
    for d in AROUND:
        if d == 0:
            fid_in[0] = ids[0:1, :]
        else:
            fid_out[d] = ids[d:d + 1, :]
            send(fid_out.at[d], fid_in.at[neg(d)], vs.at[0], vr.at[0], at_xy(d))

    def pack_far(e):
        count = FAR_SETS[e][2]
        packed = jnp.dot(far_hot[e], unit[...], preferred_element_type=jnp.float32)
        for d in AROUND:
            block = packed[count * d:count * d + count, :].astype(jnp.bfloat16)
            if d == 0:
                fin[e][0] = block
            else:
                fout[e][d] = block
                send(fout[e].at[d], fin[e].at[neg(d)], ws.at[e], wr.at[e], at_xy(d))

    pack_far(0)
    pack_far(1)
    for k in NEAR:
        meta = lax.dot_general(values, place_hot[k], NT, preferred_element_type=jnp.float32)
        mout[POS[k]] = meta
        send(mout.at[POS[k]], min_.at[POS[NZ - k]], ms.at[0], mr.at[0], at_z(k))
    pack(2)
    pack(6)

    p_copies = {}

    def forward(g):
        members, _, count = GROUPS[g]
        total = None
        for m, k in enumerate(members):
            meta = min_[POS[k]]
            valid = meta[0:1, :] > 0.5
            there = jnp.where(valid, meta[1:2, :] * float(count) + meta[2:3, :] + float(CAP * m), -1.0)
            there = there.astype(jnp.int32)
            want = lax.broadcasted_iota(jnp.int32, (NXY * count, ROOM), 0)
            if m == 0:
                arrived(zin.at[pl.ds(2 * g, 2)], zr.at[g])
            part = jnp.dot(hot(want == there), zin[POS[k]], preferred_element_type=jnp.float32)
            total = part if total is None else total + part
        for d in AROUND:
            block = total[count * d:count * d + count, :].astype(jnp.bfloat16)
            if d == 0:
                rows[g][0] = block
            else:
                xout[g][d] = block
                send(xout[g].at[d], rows[g].at[neg(d)], xs.at[g], xr.at[g], at_xy(d))

    def share(g):
        arrived(rows[g].at[others], xr.at[g])
        p_copies[g] = send(rows[g], rows_p[g], ps.at[g], pr.at[g], partner)

    def share_far(kk):
        arrived(z_far.at[kk], zr.at[2 + kk])
        p_copies[3 + kk] = send(z_far.at[kk], z_far_p.at[kk], ps.at[3 + kk], pr.at[3 + kk], partner)

    arrived(fid_in.at[others], vr.at[0])
    known = jnp.concatenate([fid_in[j] for j in range(NXY)], axis=0).astype(jnp.bfloat16)
    back_at = jnp.zeros((NXY, 128), jnp.float32)
    far_values, far_places = [], []
    for planes, first, count in FAR_SETS:
        width = NXY * count
        flat = lax.broadcasted_iota(jnp.int32, (1, width), 1)
        holder = (flat * 2731) >> 16
        within = flat - holder * count
        lane = jnp.where(within < CAP * len(planes), within + CAP * first, -1)
        spread = hot(lax.broadcasted_iota(jnp.int32, (128, width), 0) == lane)
        mine16 = lax.broadcasted_iota(jnp.int32, (NXY, width), 0) == holder
        far_ids = jnp.dot(known, spread, preferred_element_type=jnp.float32)
        far_ids = jnp.sum(jnp.where(mine16, far_ids, 0.0), axis=0, keepdims=True)
        low = lax.broadcasted_iota(jnp.int32, (8, width), 0) * CAP
        inside = (within >= low) & (within < low + CAP) & (low < CAP * len(planes)) & (far_ids > 0.5)
        base_f = jnp.zeros((8, 128), jnp.float32)
        runs = []
        for b in range(width // 128):
            run = base_f + jnp.dot(hot(inside[:, 128 * b:128 * b + 128]), upto, preferred_element_type=jnp.float32)
            runs.append(run)
            base_f = jnp.broadcast_to(run[:, 127:128], (8, 128))
        over = jnp.maximum(over, jnp.where(jnp.max(base_f, axis=0, keepdims=True) > float(ROOM), 1.0, 0.0))
        far_place = jnp.where(inside, jnp.concatenate(runs, axis=1) - 1.0, -1.0)
        far_place = jnp.where(far_place < float(ROOM), far_place, -1.0)
        any_place = jnp.maximum(jnp.max(far_place, axis=0, keepdims=True), 0.0)
        back_at = back_at + lax.dot_general(
            jnp.where(mine16, any_place, 0.0).astype(jnp.bfloat16), spread, NT, preferred_element_type=jnp.float32)
        far_values.append(jnp.broadcast_to(far_ids, (8, width)).astype(jnp.bfloat16))
        far_places.append(far_place)
    back_at = back_at.astype(jnp.int32)

    def relay_far(e):
        planes, _, count = FAR_SETS[e]
        width = NXY * count
        chosen = []
        for m, k in enumerate(planes):
            want = lax.broadcasted_iota(jnp.int32, (ROOM, width), 0).astype(jnp.float32)
            chosen.append(hot(want == far_places[e][m:m + 1, :]))
            mout[POS[k]] = lax.dot_general(far_values[e], chosen[m], NT, preferred_element_type=jnp.float32)
            there = FAR.index(NZ - k)
            send(mout.at[POS[k]], min_.at[POS[NZ - k]], ms.at[0], mr.at[1 + there], at_z(k))
        arrived(fin[e].at[others], wr.at[e])
        for m, k in enumerate(planes):
            zout[POS[k]] = jnp.dot(
                chosen[m], fin[e][...].reshape(width, HALF), preferred_element_type=jnp.float32).astype(jnp.bfloat16)
            there = FAR.index(NZ - k)
            send(zout.at[POS[k]], z_far.at[there], zs.at[0], zr.at[2 + there], at_z(k))

    arrived(min_.at[pl.ds(0, 4)], mr.at[0])
    ids = jnp.zeros((NXY, 128), jnp.float32)
    for k in NEAR:
        meta = min_[POS[k]]
        valid = meta[0:1, :] > 0.5
        to = jnp.where(valid, meta[1:2, :], -1.0).astype(jnp.int32)
        place_k = meta[2:3, :].astype(jnp.int32) + LANE[k]
        left = jnp.where(sub16 == to, meta[0:1, :], 0.0).astype(jnp.bfloat16)
        ids = ids + lax.dot_general(left, hot(sub128 == place_k), NT, preferred_element_type=jnp.float32)
    for d in AROUND:
        if d == 0:
            idin[0] = ids[0:1, :]
        else:
            idout[d] = ids[d:d + 1, :]
            send(idout.at[d], idin.at[neg(d)], ids_s.at[0], ids_r.at[0], at_xy(d))

    forward(0)
    relay_far(0)

    forward(1)
    relay_far(1)

    p_copies[OWN] = send(rows[OWN], rows_p[OWN], ps.at[OWN], pr.at[OWN], partner)
    arrived(idin.at[others], ids_r.at[0])
    for j in range(NXY):
        line = idin[j]
        line = jnp.where(line < 0.5, -1.0, line)
        turned = jnp.broadcast_to(line, (128, 128)).T
        for g, (_, base, count) in enumerate(GROUPS[:OWN]):
            idkey[g][count * j:count * j + count, :] = turned[base:base + count, :]
        line = fid_in[j]
        line = jnp.where((line < 0.5) | (lane128[0:1, :] < 3 * CAP), -1.0, line)
        idkey[OWN][24 * j:24 * j + 24, :] = jnp.broadcast_to(line, (128, 128)).T[2 * CAP:4 * CAP, :]
    for g in range(3):
        half = WIDTH[g] // 2
        for h in range(-(-half // 128)):
            size = min(128, half - 128 * h)
            block = idkey[g][pl.ds(pl.multiple_of(half * c + 128 * h, 8), size), :]
            idq[g, :, 128 * h:128 * h + size] = block.T[0:8, :]
    for ref in (top, top_far, acc0, acc1, acc2, acc_far):
        ref[...] = jnp.full(ref.shape, -float(D), jnp.float32)
    sub256 = lax.broadcasted_iota(jnp.int32, (CLUSTERS, 128), 0).astype(jnp.float32) + 1.0

    def member_sums(source, key):
        seen = jnp.zeros((CLUSTERS, 128), jnp.float32)
        parts = []
        for h in range(key.shape[0] // 128):
            line = source[128 * h:128 * h + 128, :].T[0:1, :]
            member = jnp.where(sub256 == line, 1.0, 0.0)
            seen = seen + member
            parts.append(member.astype(jnp.bfloat16))
        member = jnp.concatenate(parts, axis=1) if len(parts) > 1 else parts[0]
        return seen, jnp.dot(member, key, preferred_element_type=jnp.float32)

    def near_sums(g):
        return member_sums(idkey[g], rows[g][...].reshape(WIDTH[g], HALF))

    def keys_of(g):
        return rows[g][...].reshape(WIDTH[g], HALF), rows_p[g][...].reshape(WIDTH[g], HALF)

    def own_half(g):
        half = WIDTH[g] // 2
        first = pl.ds(pl.multiple_of(NXY // 2 * c, 8), NXY // 2)
        return rows[g][first].reshape(half, HALF), rows_p[g][first].reshape(half, HALF)

    def nt(a, b):
        return lax.dot_general(a, b, NT, preferred_element_type=jnp.float32)

    def near_own(pairs):
        return [(pair, nt(keys_of(pair[0])[0], own_half(pair[1])[0])) for pair in pairs]

    def near_finish(parts):
        for (kg, qg), part in parts:
            nk, nq = WIDTH[kg], WIDTH[qg] // 2
            scores = part + nt(keys_of(kg)[1], own_half(qg)[1])
            for h in range(-(-nq // 128)):
                cut = slice(128 * h, min(128 * h + 128, nq))
                size = cut.stop - cut.start
                same = idkey[kg][...][:, :size] == idq[qg, 0:1, cut]
                if kg == qg:
                    apart = (lax.broadcasted_iota(jnp.int32, (nk, size), 0)
                             - lax.broadcasted_iota(jnp.int32, (nk, size), 1))
                    same = same & (apart != nq * c + 128 * h)
                kept = jnp.where(same, scores[:, cut], -float(D))
                top[qg, :, cut] = jnp.maximum(top[qg, :, cut], jnp.max(kept.reshape(nk // 8, 8, size), axis=0))

    half_far = pl.ds(pl.multiple_of(ROOM // 2 * c, ROOM // 2), ROOM // 2)

    def side(g):
        if g < 3:
            return own_half(g)
        return z_far[g - 3, half_far, :], z_far_p[g - 3, half_far, :]

    def far_own(groups, planes):
        columns = z_far[planes[0]:planes[0] + len(planes)].reshape(ROOM * len(planes), HALF)
        return [(g, nt(side(g)[0], columns)) for g in groups]

    def far_finish(parts, planes):
        first = planes[0]
        columns = z_far_p[first:first + len(planes)].reshape(ROOM * len(planes), HALF)
        for g, part in parts:
            scores = part + nt(side(g)[1], columns)
            n = scores.shape[0]
            if g < 3:
                mine = idkey[g][pl.ds(pl.multiple_of(n * c, 8), n), :]
            else:
                mine = ik_far[g - 3, half_far, :]
            for kk in planes:
                line = min_[POS[FAR[kk]]][0:1, :]
                same = mine == line
                if g == 3 + kk:
                    apart = (lax.broadcasted_iota(jnp.int32, (n, ROOM), 1)
                             - lax.broadcasted_iota(jnp.int32, (n, ROOM), 0))
                    same = same & (apart != n * c)
                kept = jnp.where(same, scores[:, ROOM * (kk - first):ROOM * (kk - first) + ROOM], -float(D))
                top_far[kk] = jnp.maximum(top_far[kk], jnp.max(kept.reshape(n // 8, 8, ROOM), axis=0))
                if g < 3:
                    acc[g][...] = jnp.maximum(acc[g][...], kept)
                elif g - 3 < first:
                    acc_far[g - 3] = jnp.maximum(acc_far[g - 3], kept)

    def take_far(kk):
        arrived(min_.at[POS[FAR[kk]]], mr.at[1 + kk])
        line = min_[POS[FAR[kk]]][0:1, :]
        ik_far[kk] = jnp.broadcast_to(jnp.where(line < 0.5, -1.0, line), (128, 128)).T
        share_far(kk)

    counts, total = near_sums(OWN)
    sums[...] = total
    parts = near_own([(2, 2)])
    p_copies[OWN].wait_recv()
    near_finish(parts)
    share(0)
    parts = near_own([(0, 0), (0, 2), (2, 0)])
    more, total = near_sums(0)
    counts = counts + more
    sums[...] += total
    p_copies[0].wait_recv()
    near_finish(parts)
    share(1)
    parts = near_own([(1, 1), (0, 1), (1, 0), (2, 1), (1, 2)])
    take_far(0)
    take_far(1)
    p_copies[1].wait_recv()
    near_finish(parts)
    parts = far_own([2, 0, 1, 3, 4], (0, 1))
    p_copies[3].wait_recv()
    p_copies[4].wait_recv()
    far_finish(parts, (0, 1))
    take_far(2)
    parts = far_own([2, 0, 1, 3, 4, 5], (2,))
    p_copies[5].wait_recv()
    far_finish(parts, (2,))
    for g, (_, base, count) in enumerate(GROUPS):
        half = WIDTH[g] // 2
        pieces = []
        for h in range(-(-half // 128)):
            size = min(128, half - 128 * h)
            best = jnp.max(top[g, :, 128 * h:128 * h + size], axis=0, keepdims=True)
            pieces.append(jnp.broadcast_to(best, (128, size)).T)
        best = jnp.concatenate(pieces, axis=0)
        best = jnp.maximum(best, jnp.max(acc[g][...], axis=1, keepdims=True)) * (1.0 / D)
        for i in range(NXY // 2):
            column[i, base:base + count, :] = best[count * i:count * i + count, :]
    for kk in range(3):
        best = jnp.max(top_far[kk], axis=0, keepdims=True)
        if kk < 2:
            mine = jnp.broadcast_to(jnp.max(acc_far[kk], axis=1, keepdims=True), (ROOM // 2, 128))
            mine = jnp.concatenate([jnp.where(c == h, mine, -float(D)) for h in range(2)], axis=0)
            best = jnp.maximum(best, mine.T[0:1, :])
        far_out[kk, :, 0:128] = best * (1.0 / D)
        far_out[kk, :, 128:256] = over
    for kk, k in enumerate(FAR):
        there = FAR.index(NZ - k)
        for core in range(2):
            send(far_out.at[kk], far_z.at[c, there], us.at[core], ur.at[0], (at_z(k)[0], core))
    for i in range(NXY // 2):
        best_out[i] = jnp.where(last, over, column[i].T[0:1, :])

    def best_copy(i, other):
        jx, jy = 2 * c + i // 4, i % 4
        there = (z * 16 + ((x + jx) % 4) * 4 + (y + jy) % 4, 1 - c if other else c)
        return pltpu.make_async_remote_copy(
            best_out.at[i], ret1.at[8 * c + i], bs.at[int(other)], br.at[0],
            device_id=there, device_id_type=MESH)

    @pl.when(c == 0)
    def _():
        ret1[0] = best_out[0]

    @pl.when(c == 1)
    def _():
        best_copy(0, False).start()

    best_copy(0, True).start()
    for i in range(1, 8):
        best_copy(i, False).start()
        best_copy(i, True).start()

    more, total = near_sums(1)
    counts = counts + more
    for kk in range(3):
        more, part = member_sums(ik_far[kk], z_far[kk])
        counts = counts + more
        total = total + part
    cent_load.wait()
    mass_load.wait()
    number = jnp.sum(counts, axis=1, keepdims=True)
    mass = jnp.broadcast_to(mass_v[...], (128, CLUSTERS)).T[:, 0:1]
    cent[...] = (mass * cent[...] + (sums[...] + total)) / (mass + number)
    nc_copy = pltpu.make_async_copy(cent, nc_ref, local_sem.at[2])
    nc_copy.start()

    @pl.when(c == 0)
    def _():
        arrived(ret1.at[others], br.at[0])

    @pl.when(c == 1)
    def _():
        arrived(ret1, br.at[0])

    back = {}
    for k in (2, 6, 1, 7):
        back[NZ - k] = send(
            ret1, ret2.at[POS[NZ - k]], fs.at[POS[k]], fr.at[POS[NZ - k]], at_z(k))
    arrived(far_z, ur.at[0])
    lane16 = lax.broadcasted_iota(jnp.int32, (NXY, 128), 1)
    got = jnp.zeros((NXY, 128), jnp.float32)
    for kk in range(3):
        line = jnp.maximum(far_z[0, kk][:, 0:128], far_z[1, kk][:, 0:128])
        line = jnp.broadcast_to(line, (8, 128))
        found = jnp.concatenate(
            [jnp.take_along_axis(line, back_at[8 * h:8 * h + 8, :], axis=1, mode="promise_in_bounds") for h in range(2)],
            axis=0)
        got = jnp.where(lane16 >= kk * CAP, found, got)
    far_over = far_z[0, 0][:, 128:256]
    for h in range(2):
        for kk in range(3):
            far_over = jnp.maximum(far_over, far_z[h, kk][:, 128:256])
    got = jnp.where(lane16 == 127, far_over, got)
    for j in AROUND:
        if j == 0:
            far_ret[0] = got[0:1, :]
        else:
            back_out[j] = got[j:j + 1, :]
            send(back_out.at[j], far_ret.at[neg(j)], ts.at[0], tr.at[0], at_xy(j))
    tile_t = tiles_i[0]
    lane_t = tiles_i[1]
    result = jnp.zeros((8, 128), jnp.float32)
    flag = jnp.zeros((1, 128), jnp.float32)

    def pick(line, tile, result, flag):
        got = jnp.take_along_axis(jnp.broadcast_to(line, (8, 128)), lane_t, axis=1, mode="promise_in_bounds")
        return jnp.where(tile_t == tile, got, result), jnp.maximum(flag, jnp.where(last, line, 0.0))

    for j in range(NXY):
        result, flag = pick(ret1[j], j, result, flag)
    for k in NEAR:
        back[k].wait_recv()
        for j in range(NXY):
            result, flag = pick(ret2[POS[k], j], k * NXY + j, result, flag)
    arrived(far_ret.at[others], tr.at[0])
    for d in range(NXY):
        result, flag = pick(far_ret[d], NZ * NXY + d, result, flag)
    for b in range(ROWS // 128):
        best_ref[:, 128 * b:128 * b + 128] = result[b:b + 1, :]
    flag_ref[0, 0] = jnp.max(flag).astype(jnp.int32)

    @pl.when(c == 0)
    def _():
        sent(best_out.at[pl.ds(1, 7)], bs.at[0])

    @pl.when(c == 1)
    def _():
        sent(best_out, bs.at[0])

    sent(best_out, bs.at[1])
    for copy in list(back.values()) + list(p_copies.values()):
        copy.wait_send()
    sent(zout, zs.at[0])
    sent(mout, ms.at[0])
    for e in range(2):
        sent(xout[e].at[others], xs.at[e])
        sent(fout[e].at[others], ws.at[e])
        sent(far_out, us.at[e])
    sent(fid_out.at[others], vs.at[0])
    sent(idout.at[others], ids_s.at[0])
    sent(back_out.at[others], ts.at[0])
    nc_copy.wait()


def compact(embeddings, cluster_id, centroids, cluster_mass):
    vmem = pl.BlockSpec(memory_space=pltpu.VMEM)
    anywhere = pl.BlockSpec(memory_space=pl.ANY)
    f32, bf16, i32 = jnp.float32, jnp.bfloat16, jnp.int32
    dma = pltpu.SemaphoreType.DMA
    line = (1, 128)
    return pl.pallas_call(
        exchange_kernel,
        out_shape=(
            jax.ShapeDtypeStruct((1, ROWS), f32),
            jax.ShapeDtypeStruct((CLUSTERS, HALF), f32),
            jax.ShapeDtypeStruct((1, 1), i32),
        ),
        in_specs=[anywhere, anywhere, anywhere, anywhere],
        out_specs=(vmem, anywhere, pl.BlockSpec(memory_space=pltpu.SMEM)),
        scratch_shapes=[
            pltpu.VMEM((ROWS, HALF), f32),
            pltpu.VMEM((ROWS, HALF), bf16),
            pltpu.VMEM((1, ROWS), f32),
            pltpu.VMEM((1, ROWS), f32),
            pltpu.VMEM((NZ - 1, ROOM, HALF), bf16),
            pltpu.VMEM((len(NEAR), ROOM, HALF), bf16),
            pltpu.VMEM((3, ROOM, HALF), bf16),
            pltpu.VMEM((3, ROOM, HALF), bf16),
            pltpu.VMEM((NZ - 1, 8, 128), f32),
            pltpu.VMEM((NZ - 1, 8, 128), f32),
            *[pltpu.VMEM((NXY, count, HALF), bf16) for _, _, count in GROUPS[:OWN]],
            pltpu.VMEM((NXY, *line), f32),
            *[pltpu.VMEM((NXY, far[2], HALF), bf16) for far in FAR_SETS],
            *[pltpu.VMEM((NXY, far[2], HALF), bf16) for far in FAR_SETS],
            pltpu.VMEM((NXY, FAR_SETS[1][2], HALF), bf16),
            pltpu.VMEM((NXY, *line), f32),
            pltpu.VMEM((NXY, *line), f32),
            *[pltpu.VMEM((NXY, count, HALF), bf16) for _, _, count in GROUPS[:OWN]],
            *[pltpu.VMEM((NXY, count, HALF), bf16) for _, _, count in GROUPS[:OWN]],
            pltpu.VMEM((NXY, *line), f32),
            *[pltpu.VMEM((NXY * count, 128), f32) for _, _, count in GROUPS],
            pltpu.VMEM((3, 128, 128), f32),
            pltpu.VMEM((3, 8, 256), f32),
            pltpu.VMEM((3, 8, 256), f32),
            *[pltpu.VMEM((width // 2, 128), f32) for width in WIDTH],
            pltpu.VMEM((2, ROOM // 2, 128), f32),
            pltpu.VMEM((3, 8, 128), f32),
            pltpu.VMEM((CLUSTERS, HALF), f32),
            pltpu.VMEM((2, 8, 128), i32),
            pltpu.VMEM((8, 128, 128), f32),
            pltpu.VMEM((8, *line), f32),
            pltpu.VMEM((3, 1, 256), f32),
            pltpu.VMEM((NXY, *line), f32),
            pltpu.VMEM((len(NEAR), NXY, *line), f32),
            pltpu.VMEM((2, 3, 1, 256), f32),
            pltpu.VMEM((NXY, *line), f32),
            pltpu.VMEM((NXY, *line), f32),
            pltpu.VMEM((CLUSTERS, HALF), f32),
            pltpu.VMEM((ROWS,), i32),
            pltpu.VMEM((1, CLUSTERS), f32),
            dma((5,)), dma((2,)), dma((1,)), dma((5,)), dma((1,)), dma((4,)), dma((2,)), dma((2,)),
            dma((1,)), dma((1,)), dma((6,)), dma((6,)), dma((2,)), dma((1,)), dma((4,)), dma((4,)),
            dma((2,)), dma((2,)), dma((1,)), dma((1,)), dma((2,)), dma((1,)), dma((1,)), dma((1,)),
        ],
        compiler_params=pltpu.CompilerParams(
            collective_id=0, has_side_effects=True, vmem_limit_bytes=48 * 2**20),
    )(embeddings, cluster_id, centroids, cluster_mass.reshape(1, CLUSTERS))


def from_partner(value):
    return lax.ppermute(value, "mp", [(0, 1), (1, 0)])


def general(embeddings, cluster_id, centroids, cluster_mass):
    owners = lax.axis_size("dp")
    row_count = embeddings.shape[0]
    slot_count = 2 * row_count
    capacity = slot_count // owners
    cluster_count = centroids.shape[0]
    core = lax.axis_index("mp")
    squares = jnp.sum(embeddings * embeddings, axis=1)
    squares = squares + from_partner(squares)
    unit = (embeddings * lax.rsqrt(squares / D + 1e-06)[:, None]).astype(jnp.bfloat16)
    owner = cluster_id // cluster_count
    local = cluster_id - owner * cluster_count
    owner_hot = (owner[:, None] == jnp.arange(owners, dtype=jnp.int32)[None, :]).astype(jnp.bfloat16)
    row_index = jnp.arange(row_count, dtype=jnp.int32)
    lower = (row_index[:, None] >= row_index[None, :]).astype(jnp.bfloat16)
    running = jnp.dot(lower, owner_hot, preferred_element_type=jnp.float32)
    rank = jnp.sum(running * owner_hot.astype(jnp.float32), axis=1).astype(jnp.int32) - 1
    slot = owner * capacity + rank
    slot_index = jnp.arange(slot_count, dtype=jnp.int32)
    placed = slot_index[:, None] == slot[None, :]
    outgoing = jnp.dot(
        placed.astype(jnp.bfloat16), unit, preferred_element_type=jnp.float32
    ).astype(jnp.bfloat16)
    out_ids = jnp.max(jnp.where(placed, local[None, :] + 1, 0), axis=1) - 1
    incoming = lax.all_to_all(outgoing, "dp", split_axis=0, concat_axis=0, tiled=True)
    in_ids = lax.all_to_all(out_ids, "dp", split_axis=0, concat_axis=0, tiled=True)
    member = (jnp.arange(cluster_count, dtype=jnp.int32)[:, None] == in_ids[None, :]).astype(jnp.bfloat16)
    sums = jnp.dot(member, incoming, preferred_element_type=jnp.float32)
    counts = jnp.sum(member.astype(jnp.float32), axis=1)
    new_centroids = (cluster_mass[:, None] * centroids + sums) / (cluster_mass + counts)[:, None]
    half = slot_count // 2
    start = core * half
    contract = (((1,), (1,)), ((), ()))
    other = from_partner(incoming)
    scores = lax.dot_general(
        lax.dynamic_slice_in_dim(incoming, start, half, 0), incoming, contract, preferred_element_type=jnp.float32)
    scores = scores + lax.dot_general(
        lax.dynamic_slice_in_dim(other, start, half, 0), other, contract, preferred_element_type=jnp.float32)
    scores = scores / D
    query_ids = lax.dynamic_slice_in_dim(in_ids, start, half, 0)
    query_pos = start + jnp.arange(half, dtype=jnp.int32)
    same = (
        (query_ids[:, None] == in_ids[None, :])
        & (query_ids[:, None] >= 0)
        & (query_pos[:, None] != slot_index[None, :])
    )
    best = jnp.max(jnp.where(same, scores, -1.0), axis=1)
    best_p = from_partner(best)
    low, high = jnp.where(core == 0, best, best_p), jnp.where(core == 0, best_p, best)
    returned = lax.all_to_all(
        jnp.concatenate([low, high]), "dp", split_axis=0, concat_axis=0, tiled=True)
    return jnp.take(returned, slot), new_centroids


def shards(embeddings, cluster_id, centroids, cluster_mass):
    best, new_centroids, flag = compact(embeddings, cluster_id, centroids, cluster_mass)
    return lax.cond(
        flag[0, 0] > 0,
        lambda *args: general(*args),
        lambda *args: (best.reshape(ROWS), new_centroids),
        embeddings, cluster_id, centroids, cluster_mass,
    )


def solution(mesh):
    in_specs = (P("dp", "mp"), P("dp"), P("dp", "mp"), P("dp"))
    out_specs = (P("dp"), P("dp", "mp"))
    return jax.shard_map(shards, mesh=mesh, in_specs=in_specs, out_specs=out_specs, check_vma=False)
```

```python
import functools

import jax
import jax.numpy as jnp
from jax import lax
from jax.experimental import pallas as pl
from jax.experimental.pallas import tpu as pltpu
from jax.sharding import PartitionSpec as P

D = 1024
HALF = 512
ROWS = 768
CLUSTERS = 256
CAP = 12
ROOM = 128
NZ = 8
NXY = 16
GROUPS = (((1, 7), 0, 24), ((2, 6), 24, 24), ((None, 0), 48, 24))
LANE = {k: base + CAP * m for members, base, _ in GROUPS for m, k in enumerate(members) if k is not None}
OWN = 2
FAR = (3, 5, 4)
FAR_SETS = (((3, 5), 0, 24), ((4,), 2, 24))
WIDTH = tuple(count * NXY for _, _, count in GROUPS)
MESH = pl.DeviceIdType.MESH
NT = (((1,), (1,)), ((), ()))
NEAR = (1, 7, 2, 6)
AROUND = (10, 9, 11, 6, 14, 2, 8, 5, 7, 13, 15, 1, 3, 4, 12, 0)
POS = {k: i for i, k in enumerate(NEAR + FAR)}


def neg(d):
    return ((4 - d // 4) % 4) * 4 + (4 - d % 4) % 4


def hot(mask):
    return jnp.where(mask, 1.0, 0.0).astype(jnp.bfloat16)


def exchange_kernel(
    emb_ref, cid_ref, cent_ref, mass_ref,
    best_ref, nc_ref, flag_ref,
    emb, unit, sq_mine, sq_peer, zout, zin, z_far, z_far_p, mout, min_, xo0, xo1, idout, fo0, fo1, fi0, fi1, fi1_p, fid_out, fid_in,
    r0, r1, p0, p1, idin, ik0, ik1, ik2, ik_far, top, idq, acc0, acc1, acc2, acc_far, top_far, sums,
    tiles_i, column, best_out, far_out, ret1, ret2, far_z, back_out, far_ret, cent, cid_v, mass_v,
    local_sem, sq_sem, zs, zr, ms, mr, xs, xr, ids_s, ids_r, ps, pr, bs, br, fs, fr,
    ws, wr, vs, vr, us, ur, ts, tr,
):
    xout, rows, rows_p, idkey = (xo0, xo1), (r0, r1, fi1), (p0, p1, fi1_p), (ik0, ik1, ik2)
    fout, fin, acc = (fo0, fo1), (fi0, fi1), (acc0, acc1, acc2)
    me = lax.axis_index("dp")
    c = lax.axis_index("mp")
    z, x, y = me // 16, (me // 4) % 4, me % 4

    def at_z(k):
        return (((z + k) % NZ) * 16 + x * 4 + y, c)

    def at_xy(d):
        return (z * 16 + ((x + d // 4) % 4) * 4 + (y + d % 4) % 4, c)

    partner = (me, 1 - c)

    def send(src, dst, send_sem, recv_sem, to):
        copy = pltpu.make_async_remote_copy(src, dst, send_sem, recv_sem, device_id=to, device_id_type=MESH)
        copy.start()
        return copy

    def sent(ref, sem):
        pltpu.make_async_remote_copy(ref, ref, sem, sem, device_id=partner, device_id_type=MESH).wait_send()

    def arrived(ref, sem):
        pltpu.make_async_remote_copy(ref, ref, sem, sem, device_id=partner, device_id_type=MESH).wait_recv()

    others = pl.ds(1, NXY - 1)

    cid_load = pltpu.make_async_copy(cid_ref, cid_v, local_sem.at[3])
    cid_load.start()
    mass_load = pltpu.make_async_copy(mass_ref, mass_v, local_sem.at[4])
    mass_load.start()
    load = pltpu.make_async_copy(emb_ref, emb, local_sem.at[0])
    load.start()
    cent_load = pltpu.make_async_copy(cent_ref, cent, local_sem.at[1])
    cent_load.start()
    barrier = pltpu.get_barrier_semaphore()
    for k in FAR[::-1]:
        pl.semaphore_signal(barrier, inc=1, device_id=at_z(k), device_id_type=MESH)
        pl.semaphore_signal(barrier, inc=1, device_id=(at_z(k)[0], 1 - c), device_id_type=MESH)
    for d in AROUND[:-1]:
        pl.semaphore_signal(barrier, inc=1, device_id=at_xy(d), device_id_type=MESH)
        pl.semaphore_signal(barrier, inc=1, device_id=(at_xy(d)[0], 1 - c), device_id_type=MESH)
    for k in NEAR:
        pl.semaphore_signal(barrier, inc=1, device_id=at_z(k), device_id_type=MESH)
    pl.semaphore_signal(barrier, inc=1, device_id=partner, device_id_type=MESH)

    cid_load.wait()
    cid = cid_v[...].reshape(1, ROWS)
    owner = cid >> 8
    dz = ((owner >> 4) - z) & 7
    dxy = ((((owner >> 2) & 3) - x) & 3) * 4 + (((owner & 3) - y) & 3)
    target = dz * 16 + dxy
    lane128 = lax.broadcasted_iota(jnp.int32, (128, 128), 1)
    sub128 = lax.broadcasted_iota(jnp.int32, (128, 128), 0)
    upto = hot(sub128 <= lane128)
    sub8 = lax.broadcasted_iota(jnp.int32, (8, 128), 0)
    sub16 = lax.broadcasted_iota(jnp.int32, (NXY, 128), 0)
    last = lax.broadcasted_iota(jnp.int32, (1, 128), 1) == 127
    base_t = jnp.zeros((128, 128), jnp.float32)
    base_z = jnp.zeros((8, 128), jnp.float32)
    ranks, places = [], []
    for b in range(ROWS // 128):
        cut = slice(128 * b, 128 * b + 128)
        is_t = sub128 == target[:, cut]
        is_z = sub8 == dz[:, cut]
        run_t = base_t + jnp.dot(hot(is_t), upto, preferred_element_type=jnp.float32)
        run_z = base_z + jnp.dot(hot(is_z), upto, preferred_element_type=jnp.float32)
        ranks.append(jnp.sum(jnp.where(is_t, run_t, 0.0), axis=0, keepdims=True) - 1.0)
        places.append(jnp.sum(jnp.where(is_z, run_z, 0.0), axis=0, keepdims=True) - 1.0)
        base_t = jnp.broadcast_to(run_t[:, 127:128], (128, 128))
        base_z = jnp.broadcast_to(run_z[:, 127:128], (8, 128))
    near_most = jnp.where((sub8 == 1) | (sub8 == 2) | (sub8 > 5), base_z, 0.0)
    over = jnp.where(jnp.max(near_most, axis=0, keepdims=True) > float(ROOM), 1.0, 0.0)
    rank_f = jnp.concatenate(ranks, axis=1)
    rank = rank_f.astype(jnp.int32)
    place = jnp.concatenate(places, axis=1).astype(jnp.int32)
    slot = jnp.where(place < ROOM, dz * ROOM + place, -1)
    far_row = (dz >= 3) & (dz <= 5)
    far_lane = jnp.where(dz == 3, rank, jnp.where(dz == 5, rank + CAP, rank + 2 * CAP))
    far_lane = jnp.where(far_row, far_lane, jnp.where(dz == 0, rank + 3 * CAP, -1))
    far_slot = (
        jnp.where((dz == 3) | (dz == 5), dxy * FAR_SETS[0][2] + far_lane, -1),
        jnp.where((dz == 4) | (dz == 0), dxy * FAR_SETS[1][2] + far_lane - 2 * CAP, -1),
    )
    turned = ((4 - (dxy >> 2)) & 3) * 4 + ((4 - (dxy & 3)) & 3)
    tile_of = jnp.where(far_row, NZ * NXY + dxy, dz * NXY + turned)
    lane_of = jnp.where(far_row, far_lane, rank)
    for k in (0,) + NEAR:
        lane_of = jnp.where(dz == k, rank + LANE[(NZ - k) % NZ], lane_of)
    tiles_i[...] = jnp.zeros_like(tiles_i)
    for b in range(ROWS // 128):
        cut = slice(128 * b, 128 * b + 128)
        tiles_i[0, b:b + 1, :] = tile_of[:, cut]
        tiles_i[1, b:b + 1, :] = lane_of[:, cut]
    row8 = lax.broadcasted_iota(jnp.int32, (8, ROWS), 0)
    local = ((cid & 255) + 1).astype(jnp.float32)
    values = jnp.where(
        row8 == 0, local,
        jnp.where(row8 == 1, dxy.astype(jnp.float32), jnp.where(row8 == 2, rank_f, 0.0)),
    ).astype(jnp.bfloat16)

    load.wait()
    squares = jnp.zeros((ROWS, 128), jnp.float32)
    for f in range(HALF // 128):
        part = emb[:, 128 * f:128 * f + 128]
        squares = squares + part * part
    mine = jnp.sum(squares.T, axis=0, keepdims=True)
    sq_mine[...] = mine
    pl.semaphore_wait(barrier, NZ - 1 + 2 * (NXY - 1) + len(FAR) + 1)
    sq_copy = send(sq_mine, sq_peer, sq_sem.at[0], sq_sem.at[1], partner)

    place_hot = {}
    for k in NEAR:
        want = lax.broadcasted_iota(jnp.int32, (ROOM, ROWS), 0) + k * ROOM
        place_hot[k] = hot(want == slot)
    far_hot = [
        hot(lax.broadcasted_iota(jnp.int32, (NXY * count, ROWS), 0) == far_slot[e])
        for e, (_, _, count) in enumerate(FAR_SETS)
    ]

    sq_copy.wait()
    scale = lax.rsqrt((sq_mine[...] + sq_peer[...]) / D + 1e-06)
    scale = jnp.broadcast_to(scale, (128, ROWS)).T
    for f in range(HALF // 128):
        unit[:, 128 * f:128 * f + 128] = (emb[:, 128 * f:128 * f + 128] * scale).astype(jnp.bfloat16)

    def pack(k):
        packed = jnp.dot(place_hot[k], unit[...], preferred_element_type=jnp.float32).astype(jnp.bfloat16)
        zout[POS[k]] = packed
        send(zout.at[POS[k]], zin.at[POS[NZ - k]], zs.at[0], zr.at[0 if k in (1, 7) else 1], at_z(k))

    pack(1)
    pack(7)
    left = jnp.where(
        (far_row | (dz == 0)) & (lax.broadcasted_iota(jnp.int32, (NXY, ROWS), 0) == dxy), local, 0.0).astype(jnp.bfloat16)
    right = hot(lax.broadcasted_iota(jnp.int32, (128, ROWS), 0) == far_lane)
    ids = lax.dot_general(left, right, NT, preferred_element_type=jnp.float32)
    for d in AROUND:
        if d == 0:
            fid_in[0] = ids[0:1, :]
        else:
            fid_out[d] = ids[d:d + 1, :]
            send(fid_out.at[d], fid_in.at[neg(d)], vs.at[0], vr.at[0], at_xy(d))

    def pack_far(e):
        count = FAR_SETS[e][2]
        packed = jnp.dot(far_hot[e], unit[...], preferred_element_type=jnp.float32)
        for d in AROUND:
            block = packed[count * d:count * d + count, :].astype(jnp.bfloat16)
            if d == 0:
                fin[e][0] = block
            else:
                fout[e][d] = block
                send(fout[e].at[d], fin[e].at[neg(d)], ws.at[e], wr.at[e], at_xy(d))

    pack_far(0)
    pack_far(1)
    for k in NEAR:
        meta = lax.dot_general(values, place_hot[k], NT, preferred_element_type=jnp.float32)
        mout[POS[k]] = meta
        send(mout.at[POS[k]], min_.at[POS[NZ - k]], ms.at[0], mr.at[0], at_z(k))
    pack(2)
    pack(6)

    p_copies = {}

    def forward(g):
        members, _, count = GROUPS[g]
        total = None
        for m, k in enumerate(members):
            meta = min_[POS[k]]
            valid = meta[0:1, :] > 0.5
            there = jnp.where(valid, meta[1:2, :] * float(count) + meta[2:3, :] + float(CAP * m), -1.0)
            there = there.astype(jnp.int32)
            want = lax.broadcasted_iota(jnp.int32, (NXY * count, ROOM), 0)
            if m == 0:
                arrived(zin.at[pl.ds(2 * g, 2)], zr.at[g])
            part = jnp.dot(hot(want == there), zin[POS[k]], preferred_element_type=jnp.float32)
            total = part if total is None else total + part
        for d in AROUND:
            block = total[count * d:count * d + count, :].astype(jnp.bfloat16)
            if d == 0:
                rows[g][0] = block
            else:
                xout[g][d] = block
                send(xout[g].at[d], rows[g].at[neg(d)], xs.at[g], xr.at[g], at_xy(d))

    def share(g):
        arrived(rows[g].at[others], xr.at[g])
        p_copies[g] = send(rows[g], rows_p[g], ps.at[g], pr.at[g], partner)

    def share_far(kk):
        arrived(z_far.at[kk], zr.at[2 + kk])
        p_copies[3 + kk] = send(z_far.at[kk], z_far_p.at[kk], ps.at[3 + kk], pr.at[3 + kk], partner)

    arrived(fid_in.at[others], vr.at[0])
    known = jnp.concatenate([fid_in[j] for j in range(NXY)], axis=0).astype(jnp.bfloat16)
    back_at = jnp.zeros((NXY, 128), jnp.float32)
    far_values, far_places = [], []
    for planes, first, count in FAR_SETS:
        width = NXY * count
        flat = lax.broadcasted_iota(jnp.int32, (1, width), 1)
        holder = (flat * 2731) >> 16
        within = flat - holder * count
        lane = jnp.where(within < CAP * len(planes), within + CAP * first, -1)
        spread = hot(lax.broadcasted_iota(jnp.int32, (128, width), 0) == lane)
        mine16 = lax.broadcasted_iota(jnp.int32, (NXY, width), 0) == holder
        far_ids = jnp.dot(known, spread, preferred_element_type=jnp.float32)
        far_ids = jnp.sum(jnp.where(mine16, far_ids, 0.0), axis=0, keepdims=True)
        low = lax.broadcasted_iota(jnp.int32, (8, width), 0) * CAP
        inside = (within >= low) & (within < low + CAP) & (low < CAP * len(planes)) & (far_ids > 0.5)
        base_f = jnp.zeros((8, 128), jnp.float32)
        runs = []
        for b in range(width // 128):
            run = base_f + jnp.dot(hot(inside[:, 128 * b:128 * b + 128]), upto, preferred_element_type=jnp.float32)
            runs.append(run)
            base_f = jnp.broadcast_to(run[:, 127:128], (8, 128))
        over = jnp.maximum(over, jnp.where(jnp.max(base_f, axis=0, keepdims=True) > float(ROOM), 1.0, 0.0))
        far_place = jnp.where(inside, jnp.concatenate(runs, axis=1) - 1.0, -1.0)
        far_place = jnp.where(far_place < float(ROOM), far_place, -1.0)
        any_place = jnp.maximum(jnp.max(far_place, axis=0, keepdims=True), 0.0)
        back_at = back_at + lax.dot_general(
            jnp.where(mine16, any_place, 0.0).astype(jnp.bfloat16), spread, NT, preferred_element_type=jnp.float32)
        far_values.append(jnp.broadcast_to(far_ids, (8, width)).astype(jnp.bfloat16))
        far_places.append(far_place)
    back_at = back_at.astype(jnp.int32)

    def relay_far(e):
        planes, _, count = FAR_SETS[e]
        width = NXY * count
        chosen = []
        for m, k in enumerate(planes):
            want = lax.broadcasted_iota(jnp.int32, (ROOM, width), 0).astype(jnp.float32)
            chosen.append(hot(want == far_places[e][m:m + 1, :]))
            mout[POS[k]] = lax.dot_general(far_values[e], chosen[m], NT, preferred_element_type=jnp.float32)
            there = FAR.index(NZ - k)
            send(mout.at[POS[k]], min_.at[POS[NZ - k]], ms.at[0], mr.at[1 + there], at_z(k))
        arrived(fin[e].at[others], wr.at[e])
        for m, k in enumerate(planes):
            zout[POS[k]] = jnp.dot(
                chosen[m], fin[e][...].reshape(width, HALF), preferred_element_type=jnp.float32).astype(jnp.bfloat16)
            there = FAR.index(NZ - k)
            send(zout.at[POS[k]], z_far.at[there], zs.at[0], zr.at[2 + there], at_z(k))

    arrived(min_.at[pl.ds(0, 4)], mr.at[0])
    ids = jnp.zeros((NXY, 128), jnp.float32)
    for k in NEAR:
        meta = min_[POS[k]]
        valid = meta[0:1, :] > 0.5
        to = jnp.where(valid, meta[1:2, :], -1.0).astype(jnp.int32)
        place_k = meta[2:3, :].astype(jnp.int32) + LANE[k]
        left = jnp.where(sub16 == to, meta[0:1, :], 0.0).astype(jnp.bfloat16)
        ids = ids + lax.dot_general(left, hot(sub128 == place_k), NT, preferred_element_type=jnp.float32)
    for d in AROUND:
        if d == 0:
            idin[0] = ids[0:1, :]
        else:
            idout[d] = ids[d:d + 1, :]
            send(idout.at[d], idin.at[neg(d)], ids_s.at[0], ids_r.at[0], at_xy(d))

    forward(0)
    relay_far(0)

    forward(1)
    relay_far(1)

    p_copies[OWN] = send(rows[OWN], rows_p[OWN], ps.at[OWN], pr.at[OWN], partner)
    arrived(idin.at[others], ids_r.at[0])
    for j in range(NXY):
        line = idin[j]
        line = jnp.where(line < 0.5, -1.0, line)
        turned = jnp.broadcast_to(line, (128, 128)).T
        for g, (_, base, count) in enumerate(GROUPS[:OWN]):
            idkey[g][count * j:count * j + count, :] = turned[base:base + count, :]
        line = fid_in[j]
        line = jnp.where((line < 0.5) | (lane128[0:1, :] < 3 * CAP), -1.0, line)
        idkey[OWN][24 * j:24 * j + 24, :] = jnp.broadcast_to(line, (128, 128)).T[2 * CAP:4 * CAP, :]
    for g in range(3):
        half = WIDTH[g] // 2
        for h in range(-(-half // 128)):
            size = min(128, half - 128 * h)
            block = idkey[g][pl.ds(pl.multiple_of(half * c + 128 * h, 8), size), :]
            idq[g, :, 128 * h:128 * h + size] = block.T[0:8, :]
    for ref in (top, top_far, acc0, acc1, acc2, acc_far):
        ref[...] = jnp.full(ref.shape, -float(D), jnp.float32)
    sub256 = lax.broadcasted_iota(jnp.int32, (CLUSTERS, 128), 0).astype(jnp.float32) + 1.0

    def member_sums(source, key):
        seen = jnp.zeros((CLUSTERS, 128), jnp.float32)
        parts = []
        for h in range(key.shape[0] // 128):
            line = source[128 * h:128 * h + 128, :].T[0:1, :]
            member = jnp.where(sub256 == line, 1.0, 0.0)
            seen = seen + member
            parts.append(member.astype(jnp.bfloat16))
        member = jnp.concatenate(parts, axis=1) if len(parts) > 1 else parts[0]
        return seen, jnp.dot(member, key, preferred_element_type=jnp.float32)

    def near_sums(g):
        return member_sums(idkey[g], rows[g][...].reshape(WIDTH[g], HALF))

    def keys_of(g):
        return rows[g][...].reshape(WIDTH[g], HALF), rows_p[g][...].reshape(WIDTH[g], HALF)

    def own_half(g):
        half = WIDTH[g] // 2
        first = pl.ds(pl.multiple_of(NXY // 2 * c, 8), NXY // 2)
        return rows[g][first].reshape(half, HALF), rows_p[g][first].reshape(half, HALF)

    def nt(a, b):
        return lax.dot_general(a, b, NT, preferred_element_type=jnp.float32)

    def near_own(pairs):
        return [(pair, nt(keys_of(pair[0])[0], own_half(pair[1])[0])) for pair in pairs]

    def near_finish(parts):
        for (kg, qg), part in parts:
            nk, nq = WIDTH[kg], WIDTH[qg] // 2
            scores = part + nt(keys_of(kg)[1], own_half(qg)[1])
            for h in range(-(-nq // 128)):
                cut = slice(128 * h, min(128 * h + 128, nq))
                size = cut.stop - cut.start
                same = idkey[kg][...][:, :size] == idq[qg, 0:1, cut]
                if kg == qg:
                    apart = (lax.broadcasted_iota(jnp.int32, (nk, size), 0)
                             - lax.broadcasted_iota(jnp.int32, (nk, size), 1))
                    same = same & (apart != nq * c + 128 * h)
                kept = jnp.where(same, scores[:, cut], -float(D))
                top[qg, :, cut] = jnp.maximum(top[qg, :, cut], jnp.max(kept.reshape(nk // 8, 8, size), axis=0))

    half_far = pl.ds(pl.multiple_of(ROOM // 2 * c, ROOM // 2), ROOM // 2)

    def side(g):
        if g < 3:
            return own_half(g)
        return z_far[g - 3, half_far, :], z_far_p[g - 3, half_far, :]

    def far_own(groups, planes):
        columns = z_far[planes[0]:planes[0] + len(planes)].reshape(ROOM * len(planes), HALF)
        return [(g, nt(side(g)[0], columns)) for g in groups]

    def far_finish(parts, planes):
        first = planes[0]
        columns = z_far_p[first:first + len(planes)].reshape(ROOM * len(planes), HALF)
        for g, part in parts:
            scores = part + nt(side(g)[1], columns)
            n = scores.shape[0]
            if g < 3:
                mine = idkey[g][pl.ds(pl.multiple_of(n * c, 8), n), :]
            else:
                mine = ik_far[g - 3, half_far, :]
            for kk in planes:
                line = min_[POS[FAR[kk]]][0:1, :]
                same = mine == line
                if g == 3 + kk:
                    apart = (lax.broadcasted_iota(jnp.int32, (n, ROOM), 1)
                             - lax.broadcasted_iota(jnp.int32, (n, ROOM), 0))
                    same = same & (apart != n * c)
                kept = jnp.where(same, scores[:, ROOM * (kk - first):ROOM * (kk - first) + ROOM], -float(D))
                top_far[kk] = jnp.maximum(top_far[kk], jnp.max(kept.reshape(n // 8, 8, ROOM), axis=0))
                if g < 3:
                    acc[g][...] = jnp.maximum(acc[g][...], kept)
                elif g - 3 < first:
                    acc_far[g - 3] = jnp.maximum(acc_far[g - 3], kept)

    def take_far(kk):
        arrived(min_.at[POS[FAR[kk]]], mr.at[1 + kk])
        line = min_[POS[FAR[kk]]][0:1, :]
        ik_far[kk] = jnp.broadcast_to(jnp.where(line < 0.5, -1.0, line), (128, 128)).T
        share_far(kk)

    counts, total = near_sums(OWN)
    sums[...] = total
    parts = near_own([(2, 2)])
    p_copies[OWN].wait_recv()
    near_finish(parts)
    share(0)
    parts = near_own([(0, 0), (0, 2), (2, 0)])
    more, total = near_sums(0)
    counts = counts + more
    sums[...] += total
    p_copies[0].wait_recv()
    near_finish(parts)
    share(1)
    parts = near_own([(1, 1), (0, 1), (1, 0), (2, 1), (1, 2)])
    take_far(0)
    take_far(1)
    p_copies[1].wait_recv()
    near_finish(parts)
    parts = far_own([2, 0, 1, 3, 4], (0, 1))
    p_copies[3].wait_recv()
    p_copies[4].wait_recv()
    far_finish(parts, (0, 1))
    take_far(2)
    parts = far_own([2, 0, 1, 3, 4, 5], (2,))
    p_copies[5].wait_recv()
    far_finish(parts, (2,))
    for kk in range(3):
        best = jnp.max(top_far[kk], axis=0, keepdims=True)
        if kk < 2:
            mine = jnp.broadcast_to(jnp.max(acc_far[kk], axis=1, keepdims=True), (ROOM // 2, 128))
            mine = jnp.concatenate([jnp.where(c == h, mine, -float(D)) for h in range(2)], axis=0)
            best = jnp.maximum(best, mine.T[0:1, :])
        far_out[kk, :, 0:128] = best * (1.0 / D)
        far_out[kk, :, 128:256] = over
    for kk, k in enumerate(FAR):
        there = FAR.index(NZ - k)
        for core in range(2):
            send(far_out.at[kk], far_z.at[c, there], us.at[core], ur.at[0], (at_z(k)[0], core))
    for g, (_, base, count) in enumerate(GROUPS):
        half = WIDTH[g] // 2
        pieces = []
        for h in range(-(-half // 128)):
            size = min(128, half - 128 * h)
            best = jnp.max(top[g, :, 128 * h:128 * h + size], axis=0, keepdims=True)
            pieces.append(jnp.broadcast_to(best, (128, size)).T)
        best = jnp.concatenate(pieces, axis=0)
        best = jnp.maximum(best, jnp.max(acc[g][...], axis=1, keepdims=True)) * (1.0 / D)
        for i in range(NXY // 2):
            column[i, base:base + count, :] = best[count * i:count * i + count, :]
    for i in range(NXY // 2):
        best_out[i] = jnp.where(last, over, column[i].T[0:1, :])

    def best_copy(i, other):
        jx, jy = 2 * c + i // 4, i % 4
        there = (z * 16 + ((x + jx) % 4) * 4 + (y + jy) % 4, 1 - c if other else c)
        return pltpu.make_async_remote_copy(
            best_out.at[i], ret1.at[8 * c + i], bs.at[int(other)], br.at[0],
            device_id=there, device_id_type=MESH)

    @pl.when(c == 0)
    def _():
        ret1[0] = best_out[0]

    @pl.when(c == 1)
    def _():
        best_copy(0, False).start()

    best_copy(0, True).start()
    for i in range(1, 8):
        best_copy(i, False).start()
        best_copy(i, True).start()

    more, total = near_sums(1)
    counts = counts + more
    for kk in range(3):
        more, part = member_sums(ik_far[kk], z_far[kk])
        counts = counts + more
        total = total + part
    cent_load.wait()
    mass_load.wait()
    number = jnp.sum(counts, axis=1, keepdims=True)
    mass = jnp.broadcast_to(mass_v[...], (128, CLUSTERS)).T[:, 0:1]
    cent[...] = (mass * cent[...] + (sums[...] + total)) / (mass + number)
    nc_copy = pltpu.make_async_copy(cent, nc_ref, local_sem.at[2])
    nc_copy.start()

    arrived(far_z, ur.at[0])
    lane16 = lax.broadcasted_iota(jnp.int32, (NXY, 128), 1)
    got = jnp.zeros((NXY, 128), jnp.float32)
    for kk in range(3):
        line = jnp.maximum(far_z[0, kk][:, 0:128], far_z[1, kk][:, 0:128])
        line = jnp.broadcast_to(line, (8, 128))
        found = jnp.concatenate(
            [jnp.take_along_axis(line, back_at[8 * h:8 * h + 8, :], axis=1, mode="promise_in_bounds") for h in range(2)],
            axis=0)
        got = jnp.where(lane16 >= kk * CAP, found, got)
    far_over = far_z[0, 0][:, 128:256]
    for h in range(2):
        for kk in range(3):
            far_over = jnp.maximum(far_over, far_z[h, kk][:, 128:256])
    got = jnp.where(lane16 == 127, far_over, got)
    for j in AROUND:
        if j == 0:
            far_ret[0] = got[0:1, :]
        else:
            back_out[j] = got[j:j + 1, :]
            send(back_out.at[j], far_ret.at[neg(j)], ts.at[0], tr.at[0], at_xy(j))
    @pl.when(c == 0)
    def _():
        arrived(ret1.at[others], br.at[0])

    @pl.when(c == 1)
    def _():
        arrived(ret1, br.at[0])

    back = {}
    for k in (2, 6, 1, 7):
        back[NZ - k] = send(
            ret1, ret2.at[POS[NZ - k]], fs.at[POS[k]], fr.at[POS[NZ - k]], at_z(k))
    tile_t = tiles_i[0]
    lane_t = tiles_i[1]
    result = jnp.zeros((8, 128), jnp.float32)
    flag = jnp.zeros((1, 128), jnp.float32)

    def pick(line, tile, result, flag):
        got = jnp.take_along_axis(jnp.broadcast_to(line, (8, 128)), lane_t, axis=1, mode="promise_in_bounds")
        return jnp.where(tile_t == tile, got, result), jnp.maximum(flag, jnp.where(last, line, 0.0))

    for j in range(NXY):
        result, flag = pick(ret1[j], j, result, flag)
    for k in NEAR:
        back[k].wait_recv()
        for j in range(NXY):
            result, flag = pick(ret2[POS[k], j], k * NXY + j, result, flag)
    arrived(far_ret.at[others], tr.at[0])
    for d in range(NXY):
        result, flag = pick(far_ret[d], NZ * NXY + d, result, flag)
    for b in range(ROWS // 128):
        best_ref[:, 128 * b:128 * b + 128] = result[b:b + 1, :]
    flag_ref[0, 0] = jnp.max(flag).astype(jnp.int32)

    @pl.when(c == 0)
    def _():
        sent(best_out.at[pl.ds(1, 7)], bs.at[0])

    @pl.when(c == 1)
    def _():
        sent(best_out, bs.at[0])

    sent(best_out, bs.at[1])
    for copy in list(back.values()) + list(p_copies.values()):
        copy.wait_send()
    sent(zout, zs.at[0])
    sent(mout, ms.at[0])
    for e in range(2):
        sent(xout[e].at[others], xs.at[e])
        sent(fout[e].at[others], ws.at[e])
        sent(far_out, us.at[e])
    sent(fid_out.at[others], vs.at[0])
    sent(idout.at[others], ids_s.at[0])
    sent(back_out.at[others], ts.at[0])
    nc_copy.wait()


def compact(embeddings, cluster_id, centroids, cluster_mass):
    vmem = pl.BlockSpec(memory_space=pltpu.VMEM)
    anywhere = pl.BlockSpec(memory_space=pl.ANY)
    f32, bf16, i32 = jnp.float32, jnp.bfloat16, jnp.int32
    dma = pltpu.SemaphoreType.DMA
    line = (1, 128)
    return pl.pallas_call(
        exchange_kernel,
        out_shape=(
            jax.ShapeDtypeStruct((1, ROWS), f32),
            jax.ShapeDtypeStruct((CLUSTERS, HALF), f32),
            jax.ShapeDtypeStruct((1, 1), i32),
        ),
        in_specs=[anywhere, anywhere, anywhere, anywhere],
        out_specs=(vmem, anywhere, pl.BlockSpec(memory_space=pltpu.SMEM)),
        scratch_shapes=[
            pltpu.VMEM((ROWS, HALF), f32),
            pltpu.VMEM((ROWS, HALF), bf16),
            pltpu.VMEM((1, ROWS), f32),
            pltpu.VMEM((1, ROWS), f32),
            pltpu.VMEM((NZ - 1, ROOM, HALF), bf16),
            pltpu.VMEM((len(NEAR), ROOM, HALF), bf16),
            pltpu.VMEM((3, ROOM, HALF), bf16),
            pltpu.VMEM((3, ROOM, HALF), bf16),
            pltpu.VMEM((NZ - 1, 8, 128), f32),
            pltpu.VMEM((NZ - 1, 8, 128), f32),
            *[pltpu.VMEM((NXY, count, HALF), bf16) for _, _, count in GROUPS[:OWN]],
            pltpu.VMEM((NXY, *line), f32),
            *[pltpu.VMEM((NXY, far[2], HALF), bf16) for far in FAR_SETS],
            *[pltpu.VMEM((NXY, far[2], HALF), bf16) for far in FAR_SETS],
            pltpu.VMEM((NXY, FAR_SETS[1][2], HALF), bf16),
            pltpu.VMEM((NXY, *line), f32),
            pltpu.VMEM((NXY, *line), f32),
            *[pltpu.VMEM((NXY, count, HALF), bf16) for _, _, count in GROUPS[:OWN]],
            *[pltpu.VMEM((NXY, count, HALF), bf16) for _, _, count in GROUPS[:OWN]],
            pltpu.VMEM((NXY, *line), f32),
            *[pltpu.VMEM((NXY * count, 128), f32) for _, _, count in GROUPS],
            pltpu.VMEM((3, 128, 128), f32),
            pltpu.VMEM((3, 8, 256), f32),
            pltpu.VMEM((3, 8, 256), f32),
            *[pltpu.VMEM((width // 2, 128), f32) for width in WIDTH],
            pltpu.VMEM((2, ROOM // 2, 128), f32),
            pltpu.VMEM((3, 8, 128), f32),
            pltpu.VMEM((CLUSTERS, HALF), f32),
            pltpu.VMEM((2, 8, 128), i32),
            pltpu.VMEM((8, 128, 128), f32),
            pltpu.VMEM((8, *line), f32),
            pltpu.VMEM((3, 1, 256), f32),
            pltpu.VMEM((NXY, *line), f32),
            pltpu.VMEM((len(NEAR), NXY, *line), f32),
            pltpu.VMEM((2, 3, 1, 256), f32),
            pltpu.VMEM((NXY, *line), f32),
            pltpu.VMEM((NXY, *line), f32),
            pltpu.VMEM((CLUSTERS, HALF), f32),
            pltpu.VMEM((ROWS,), i32),
            pltpu.VMEM((1, CLUSTERS), f32),
            dma((5,)), dma((2,)), dma((1,)), dma((5,)), dma((1,)), dma((4,)), dma((2,)), dma((2,)),
            dma((1,)), dma((1,)), dma((6,)), dma((6,)), dma((2,)), dma((1,)), dma((4,)), dma((4,)),
            dma((2,)), dma((2,)), dma((1,)), dma((1,)), dma((2,)), dma((1,)), dma((1,)), dma((1,)),
        ],
        compiler_params=pltpu.CompilerParams(
            collective_id=0, has_side_effects=True, vmem_limit_bytes=48 * 2**20),
    )(embeddings, cluster_id, centroids, cluster_mass.reshape(1, CLUSTERS))


def from_partner(value):
    return lax.ppermute(value, "mp", [(0, 1), (1, 0)])


def general(embeddings, cluster_id, centroids, cluster_mass):
    owners = lax.axis_size("dp")
    row_count = embeddings.shape[0]
    slot_count = 2 * row_count
    capacity = slot_count // owners
    cluster_count = centroids.shape[0]
    core = lax.axis_index("mp")
    squares = jnp.sum(embeddings * embeddings, axis=1)
    squares = squares + from_partner(squares)
    unit = (embeddings * lax.rsqrt(squares / D + 1e-06)[:, None]).astype(jnp.bfloat16)
    owner = cluster_id // cluster_count
    local = cluster_id - owner * cluster_count
    owner_hot = (owner[:, None] == jnp.arange(owners, dtype=jnp.int32)[None, :]).astype(jnp.bfloat16)
    row_index = jnp.arange(row_count, dtype=jnp.int32)
    lower = (row_index[:, None] >= row_index[None, :]).astype(jnp.bfloat16)
    running = jnp.dot(lower, owner_hot, preferred_element_type=jnp.float32)
    rank = jnp.sum(running * owner_hot.astype(jnp.float32), axis=1).astype(jnp.int32) - 1
    slot = owner * capacity + rank
    slot_index = jnp.arange(slot_count, dtype=jnp.int32)
    placed = slot_index[:, None] == slot[None, :]
    outgoing = jnp.dot(
        placed.astype(jnp.bfloat16), unit, preferred_element_type=jnp.float32
    ).astype(jnp.bfloat16)
    out_ids = jnp.max(jnp.where(placed, local[None, :] + 1, 0), axis=1) - 1
    incoming = lax.all_to_all(outgoing, "dp", split_axis=0, concat_axis=0, tiled=True)
    in_ids = lax.all_to_all(out_ids, "dp", split_axis=0, concat_axis=0, tiled=True)
    member = (jnp.arange(cluster_count, dtype=jnp.int32)[:, None] == in_ids[None, :]).astype(jnp.bfloat16)
    sums = jnp.dot(member, incoming, preferred_element_type=jnp.float32)
    counts = jnp.sum(member.astype(jnp.float32), axis=1)
    new_centroids = (cluster_mass[:, None] * centroids + sums) / (cluster_mass + counts)[:, None]
    half = slot_count // 2
    start = core * half
    contract = (((1,), (1,)), ((), ()))
    other = from_partner(incoming)
    scores = lax.dot_general(
        lax.dynamic_slice_in_dim(incoming, start, half, 0), incoming, contract, preferred_element_type=jnp.float32)
    scores = scores + lax.dot_general(
        lax.dynamic_slice_in_dim(other, start, half, 0), other, contract, preferred_element_type=jnp.float32)
    scores = scores / D
    query_ids = lax.dynamic_slice_in_dim(in_ids, start, half, 0)
    query_pos = start + jnp.arange(half, dtype=jnp.int32)
    same = (
        (query_ids[:, None] == in_ids[None, :])
        & (query_ids[:, None] >= 0)
        & (query_pos[:, None] != slot_index[None, :])
    )
    best = jnp.max(jnp.where(same, scores, -1.0), axis=1)
    best_p = from_partner(best)
    low, high = jnp.where(core == 0, best, best_p), jnp.where(core == 0, best_p, best)
    returned = lax.all_to_all(
        jnp.concatenate([low, high]), "dp", split_axis=0, concat_axis=0, tiled=True)
    return jnp.take(returned, slot), new_centroids


def shards(embeddings, cluster_id, centroids, cluster_mass):
    best, new_centroids, flag = compact(embeddings, cluster_id, centroids, cluster_mass)
    return lax.cond(
        flag[0, 0] > 0,
        lambda *args: general(*args),
        lambda *args: (best.reshape(ROWS), new_centroids),
        embeddings, cluster_id, centroids, cluster_mass,
    )


def solution(mesh):
    in_specs = (P("dp", "mp"), P("dp"), P("dp", "mp"), P("dp"))
    out_specs = (P("dp"), P("dp", "mp"))
    return jax.shard_map(shards, mesh=mesh, in_specs=in_specs, out_specs=out_specs, check_vma=False)
```

```python
import functools

import jax
import jax.numpy as jnp
from jax import lax
from jax.experimental import pallas as pl
from jax.experimental.pallas import tpu as pltpu
from jax.sharding import PartitionSpec as P

D = 1024
HALF = 512
ROWS = 768
CLUSTERS = 256
CAP = 12
ROOM = 128
NZ = 8
NXY = 16
GROUPS = (((1, 7), 0, 24), ((2, 6), 24, 24), ((None, 0), 48, 24))
LANE = {k: base + CAP * m for members, base, _ in GROUPS for m, k in enumerate(members) if k is not None}
OWN = 2
FAR = (3, 5, 4)
FAR_SETS = (((3, 5), 0, 24), ((4,), 2, 24))
WIDTH = tuple(count * NXY for _, _, count in GROUPS)
MESH = pl.DeviceIdType.MESH
NT = (((1,), (1,)), ((), ()))
NEAR = (1, 7, 2, 6)
AROUND = (10, 9, 11, 6, 14, 2, 8, 5, 7, 13, 15, 1, 3, 4, 12, 0)
POS = {k: i for i, k in enumerate(NEAR + FAR)}


def neg(d):
    return ((4 - d // 4) % 4) * 4 + (4 - d % 4) % 4


def hot(mask):
    return jnp.where(mask, 1.0, 0.0).astype(jnp.bfloat16)


def exchange_kernel(
    emb_ref, cid_ref, cent_ref, mass_ref,
    best_ref, nc_ref, flag_ref,
    emb, unit, sq_mine, sq_peer, zout, zin, z_far, z_far_p, mout, min_, xo0, xo1, idout, fo0, fo1, fi0, fi1, fi1_p, fid_out, fid_in,
    r0, r1, p0, p1, idin, ik0, ik1, ik2, ik_far, top, idq, acc0, acc1, acc2, acc_far, top_far, sums,
    tiles_i, column, best_out, far_out, ret1, ret2, far_z, back_out, far_ret, cent, cid_v, mass_v,
    local_sem, sq_sem, zs, zr, ms, mr, xs, xr, ids_s, ids_r, ps, pr, bs, br, fs, fr,
    ws, wr, vs, vr, us, ur, ts, tr,
):
    xout, rows, rows_p, idkey = (xo0, xo1), (r0, r1, fi1), (p0, p1, fi1_p), (ik0, ik1, ik2)
    fout, fin, acc = (fo0, fo1), (fi0, fi1), (acc0, acc1, acc2)
    me = lax.axis_index("dp")
    c = lax.axis_index("mp")
    z, x, y = me // 16, (me // 4) % 4, me % 4

    def at_z(k):
        return (((z + k) % NZ) * 16 + x * 4 + y, c)

    def at_xy(d):
        return (z * 16 + ((x + d // 4) % 4) * 4 + (y + d % 4) % 4, c)

    partner = (me, 1 - c)

    def send(src, dst, send_sem, recv_sem, to):
        copy = pltpu.make_async_remote_copy(src, dst, send_sem, recv_sem, device_id=to, device_id_type=MESH)
        copy.start()
        return copy

    def sent(ref, sem):
        pltpu.make_async_remote_copy(ref, ref, sem, sem, device_id=partner, device_id_type=MESH).wait_send()

    def arrived(ref, sem):
        pltpu.make_async_remote_copy(ref, ref, sem, sem, device_id=partner, device_id_type=MESH).wait_recv()

    others = pl.ds(1, NXY - 1)

    cid_load = pltpu.make_async_copy(cid_ref, cid_v, local_sem.at[3])
    cid_load.start()
    mass_load = pltpu.make_async_copy(mass_ref, mass_v, local_sem.at[4])
    mass_load.start()
    load = pltpu.make_async_copy(emb_ref, emb, local_sem.at[0])
    load.start()
    cent_load = pltpu.make_async_copy(cent_ref, cent, local_sem.at[1])
    cent_load.start()
    barrier = pltpu.get_barrier_semaphore()
    for k in FAR[::-1]:
        pl.semaphore_signal(barrier, inc=1, device_id=at_z(k), device_id_type=MESH)
        pl.semaphore_signal(barrier, inc=1, device_id=(at_z(k)[0], 1 - c), device_id_type=MESH)
    for d in AROUND[:-1]:
        pl.semaphore_signal(barrier, inc=1, device_id=at_xy(d), device_id_type=MESH)
        pl.semaphore_signal(barrier, inc=1, device_id=(at_xy(d)[0], 1 - c), device_id_type=MESH)
    for k in NEAR:
        pl.semaphore_signal(barrier, inc=1, device_id=at_z(k), device_id_type=MESH)
    pl.semaphore_signal(barrier, inc=1, device_id=partner, device_id_type=MESH)

    cid_load.wait()
    cid = cid_v[...].reshape(1, ROWS)
    owner = cid >> 8
    dz = ((owner >> 4) - z) & 7
    dxy = ((((owner >> 2) & 3) - x) & 3) * 4 + (((owner & 3) - y) & 3)
    target = dz * 16 + dxy
    lane128 = lax.broadcasted_iota(jnp.int32, (128, 128), 1)
    sub128 = lax.broadcasted_iota(jnp.int32, (128, 128), 0)
    upto = hot(sub128 <= lane128)
    sub8 = lax.broadcasted_iota(jnp.int32, (8, 128), 0)
    sub16 = lax.broadcasted_iota(jnp.int32, (NXY, 128), 0)
    last = lax.broadcasted_iota(jnp.int32, (1, 128), 1) == 127
    base_t = jnp.zeros((128, 128), jnp.float32)
    base_z = jnp.zeros((8, 128), jnp.float32)
    ranks, places = [], []
    for b in range(ROWS // 128):
        cut = slice(128 * b, 128 * b + 128)
        is_t = sub128 == target[:, cut]
        is_z = sub8 == dz[:, cut]
        run_t = base_t + jnp.dot(hot(is_t), upto, preferred_element_type=jnp.float32)
        run_z = base_z + jnp.dot(hot(is_z), upto, preferred_element_type=jnp.float32)
        ranks.append(jnp.sum(jnp.where(is_t, run_t, 0.0), axis=0, keepdims=True) - 1.0)
        places.append(jnp.sum(jnp.where(is_z, run_z, 0.0), axis=0, keepdims=True) - 1.0)
        base_t = jnp.broadcast_to(run_t[:, 127:128], (128, 128))
        base_z = jnp.broadcast_to(run_z[:, 127:128], (8, 128))
    near_most = jnp.where((sub8 == 1) | (sub8 == 2) | (sub8 > 5), base_z, 0.0)
    over = jnp.where(jnp.max(near_most, axis=0, keepdims=True) > float(ROOM), 1.0, 0.0)
    rank_f = jnp.concatenate(ranks, axis=1)
    rank = rank_f.astype(jnp.int32)
    place = jnp.concatenate(places, axis=1).astype(jnp.int32)
    slot = jnp.where(place < ROOM, dz * ROOM + place, -1)
    far_row = (dz >= 3) & (dz <= 5)
    far_lane = jnp.where(dz == 3, rank, jnp.where(dz == 5, rank + CAP, rank + 2 * CAP))
    far_lane = jnp.where(far_row, far_lane, jnp.where(dz == 0, rank + 3 * CAP, -1))
    far_slot = (
        jnp.where((dz == 3) | (dz == 5), dxy * FAR_SETS[0][2] + far_lane, -1),
        jnp.where((dz == 4) | (dz == 0), dxy * FAR_SETS[1][2] + far_lane - 2 * CAP, -1),
    )
    turned = ((4 - (dxy >> 2)) & 3) * 4 + ((4 - (dxy & 3)) & 3)
    tile_of = jnp.where(far_row, NZ * NXY + dxy, dz * NXY + turned)
    lane_of = jnp.where(far_row, far_lane, rank)
    for k in (0,) + NEAR:
        lane_of = jnp.where(dz == k, rank + LANE[(NZ - k) % NZ], lane_of)
    tiles_i[...] = jnp.zeros_like(tiles_i)
    for b in range(ROWS // 128):
        cut = slice(128 * b, 128 * b + 128)
        tiles_i[0, b:b + 1, :] = tile_of[:, cut]
        tiles_i[1, b:b + 1, :] = lane_of[:, cut]
    row8 = lax.broadcasted_iota(jnp.int32, (8, ROWS), 0)
    local = ((cid & 255) + 1).astype(jnp.float32)
    values = jnp.where(
        row8 == 0, local,
        jnp.where(row8 == 1, dxy.astype(jnp.float32), jnp.where(row8 == 2, rank_f, 0.0)),
    ).astype(jnp.bfloat16)

    load.wait()
    squares = jnp.zeros((ROWS, 128), jnp.float32)
    for f in range(HALF // 128):
        part = emb[:, 128 * f:128 * f + 128]
        squares = squares + part * part
    mine = jnp.sum(squares.T, axis=0, keepdims=True)
    sq_mine[...] = mine
    pl.semaphore_wait(barrier, NZ - 1 + 2 * (NXY - 1) + len(FAR) + 1)
    sq_copy = send(sq_mine, sq_peer, sq_sem.at[0], sq_sem.at[1], partner)

    place_hot = {}
    for k in NEAR:
        want = lax.broadcasted_iota(jnp.int32, (ROOM, ROWS), 0) + k * ROOM
        place_hot[k] = hot(want == slot)
    far_hot = [
        hot(lax.broadcasted_iota(jnp.int32, (NXY * count, ROWS), 0) == far_slot[e])
        for e, (_, _, count) in enumerate(FAR_SETS)
    ]

    sq_copy.wait()
    scale = lax.rsqrt((sq_mine[...] + sq_peer[...]) / D + 1e-06)
    scale = jnp.broadcast_to(scale, (128, ROWS)).T
    for f in range(HALF // 128):
        unit[:, 128 * f:128 * f + 128] = (emb[:, 128 * f:128 * f + 128] * scale).astype(jnp.bfloat16)

    def pack(k):
        packed = jnp.dot(place_hot[k], unit[...], preferred_element_type=jnp.float32).astype(jnp.bfloat16)
        zout[POS[k]] = packed
        send(zout.at[POS[k]], zin.at[POS[NZ - k]], zs.at[0], zr.at[0 if k in (1, 7) else 1], at_z(k))

    pack(1)
    pack(7)
    left = jnp.where(
        (far_row | (dz == 0)) & (lax.broadcasted_iota(jnp.int32, (NXY, ROWS), 0) == dxy), local, 0.0).astype(jnp.bfloat16)
    right = hot(lax.broadcasted_iota(jnp.int32, (128, ROWS), 0) == far_lane)
    ids = lax.dot_general(left, right, NT, preferred_element_type=jnp.float32)
    for d in AROUND:
        if d == 0:
            fid_in[0] = ids[0:1, :]
        else:
            fid_out[d] = ids[d:d + 1, :]
            send(fid_out.at[d], fid_in.at[neg(d)], vs.at[0], vr.at[0], at_xy(d))

    def pack_far(e):
        count = FAR_SETS[e][2]
        packed = jnp.dot(far_hot[e], unit[...], preferred_element_type=jnp.float32)
        for d in AROUND:
            block = packed[count * d:count * d + count, :].astype(jnp.bfloat16)
            if d == 0:
                fin[e][0] = block
            else:
                fout[e][d] = block
                send(fout[e].at[d], fin[e].at[neg(d)], ws.at[e], wr.at[e], at_xy(d))

    pack_far(0)
    for k in NEAR:
        meta = lax.dot_general(values, place_hot[k], NT, preferred_element_type=jnp.float32)
        mout[POS[k]] = meta
        send(mout.at[POS[k]], min_.at[POS[NZ - k]], ms.at[0], mr.at[0], at_z(k))
    pack(2)
    pack(6)
    pack_far(1)

    p_copies = {}

    def forward(g):
        members, _, count = GROUPS[g]
        total = None
        for m, k in enumerate(members):
            meta = min_[POS[k]]
            valid = meta[0:1, :] > 0.5
            there = jnp.where(valid, meta[1:2, :] * float(count) + meta[2:3, :] + float(CAP * m), -1.0)
            there = there.astype(jnp.int32)
            want = lax.broadcasted_iota(jnp.int32, (NXY * count, ROOM), 0)
            if m == 0:
                arrived(zin.at[pl.ds(2 * g, 2)], zr.at[g])
            part = jnp.dot(hot(want == there), zin[POS[k]], preferred_element_type=jnp.float32)
            total = part if total is None else total + part
        for d in AROUND:
            block = total[count * d:count * d + count, :].astype(jnp.bfloat16)
            if d == 0:
                rows[g][0] = block
            else:
                xout[g][d] = block
                send(xout[g].at[d], rows[g].at[neg(d)], xs.at[g], xr.at[g], at_xy(d))

    def share(g):
        arrived(rows[g].at[others], xr.at[g])
        p_copies[g] = send(rows[g], rows_p[g], ps.at[g], pr.at[g], partner)

    def share_far(kk):
        arrived(z_far.at[kk], zr.at[2 + kk])
        p_copies[3 + kk] = send(z_far.at[kk], z_far_p.at[kk], ps.at[3 + kk], pr.at[3 + kk], partner)

    arrived(fid_in.at[others], vr.at[0])
    known = jnp.concatenate([fid_in[j] for j in range(NXY)], axis=0).astype(jnp.bfloat16)
    back_at = jnp.zeros((NXY, 128), jnp.float32)
    far_values, far_places = [], []
    for planes, first, count in FAR_SETS:
        width = NXY * count
        flat = lax.broadcasted_iota(jnp.int32, (1, width), 1)
        holder = (flat * 2731) >> 16
        within = flat - holder * count
        lane = jnp.where(within < CAP * len(planes), within + CAP * first, -1)
        spread = hot(lax.broadcasted_iota(jnp.int32, (128, width), 0) == lane)
        mine16 = lax.broadcasted_iota(jnp.int32, (NXY, width), 0) == holder
        far_ids = jnp.dot(known, spread, preferred_element_type=jnp.float32)
        far_ids = jnp.sum(jnp.where(mine16, far_ids, 0.0), axis=0, keepdims=True)
        low = lax.broadcasted_iota(jnp.int32, (8, width), 0) * CAP
        inside = (within >= low) & (within < low + CAP) & (low < CAP * len(planes)) & (far_ids > 0.5)
        base_f = jnp.zeros((8, 128), jnp.float32)
        runs = []
        for b in range(width // 128):
            run = base_f + jnp.dot(hot(inside[:, 128 * b:128 * b + 128]), upto, preferred_element_type=jnp.float32)
            runs.append(run)
            base_f = jnp.broadcast_to(run[:, 127:128], (8, 128))
        over = jnp.maximum(over, jnp.where(jnp.max(base_f, axis=0, keepdims=True) > float(ROOM), 1.0, 0.0))
        far_place = jnp.where(inside, jnp.concatenate(runs, axis=1) - 1.0, -1.0)
        far_place = jnp.where(far_place < float(ROOM), far_place, -1.0)
        any_place = jnp.maximum(jnp.max(far_place, axis=0, keepdims=True), 0.0)
        back_at = back_at + lax.dot_general(
            jnp.where(mine16, any_place, 0.0).astype(jnp.bfloat16), spread, NT, preferred_element_type=jnp.float32)
        far_values.append(jnp.broadcast_to(far_ids, (8, width)).astype(jnp.bfloat16))
        far_places.append(far_place)
    back_at = back_at.astype(jnp.int32)

    def relay_far(e):
        planes, _, count = FAR_SETS[e]
        width = NXY * count
        chosen = []
        for m, k in enumerate(planes):
            want = lax.broadcasted_iota(jnp.int32, (ROOM, width), 0).astype(jnp.float32)
            chosen.append(hot(want == far_places[e][m:m + 1, :]))
            mout[POS[k]] = lax.dot_general(far_values[e], chosen[m], NT, preferred_element_type=jnp.float32)
            there = FAR.index(NZ - k)
            send(mout.at[POS[k]], min_.at[POS[NZ - k]], ms.at[0], mr.at[1 + there], at_z(k))
        arrived(fin[e].at[others], wr.at[e])
        for m, k in enumerate(planes):
            zout[POS[k]] = jnp.dot(
                chosen[m], fin[e][...].reshape(width, HALF), preferred_element_type=jnp.float32).astype(jnp.bfloat16)
            there = FAR.index(NZ - k)
            send(zout.at[POS[k]], z_far.at[there], zs.at[0], zr.at[2 + there], at_z(k))

    arrived(min_.at[pl.ds(0, 4)], mr.at[0])
    ids = jnp.zeros((NXY, 128), jnp.float32)
    for k in NEAR:
        meta = min_[POS[k]]
        valid = meta[0:1, :] > 0.5
        to = jnp.where(valid, meta[1:2, :], -1.0).astype(jnp.int32)
        place_k = meta[2:3, :].astype(jnp.int32) + LANE[k]
        left = jnp.where(sub16 == to, meta[0:1, :], 0.0).astype(jnp.bfloat16)
        ids = ids + lax.dot_general(left, hot(sub128 == place_k), NT, preferred_element_type=jnp.float32)
    for d in AROUND:
        if d == 0:
            idin[0] = ids[0:1, :]
        else:
            idout[d] = ids[d:d + 1, :]
            send(idout.at[d], idin.at[neg(d)], ids_s.at[0], ids_r.at[0], at_xy(d))

    forward(0)
    relay_far(0)

    forward(1)
    relay_far(1)

    p_copies[OWN] = send(rows[OWN], rows_p[OWN], ps.at[OWN], pr.at[OWN], partner)
    arrived(idin.at[others], ids_r.at[0])
    for j in range(NXY):
        line = idin[j]
        line = jnp.where(line < 0.5, -1.0, line)
        turned = jnp.broadcast_to(line, (128, 128)).T
        for g, (_, base, count) in enumerate(GROUPS[:OWN]):
            idkey[g][count * j:count * j + count, :] = turned[base:base + count, :]
        line = fid_in[j]
        line = jnp.where((line < 0.5) | (lane128[0:1, :] < 3 * CAP), -1.0, line)
        idkey[OWN][24 * j:24 * j + 24, :] = jnp.broadcast_to(line, (128, 128)).T[2 * CAP:4 * CAP, :]
    for g in range(3):
        half = WIDTH[g] // 2
        for h in range(-(-half // 128)):
            size = min(128, half - 128 * h)
            block = idkey[g][pl.ds(pl.multiple_of(half * c + 128 * h, 8), size), :]
            idq[g, :, 128 * h:128 * h + size] = block.T[0:8, :]
    for ref in (top, top_far, acc0, acc1, acc2, acc_far):
        ref[...] = jnp.full(ref.shape, -float(D), jnp.float32)
    sub256 = lax.broadcasted_iota(jnp.int32, (CLUSTERS, 128), 0).astype(jnp.float32) + 1.0

    def member_sums(source, key):
        seen = jnp.zeros((CLUSTERS, 128), jnp.float32)
        parts = []
        for h in range(key.shape[0] // 128):
            line = source[128 * h:128 * h + 128, :].T[0:1, :]
            member = jnp.where(sub256 == line, 1.0, 0.0)
            seen = seen + member
            parts.append(member.astype(jnp.bfloat16))
        member = jnp.concatenate(parts, axis=1) if len(parts) > 1 else parts[0]
        return seen, jnp.dot(member, key, preferred_element_type=jnp.float32)

    def near_sums(g):
        return member_sums(idkey[g], rows[g][...].reshape(WIDTH[g], HALF))

    def keys_of(g):
        return rows[g][...].reshape(WIDTH[g], HALF), rows_p[g][...].reshape(WIDTH[g], HALF)

    def own_half(g):
        half = WIDTH[g] // 2
        first = pl.ds(pl.multiple_of(NXY // 2 * c, 8), NXY // 2)
        return rows[g][first].reshape(half, HALF), rows_p[g][first].reshape(half, HALF)

    def nt(a, b):
        return lax.dot_general(a, b, NT, preferred_element_type=jnp.float32)

    def near_own(pairs):
        return [(pair, nt(keys_of(pair[0])[0], own_half(pair[1])[0])) for pair in pairs]

    def near_finish(parts):
        for (kg, qg), part in parts:
            nk, nq = WIDTH[kg], WIDTH[qg] // 2
            scores = part + nt(keys_of(kg)[1], own_half(qg)[1])
            for h in range(-(-nq // 128)):
                cut = slice(128 * h, min(128 * h + 128, nq))
                size = cut.stop - cut.start
                same = idkey[kg][...][:, :size] == idq[qg, 0:1, cut]
                if kg == qg:
                    apart = (lax.broadcasted_iota(jnp.int32, (nk, size), 0)
                             - lax.broadcasted_iota(jnp.int32, (nk, size), 1))
                    same = same & (apart != nq * c + 128 * h)
                kept = jnp.where(same, scores[:, cut], -float(D))
                top[qg, :, cut] = jnp.maximum(top[qg, :, cut], jnp.max(kept.reshape(nk // 8, 8, size), axis=0))

    half_far = pl.ds(pl.multiple_of(ROOM // 2 * c, ROOM // 2), ROOM // 2)

    def side(g):
        if g < 3:
            return own_half(g)
        return z_far[g - 3, half_far, :], z_far_p[g - 3, half_far, :]

    def far_own(groups, planes):
        columns = z_far[planes[0]:planes[0] + len(planes)].reshape(ROOM * len(planes), HALF)
        return [(g, nt(side(g)[0], columns)) for g in groups]

    def far_finish(parts, planes):
        first = planes[0]
        columns = z_far_p[first:first + len(planes)].reshape(ROOM * len(planes), HALF)
        for g, part in parts:
            scores = part + nt(side(g)[1], columns)
            n = scores.shape[0]
            if g < 3:
                mine = idkey[g][pl.ds(pl.multiple_of(n * c, 8), n), :]
            else:
                mine = ik_far[g - 3, half_far, :]
            for kk in planes:
                line = min_[POS[FAR[kk]]][0:1, :]
                same = mine == line
                if g == 3 + kk:
                    apart = (lax.broadcasted_iota(jnp.int32, (n, ROOM), 1)
                             - lax.broadcasted_iota(jnp.int32, (n, ROOM), 0))
                    same = same & (apart != n * c)
                kept = jnp.where(same, scores[:, ROOM * (kk - first):ROOM * (kk - first) + ROOM], -float(D))
                top_far[kk] = jnp.maximum(top_far[kk], jnp.max(kept.reshape(n // 8, 8, ROOM), axis=0))
                if g < 3:
                    acc[g][...] = jnp.maximum(acc[g][...], kept)
                elif g - 3 < first:
                    acc_far[g - 3] = jnp.maximum(acc_far[g - 3], kept)

    def take_far(kk):
        arrived(min_.at[POS[FAR[kk]]], mr.at[1 + kk])
        line = min_[POS[FAR[kk]]][0:1, :]
        ik_far[kk] = jnp.broadcast_to(jnp.where(line < 0.5, -1.0, line), (128, 128)).T
        share_far(kk)

    counts, total = near_sums(OWN)
    sums[...] = total
    parts = near_own([(2, 2)])
    p_copies[OWN].wait_recv()
    near_finish(parts)
    share(0)
    parts = near_own([(0, 0), (0, 2), (2, 0)])
    more, total = near_sums(0)
    counts = counts + more
    sums[...] += total
    p_copies[0].wait_recv()
    near_finish(parts)
    share(1)
    parts = near_own([(1, 1), (0, 1), (1, 0), (2, 1), (1, 2)])
    take_far(0)
    take_far(1)
    p_copies[1].wait_recv()
    near_finish(parts)
    parts = far_own([2, 0, 1, 3, 4], (0, 1))
    p_copies[3].wait_recv()
    p_copies[4].wait_recv()
    far_finish(parts, (0, 1))
    take_far(2)
    parts = far_own([2, 0, 1, 3, 4, 5], (2,))
    p_copies[5].wait_recv()
    far_finish(parts, (2,))
    for kk in range(3):
        best = jnp.max(top_far[kk], axis=0, keepdims=True)
        if kk < 2:
            mine = jnp.broadcast_to(jnp.max(acc_far[kk], axis=1, keepdims=True), (ROOM // 2, 128))
            mine = jnp.concatenate([jnp.where(c == h, mine, -float(D)) for h in range(2)], axis=0)
            best = jnp.maximum(best, mine.T[0:1, :])
        far_out[kk, :, 0:128] = best * (1.0 / D)
        far_out[kk, :, 128:256] = over
    for kk, k in enumerate(FAR):
        there = FAR.index(NZ - k)
        for core in range(2):
            send(far_out.at[kk], far_z.at[c, there], us.at[core], ur.at[0], (at_z(k)[0], core))
    for g, (_, base, count) in enumerate(GROUPS):
        half = WIDTH[g] // 2
        pieces = []
        for h in range(-(-half // 128)):
            size = min(128, half - 128 * h)
            best = jnp.max(top[g, :, 128 * h:128 * h + size], axis=0, keepdims=True)
            pieces.append(jnp.broadcast_to(best, (128, size)).T)
        best = jnp.concatenate(pieces, axis=0)
        best = jnp.maximum(best, jnp.max(acc[g][...], axis=1, keepdims=True)) * (1.0 / D)
        for i in range(NXY // 2):
            column[i, base:base + count, :] = best[count * i:count * i + count, :]
    for i in range(NXY // 2):
        best_out[i] = jnp.where(last, over, column[i].T[0:1, :])

    def best_copy(i, other):
        jx, jy = 2 * c + i // 4, i % 4
        there = (z * 16 + ((x + jx) % 4) * 4 + (y + jy) % 4, 1 - c if other else c)
        return pltpu.make_async_remote_copy(
            best_out.at[i], ret1.at[8 * c + i], bs.at[int(other)], br.at[0],
            device_id=there, device_id_type=MESH)

    @pl.when(c == 0)
    def _():
        ret1[0] = best_out[0]

    @pl.when(c == 1)
    def _():
        best_copy(0, False).start()

    best_copy(0, True).start()
    for i in range(1, 8):
        best_copy(i, False).start()
        best_copy(i, True).start()

    more, total = near_sums(1)
    counts = counts + more
    for kk in range(3):
        more, part = member_sums(ik_far[kk], z_far[kk])
        counts = counts + more
        total = total + part
    cent_load.wait()
    mass_load.wait()
    number = jnp.sum(counts, axis=1, keepdims=True)
    mass = jnp.broadcast_to(mass_v[...], (128, CLUSTERS)).T[:, 0:1]
    cent[...] = (mass * cent[...] + (sums[...] + total)) / (mass + number)
    nc_copy = pltpu.make_async_copy(cent, nc_ref, local_sem.at[2])
    nc_copy.start()

    arrived(far_z, ur.at[0])
    lane16 = lax.broadcasted_iota(jnp.int32, (NXY, 128), 1)
    got = jnp.zeros((NXY, 128), jnp.float32)
    for kk in range(3):
        line = jnp.maximum(far_z[0, kk][:, 0:128], far_z[1, kk][:, 0:128])
        line = jnp.broadcast_to(line, (8, 128))
        found = jnp.concatenate(
            [jnp.take_along_axis(line, back_at[8 * h:8 * h + 8, :], axis=1, mode="promise_in_bounds") for h in range(2)],
            axis=0)
        got = jnp.where(lane16 >= kk * CAP, found, got)
    far_over = far_z[0, 0][:, 128:256]
    for h in range(2):
        for kk in range(3):
            far_over = jnp.maximum(far_over, far_z[h, kk][:, 128:256])
    got = jnp.where(lane16 == 127, far_over, got)
    for j in AROUND:
        if j == 0:
            far_ret[0] = got[0:1, :]
        else:
            back_out[j] = got[j:j + 1, :]
            send(back_out.at[j], far_ret.at[neg(j)], ts.at[0], tr.at[0], at_xy(j))
    @pl.when(c == 0)
    def _():
        arrived(ret1.at[others], br.at[0])

    @pl.when(c == 1)
    def _():
        arrived(ret1, br.at[0])

    back = {}
    for k in (2, 6, 1, 7):
        back[NZ - k] = send(
            ret1, ret2.at[POS[NZ - k]], fs.at[POS[k]], fr.at[POS[NZ - k]], at_z(k))
    tile_t = tiles_i[0]
    lane_t = tiles_i[1]
    result = jnp.zeros((8, 128), jnp.float32)
    flag = jnp.zeros((1, 128), jnp.float32)

    def pick(line, tile, result, flag):
        got = jnp.take_along_axis(jnp.broadcast_to(line, (8, 128)), lane_t, axis=1, mode="promise_in_bounds")
        return jnp.where(tile_t == tile, got, result), jnp.maximum(flag, jnp.where(last, line, 0.0))

    for j in range(NXY):
        result, flag = pick(ret1[j], j, result, flag)
    for k in NEAR:
        back[k].wait_recv()
        for j in range(NXY):
            result, flag = pick(ret2[POS[k], j], k * NXY + j, result, flag)
    arrived(far_ret.at[others], tr.at[0])
    for d in range(NXY):
        result, flag = pick(far_ret[d], NZ * NXY + d, result, flag)
    for b in range(ROWS // 128):
        best_ref[:, 128 * b:128 * b + 128] = result[b:b + 1, :]
    flag_ref[0, 0] = jnp.max(flag).astype(jnp.int32)

    @pl.when(c == 0)
    def _():
        sent(best_out.at[pl.ds(1, 7)], bs.at[0])

    @pl.when(c == 1)
    def _():
        sent(best_out, bs.at[0])

    sent(best_out, bs.at[1])
    for copy in list(back.values()) + list(p_copies.values()):
        copy.wait_send()
    sent(zout, zs.at[0])
    sent(mout, ms.at[0])
    for e in range(2):
        sent(xout[e].at[others], xs.at[e])
        sent(fout[e].at[others], ws.at[e])
        sent(far_out, us.at[e])
    sent(fid_out.at[others], vs.at[0])
    sent(idout.at[others], ids_s.at[0])
    sent(back_out.at[others], ts.at[0])
    nc_copy.wait()


def compact(embeddings, cluster_id, centroids, cluster_mass):
    vmem = pl.BlockSpec(memory_space=pltpu.VMEM)
    anywhere = pl.BlockSpec(memory_space=pl.ANY)
    f32, bf16, i32 = jnp.float32, jnp.bfloat16, jnp.int32
    dma = pltpu.SemaphoreType.DMA
    line = (1, 128)
    return pl.pallas_call(
        exchange_kernel,
        out_shape=(
            jax.ShapeDtypeStruct((1, ROWS), f32),
            jax.ShapeDtypeStruct((CLUSTERS, HALF), f32),
            jax.ShapeDtypeStruct((1, 1), i32),
        ),
        in_specs=[anywhere, anywhere, anywhere, anywhere],
        out_specs=(vmem, anywhere, pl.BlockSpec(memory_space=pltpu.SMEM)),
        scratch_shapes=[
            pltpu.VMEM((ROWS, HALF), f32),
            pltpu.VMEM((ROWS, HALF), bf16),
            pltpu.VMEM((1, ROWS), f32),
            pltpu.VMEM((1, ROWS), f32),
            pltpu.VMEM((NZ - 1, ROOM, HALF), bf16),
            pltpu.VMEM((len(NEAR), ROOM, HALF), bf16),
            pltpu.VMEM((3, ROOM, HALF), bf16),
            pltpu.VMEM((3, ROOM, HALF), bf16),
            pltpu.VMEM((NZ - 1, 8, 128), f32),
            pltpu.VMEM((NZ - 1, 8, 128), f32),
            *[pltpu.VMEM((NXY, count, HALF), bf16) for _, _, count in GROUPS[:OWN]],
            pltpu.VMEM((NXY, *line), f32),
            *[pltpu.VMEM((NXY, far[2], HALF), bf16) for far in FAR_SETS],
            *[pltpu.VMEM((NXY, far[2], HALF), bf16) for far in FAR_SETS],
            pltpu.VMEM((NXY, FAR_SETS[1][2], HALF), bf16),
            pltpu.VMEM((NXY, *line), f32),
            pltpu.VMEM((NXY, *line), f32),
            *[pltpu.VMEM((NXY, count, HALF), bf16) for _, _, count in GROUPS[:OWN]],
            *[pltpu.VMEM((NXY, count, HALF), bf16) for _, _, count in GROUPS[:OWN]],
            pltpu.VMEM((NXY, *line), f32),
            *[pltpu.VMEM((NXY * count, 128), f32) for _, _, count in GROUPS],
            pltpu.VMEM((3, 128, 128), f32),
            pltpu.VMEM((3, 8, 256), f32),
            pltpu.VMEM((3, 8, 256), f32),
            *[pltpu.VMEM((width // 2, 128), f32) for width in WIDTH],
            pltpu.VMEM((2, ROOM // 2, 128), f32),
            pltpu.VMEM((3, 8, 128), f32),
            pltpu.VMEM((CLUSTERS, HALF), f32),
            pltpu.VMEM((2, 8, 128), i32),
            pltpu.VMEM((8, 128, 128), f32),
            pltpu.VMEM((8, *line), f32),
            pltpu.VMEM((3, 1, 256), f32),
            pltpu.VMEM((NXY, *line), f32),
            pltpu.VMEM((len(NEAR), NXY, *line), f32),
            pltpu.VMEM((2, 3, 1, 256), f32),
            pltpu.VMEM((NXY, *line), f32),
            pltpu.VMEM((NXY, *line), f32),
            pltpu.VMEM((CLUSTERS, HALF), f32),
            pltpu.VMEM((ROWS,), i32),
            pltpu.VMEM((1, CLUSTERS), f32),
            dma((5,)), dma((2,)), dma((1,)), dma((5,)), dma((1,)), dma((4,)), dma((2,)), dma((2,)),
            dma((1,)), dma((1,)), dma((6,)), dma((6,)), dma((2,)), dma((1,)), dma((4,)), dma((4,)),
            dma((2,)), dma((2,)), dma((1,)), dma((1,)), dma((2,)), dma((1,)), dma((1,)), dma((1,)),
        ],
        compiler_params=pltpu.CompilerParams(
            collective_id=0, has_side_effects=True, vmem_limit_bytes=48 * 2**20),
    )(embeddings, cluster_id, centroids, cluster_mass.reshape(1, CLUSTERS))


def from_partner(value):
    return lax.ppermute(value, "mp", [(0, 1), (1, 0)])


def general(embeddings, cluster_id, centroids, cluster_mass):
    owners = lax.axis_size("dp")
    row_count = embeddings.shape[0]
    slot_count = 2 * row_count
    capacity = slot_count // owners
    cluster_count = centroids.shape[0]
    core = lax.axis_index("mp")
    squares = jnp.sum(embeddings * embeddings, axis=1)
    squares = squares + from_partner(squares)
    unit = (embeddings * lax.rsqrt(squares / D + 1e-06)[:, None]).astype(jnp.bfloat16)
    owner = cluster_id // cluster_count
    local = cluster_id - owner * cluster_count
    owner_hot = (owner[:, None] == jnp.arange(owners, dtype=jnp.int32)[None, :]).astype(jnp.bfloat16)
    row_index = jnp.arange(row_count, dtype=jnp.int32)
    lower = (row_index[:, None] >= row_index[None, :]).astype(jnp.bfloat16)
    running = jnp.dot(lower, owner_hot, preferred_element_type=jnp.float32)
    rank = jnp.sum(running * owner_hot.astype(jnp.float32), axis=1).astype(jnp.int32) - 1
    slot = owner * capacity + rank
    slot_index = jnp.arange(slot_count, dtype=jnp.int32)
    placed = slot_index[:, None] == slot[None, :]
    outgoing = jnp.dot(
        placed.astype(jnp.bfloat16), unit, preferred_element_type=jnp.float32
    ).astype(jnp.bfloat16)
    out_ids = jnp.max(jnp.where(placed, local[None, :] + 1, 0), axis=1) - 1
    incoming = lax.all_to_all(outgoing, "dp", split_axis=0, concat_axis=0, tiled=True)
    in_ids = lax.all_to_all(out_ids, "dp", split_axis=0, concat_axis=0, tiled=True)
    member = (jnp.arange(cluster_count, dtype=jnp.int32)[:, None] == in_ids[None, :]).astype(jnp.bfloat16)
    sums = jnp.dot(member, incoming, preferred_element_type=jnp.float32)
    counts = jnp.sum(member.astype(jnp.float32), axis=1)
    new_centroids = (cluster_mass[:, None] * centroids + sums) / (cluster_mass + counts)[:, None]
    half = slot_count // 2
    start = core * half
    contract = (((1,), (1,)), ((), ()))
    other = from_partner(incoming)
    scores = lax.dot_general(
        lax.dynamic_slice_in_dim(incoming, start, half, 0), incoming, contract, preferred_element_type=jnp.float32)
    scores = scores + lax.dot_general(
        lax.dynamic_slice_in_dim(other, start, half, 0), other, contract, preferred_element_type=jnp.float32)
    scores = scores / D
    query_ids = lax.dynamic_slice_in_dim(in_ids, start, half, 0)
    query_pos = start + jnp.arange(half, dtype=jnp.int32)
    same = (
        (query_ids[:, None] == in_ids[None, :])
        & (query_ids[:, None] >= 0)
        & (query_pos[:, None] != slot_index[None, :])
    )
    best = jnp.max(jnp.where(same, scores, -1.0), axis=1)
    best_p = from_partner(best)
    low, high = jnp.where(core == 0, best, best_p), jnp.where(core == 0, best_p, best)
    returned = lax.all_to_all(
        jnp.concatenate([low, high]), "dp", split_axis=0, concat_axis=0, tiled=True)
    return jnp.take(returned, slot), new_centroids


def shards(embeddings, cluster_id, centroids, cluster_mass):
    best, new_centroids, flag = compact(embeddings, cluster_id, centroids, cluster_mass)
    return lax.cond(
        flag[0, 0] > 0,
        lambda *args: general(*args),
        lambda *args: (best.reshape(ROWS), new_centroids),
        embeddings, cluster_id, centroids, cluster_mass,
    )


def solution(mesh):
    in_specs = (P("dp", "mp"), P("dp"), P("dp", "mp"), P("dp"))
    out_specs = (P("dp"), P("dp", "mp"))
    return jax.shard_map(shards, mesh=mesh, in_specs=in_specs, out_specs=out_specs, check_vma=False)
```

```python
import functools

import jax
import jax.numpy as jnp
from jax import lax
from jax.experimental import pallas as pl
from jax.experimental.pallas import tpu as pltpu
from jax.sharding import PartitionSpec as P

D = 1024
HALF = 512
ROWS = 768
CLUSTERS = 256
CAP = 12
ROOM = 128
NZ = 8
NXY = 16
GROUPS = (((1, 7), 0, 24), ((2, 6), 24, 24), ((None, 0), 48, 24))
LANE = {k: base + CAP * m for members, base, _ in GROUPS for m, k in enumerate(members) if k is not None}
OWN = 2
FAR = (3, 5, 4)
FAR_SETS = (((3, 5), 0, 24), ((4,), 2, 24))
WIDTH = tuple(count * NXY for _, _, count in GROUPS)
MESH = pl.DeviceIdType.MESH
NT = (((1,), (1,)), ((), ()))
NEAR = (1, 7, 2, 6)
AROUND = (10, 9, 11, 6, 14, 2, 8, 5, 7, 13, 15, 1, 3, 4, 12, 0)
POS = {k: i for i, k in enumerate(NEAR + FAR)}


def neg(d):
    return ((4 - d // 4) % 4) * 4 + (4 - d % 4) % 4


def hot(mask):
    return jnp.where(mask, 1.0, 0.0).astype(jnp.bfloat16)


def exchange_kernel(
    emb_ref, cid_ref, cent_ref, mass_ref,
    best_ref, nc_ref, flag_ref,
    emb, unit, sq_mine, sq_peer, zout, zin, z_far, z_far_p, mout, min_, xo0, xo1, idout, fo0, fo1, fi0, fi1, fi1_p, fid_out, fid_in,
    r0, r1, p0, p1, idin, ik0, ik1, ik2, ik_far, top, idq, acc0, acc1, acc2, acc_far, top_far, sums,
    tiles_i, column, best_out, far_out, ret1, ret2, far_z, back_out, far_ret, cent, cid_v, mass_v,
    local_sem, sq_sem, zs, zr, ms, mr, xs, xr, ids_s, ids_r, ps, pr, bs, br, fs, fr,
    ws, wr, vs, vr, us, ur, ts, tr,
):
    xout, rows, rows_p, idkey = (xo0, xo1), (r0, r1, fi1), (p0, p1, fi1_p), (ik0, ik1, ik2)
    fout, fin, acc = (fo0, fo1), (fi0, fi1), (acc0, acc1, acc2)
    me = lax.axis_index("dp")
    c = lax.axis_index("mp")
    z, x, y = me // 16, (me // 4) % 4, me % 4

    def at_z(k):
        return (((z + k) % NZ) * 16 + x * 4 + y, c)

    def at_xy(d):
        return (z * 16 + ((x + d // 4) % 4) * 4 + (y + d % 4) % 4, c)

    partner = (me, 1 - c)

    def send(src, dst, send_sem, recv_sem, to):
        copy = pltpu.make_async_remote_copy(src, dst, send_sem, recv_sem, device_id=to, device_id_type=MESH)
        copy.start()
        return copy

    def sent(ref, sem):
        pltpu.make_async_remote_copy(ref, ref, sem, sem, device_id=partner, device_id_type=MESH).wait_send()

    def arrived(ref, sem):
        pltpu.make_async_remote_copy(ref, ref, sem, sem, device_id=partner, device_id_type=MESH).wait_recv()

    others = pl.ds(1, NXY - 1)

    cid_load = pltpu.make_async_copy(cid_ref, cid_v, local_sem.at[3])
    cid_load.start()
    mass_load = pltpu.make_async_copy(mass_ref, mass_v, local_sem.at[4])
    mass_load.start()
    load = pltpu.make_async_copy(emb_ref, emb, local_sem.at[0])
    load.start()
    cent_load = pltpu.make_async_copy(cent_ref, cent, local_sem.at[1])
    cent_load.start()
    barrier = pltpu.get_barrier_semaphore()
    for k in FAR[::-1]:
        pl.semaphore_signal(barrier, inc=1, device_id=at_z(k), device_id_type=MESH)
        pl.semaphore_signal(barrier, inc=1, device_id=(at_z(k)[0], 1 - c), device_id_type=MESH)
    for d in AROUND[:-1]:
        pl.semaphore_signal(barrier, inc=1, device_id=at_xy(d), device_id_type=MESH)
        pl.semaphore_signal(barrier, inc=1, device_id=(at_xy(d)[0], 1 - c), device_id_type=MESH)
    for k in NEAR:
        pl.semaphore_signal(barrier, inc=1, device_id=at_z(k), device_id_type=MESH)
    pl.semaphore_signal(barrier, inc=1, device_id=partner, device_id_type=MESH)

    cid_load.wait()
    cid = cid_v[...].reshape(1, ROWS)
    owner = cid >> 8
    dz = ((owner >> 4) - z) & 7
    dxy = ((((owner >> 2) & 3) - x) & 3) * 4 + (((owner & 3) - y) & 3)
    target = dz * 16 + dxy
    lane128 = lax.broadcasted_iota(jnp.int32, (128, 128), 1)
    sub128 = lax.broadcasted_iota(jnp.int32, (128, 128), 0)
    upto = hot(sub128 <= lane128)
    sub8 = lax.broadcasted_iota(jnp.int32, (8, 128), 0)
    sub16 = lax.broadcasted_iota(jnp.int32, (NXY, 128), 0)
    last = lax.broadcasted_iota(jnp.int32, (1, 128), 1) == 127
    base_t = jnp.zeros((128, 128), jnp.float32)
    base_z = jnp.zeros((8, 128), jnp.float32)
    ranks, places = [], []
    for b in range(ROWS // 128):
        cut = slice(128 * b, 128 * b + 128)
        is_t = sub128 == target[:, cut]
        is_z = sub8 == dz[:, cut]
        run_t = base_t + jnp.dot(hot(is_t), upto, preferred_element_type=jnp.float32)
        run_z = base_z + jnp.dot(hot(is_z), upto, preferred_element_type=jnp.float32)
        ranks.append(jnp.sum(jnp.where(is_t, run_t, 0.0), axis=0, keepdims=True) - 1.0)
        places.append(jnp.sum(jnp.where(is_z, run_z, 0.0), axis=0, keepdims=True) - 1.0)
        base_t = jnp.broadcast_to(run_t[:, 127:128], (128, 128))
        base_z = jnp.broadcast_to(run_z[:, 127:128], (8, 128))
    near_most = jnp.where((sub8 == 1) | (sub8 == 2) | (sub8 > 5), base_z, 0.0)
    over = jnp.where(jnp.max(near_most, axis=0, keepdims=True) > float(ROOM), 1.0, 0.0)
    rank_f = jnp.concatenate(ranks, axis=1)
    rank = rank_f.astype(jnp.int32)
    place = jnp.concatenate(places, axis=1).astype(jnp.int32)
    slot = jnp.where(place < ROOM, dz * ROOM + place, -1)
    far_row = (dz >= 3) & (dz <= 5)
    far_lane = jnp.where(dz == 3, rank, jnp.where(dz == 5, rank + CAP, rank + 2 * CAP))
    far_lane = jnp.where(far_row, far_lane, jnp.where(dz == 0, rank + 3 * CAP, -1))
    far_slot = (
        jnp.where((dz == 3) | (dz == 5), dxy * FAR_SETS[0][2] + far_lane, -1),
        jnp.where((dz == 4) | (dz == 0), dxy * FAR_SETS[1][2] + far_lane - 2 * CAP, -1),
    )
    turned = ((4 - (dxy >> 2)) & 3) * 4 + ((4 - (dxy & 3)) & 3)
    tile_of = jnp.where(far_row, NZ * NXY + dxy, dz * NXY + turned)
    lane_of = jnp.where(far_row, far_lane, rank)
    for k in (0,) + NEAR:
        lane_of = jnp.where(dz == k, rank + LANE[(NZ - k) % NZ], lane_of)
    tiles_i[...] = jnp.zeros_like(tiles_i)
    for b in range(ROWS // 128):
        cut = slice(128 * b, 128 * b + 128)
        tiles_i[0, b:b + 1, :] = tile_of[:, cut]
        tiles_i[1, b:b + 1, :] = lane_of[:, cut]
    row8 = lax.broadcasted_iota(jnp.int32, (8, ROWS), 0)
    local = ((cid & 255) + 1).astype(jnp.float32)
    values = jnp.where(
        row8 == 0, local,
        jnp.where(row8 == 1, dxy.astype(jnp.float32), jnp.where(row8 == 2, rank_f, 0.0)),
    ).astype(jnp.bfloat16)

    load.wait()
    squares = jnp.zeros((ROWS, 128), jnp.float32)
    for f in range(HALF // 128):
        part = emb[:, 128 * f:128 * f + 128]
        squares = squares + part * part
    mine = jnp.sum(squares.T, axis=0, keepdims=True)
    sq_mine[...] = mine
    pl.semaphore_wait(barrier, NZ - 1 + 2 * (NXY - 1) + len(FAR) + 1)
    sq_copy = send(sq_mine, sq_peer, sq_sem.at[0], sq_sem.at[1], partner)

    place_hot = {}
    for k in NEAR:
        want = lax.broadcasted_iota(jnp.int32, (ROOM, ROWS), 0) + k * ROOM
        place_hot[k] = hot(want == slot)
    far_hot = [
        hot(lax.broadcasted_iota(jnp.int32, (NXY * count, ROWS), 0) == far_slot[e])
        for e, (_, _, count) in enumerate(FAR_SETS)
    ]

    sq_copy.wait()
    scale = lax.rsqrt((sq_mine[...] + sq_peer[...]) / D + 1e-06)
    scale = jnp.broadcast_to(scale, (128, ROWS)).T
    for f in range(HALF // 128):
        unit[:, 128 * f:128 * f + 128] = (emb[:, 128 * f:128 * f + 128] * scale).astype(jnp.bfloat16)

    def pack(k):
        packed = jnp.dot(place_hot[k], unit[...], preferred_element_type=jnp.float32).astype(jnp.bfloat16)
        zout[POS[k]] = packed
        send(zout.at[POS[k]], zin.at[POS[NZ - k]], zs.at[0], zr.at[0 if k in (1, 7) else 1], at_z(k))

    pack(1)
    pack(7)
    left = jnp.where(
        (far_row | (dz == 0)) & (lax.broadcasted_iota(jnp.int32, (NXY, ROWS), 0) == dxy), local, 0.0).astype(jnp.bfloat16)
    right = hot(lax.broadcasted_iota(jnp.int32, (128, ROWS), 0) == far_lane)
    ids = lax.dot_general(left, right, NT, preferred_element_type=jnp.float32)
    for d in AROUND:
        if d == 0:
            fid_in[0] = ids[0:1, :]
        else:
            fid_out[d] = ids[d:d + 1, :]
            send(fid_out.at[d], fid_in.at[neg(d)], vs.at[0], vr.at[0], at_xy(d))

    def pack_far(e):
        count = FAR_SETS[e][2]
        packed = jnp.dot(far_hot[e], unit[...], preferred_element_type=jnp.float32)
        for d in AROUND:
            block = packed[count * d:count * d + count, :].astype(jnp.bfloat16)
            if d == 0:
                fin[e][0] = block
            else:
                fout[e][d] = block
                send(fout[e].at[d], fin[e].at[neg(d)], ws.at[e], wr.at[e], at_xy(d))

    pack_far(0)
    for k in NEAR:
        meta = lax.dot_general(values, place_hot[k], NT, preferred_element_type=jnp.float32)
        mout[POS[k]] = meta
        send(mout.at[POS[k]], min_.at[POS[NZ - k]], ms.at[0], mr.at[0], at_z(k))
    pack(2)
    pack(6)

    p_copies = {}

    def forward(g):
        members, _, count = GROUPS[g]
        total = None
        for m, k in enumerate(members):
            meta = min_[POS[k]]
            valid = meta[0:1, :] > 0.5
            there = jnp.where(valid, meta[1:2, :] * float(count) + meta[2:3, :] + float(CAP * m), -1.0)
            there = there.astype(jnp.int32)
            want = lax.broadcasted_iota(jnp.int32, (NXY * count, ROOM), 0)
            if m == 0:
                arrived(zin.at[pl.ds(2 * g, 2)], zr.at[g])
            part = jnp.dot(hot(want == there), zin[POS[k]], preferred_element_type=jnp.float32)
            total = part if total is None else total + part
        for d in AROUND:
            block = total[count * d:count * d + count, :].astype(jnp.bfloat16)
            if d == 0:
                rows[g][0] = block
            else:
                xout[g][d] = block
                send(xout[g].at[d], rows[g].at[neg(d)], xs.at[g], xr.at[g], at_xy(d))

    def share(g):
        arrived(rows[g].at[others], xr.at[g])
        p_copies[g] = send(rows[g], rows_p[g], ps.at[g], pr.at[g], partner)

    def share_far(kk):
        arrived(z_far.at[kk], zr.at[2 + kk])
        p_copies[3 + kk] = send(z_far.at[kk], z_far_p.at[kk], ps.at[3 + kk], pr.at[3 + kk], partner)

    arrived(fid_in.at[others], vr.at[0])
    known = jnp.concatenate([fid_in[j] for j in range(NXY)], axis=0).astype(jnp.bfloat16)
    back_at = jnp.zeros((NXY, 128), jnp.float32)
    far_values, far_places = [], []
    for planes, first, count in FAR_SETS:
        width = NXY * count
        flat = lax.broadcasted_iota(jnp.int32, (1, width), 1)
        holder = (flat * 2731) >> 16
        within = flat - holder * count
        lane = jnp.where(within < CAP * len(planes), within + CAP * first, -1)
        spread = hot(lax.broadcasted_iota(jnp.int32, (128, width), 0) == lane)
        mine16 = lax.broadcasted_iota(jnp.int32, (NXY, width), 0) == holder
        far_ids = jnp.dot(known, spread, preferred_element_type=jnp.float32)
        far_ids = jnp.sum(jnp.where(mine16, far_ids, 0.0), axis=0, keepdims=True)
        low = lax.broadcasted_iota(jnp.int32, (8, width), 0) * CAP
        inside = (within >= low) & (within < low + CAP) & (low < CAP * len(planes)) & (far_ids > 0.5)
        base_f = jnp.zeros((8, 128), jnp.float32)
        runs = []
        for b in range(width // 128):
            run = base_f + jnp.dot(hot(inside[:, 128 * b:128 * b + 128]), upto, preferred_element_type=jnp.float32)
            runs.append(run)
            base_f = jnp.broadcast_to(run[:, 127:128], (8, 128))
        over = jnp.maximum(over, jnp.where(jnp.max(base_f, axis=0, keepdims=True) > float(ROOM), 1.0, 0.0))
        far_place = jnp.where(inside, jnp.concatenate(runs, axis=1) - 1.0, -1.0)
        far_place = jnp.where(far_place < float(ROOM), far_place, -1.0)
        any_place = jnp.maximum(jnp.max(far_place, axis=0, keepdims=True), 0.0)
        back_at = back_at + lax.dot_general(
            jnp.where(mine16, any_place, 0.0).astype(jnp.bfloat16), spread, NT, preferred_element_type=jnp.float32)
        far_values.append(jnp.broadcast_to(far_ids, (8, width)).astype(jnp.bfloat16))
        far_places.append(far_place)
    back_at = back_at.astype(jnp.int32)

    def relay_far(e):
        planes, _, count = FAR_SETS[e]
        width = NXY * count
        chosen = []
        for m, k in enumerate(planes):
            want = lax.broadcasted_iota(jnp.int32, (ROOM, width), 0).astype(jnp.float32)
            chosen.append(hot(want == far_places[e][m:m + 1, :]))
            mout[POS[k]] = lax.dot_general(far_values[e], chosen[m], NT, preferred_element_type=jnp.float32)
            there = FAR.index(NZ - k)
            send(mout.at[POS[k]], min_.at[POS[NZ - k]], ms.at[0], mr.at[1 + there], at_z(k))
        arrived(fin[e].at[others], wr.at[e])
        for m, k in enumerate(planes):
            zout[POS[k]] = jnp.dot(
                chosen[m], fin[e][...].reshape(width, HALF), preferred_element_type=jnp.float32).astype(jnp.bfloat16)
            there = FAR.index(NZ - k)
            send(zout.at[POS[k]], z_far.at[there], zs.at[0], zr.at[2 + there], at_z(k))

    pack_far(1)
    arrived(min_.at[pl.ds(0, 4)], mr.at[0])
    ids = jnp.zeros((NXY, 128), jnp.float32)
    for k in NEAR:
        meta = min_[POS[k]]
        valid = meta[0:1, :] > 0.5
        to = jnp.where(valid, meta[1:2, :], -1.0).astype(jnp.int32)
        place_k = meta[2:3, :].astype(jnp.int32) + LANE[k]
        left = jnp.where(sub16 == to, meta[0:1, :], 0.0).astype(jnp.bfloat16)
        ids = ids + lax.dot_general(left, hot(sub128 == place_k), NT, preferred_element_type=jnp.float32)
    for d in AROUND:
        if d == 0:
            idin[0] = ids[0:1, :]
        else:
            idout[d] = ids[d:d + 1, :]
            send(idout.at[d], idin.at[neg(d)], ids_s.at[0], ids_r.at[0], at_xy(d))

    forward(0)
    relay_far(0)

    forward(1)
    relay_far(1)

    p_copies[OWN] = send(rows[OWN], rows_p[OWN], ps.at[OWN], pr.at[OWN], partner)
    arrived(idin.at[others], ids_r.at[0])
    for j in range(NXY):
        line = idin[j]
        line = jnp.where(line < 0.5, -1.0, line)
        turned = jnp.broadcast_to(line, (128, 128)).T
        for g, (_, base, count) in enumerate(GROUPS[:OWN]):
            idkey[g][count * j:count * j + count, :] = turned[base:base + count, :]
        line = fid_in[j]
        line = jnp.where((line < 0.5) | (lane128[0:1, :] < 3 * CAP), -1.0, line)
        idkey[OWN][24 * j:24 * j + 24, :] = jnp.broadcast_to(line, (128, 128)).T[2 * CAP:4 * CAP, :]
    for g in range(3):
        half = WIDTH[g] // 2
        for h in range(-(-half // 128)):
            size = min(128, half - 128 * h)
            block = idkey[g][pl.ds(pl.multiple_of(half * c + 128 * h, 8), size), :]
            idq[g, :, 128 * h:128 * h + size] = block.T[0:8, :]
    for ref in (top, top_far, acc0, acc1, acc2, acc_far):
        ref[...] = jnp.full(ref.shape, -float(D), jnp.float32)
    sub256 = lax.broadcasted_iota(jnp.int32, (CLUSTERS, 128), 0).astype(jnp.float32) + 1.0

    def member_sums(source, key):
        seen = jnp.zeros((CLUSTERS, 128), jnp.float32)
        parts = []
        for h in range(key.shape[0] // 128):
            line = source[128 * h:128 * h + 128, :].T[0:1, :]
            member = jnp.where(sub256 == line, 1.0, 0.0)
            seen = seen + member
            parts.append(member.astype(jnp.bfloat16))
        member = jnp.concatenate(parts, axis=1) if len(parts) > 1 else parts[0]
        return seen, jnp.dot(member, key, preferred_element_type=jnp.float32)

    def near_sums(g):
        return member_sums(idkey[g], rows[g][...].reshape(WIDTH[g], HALF))

    def keys_of(g):
        return rows[g][...].reshape(WIDTH[g], HALF), rows_p[g][...].reshape(WIDTH[g], HALF)

    def own_half(g):
        half = WIDTH[g] // 2
        first = pl.ds(pl.multiple_of(NXY // 2 * c, 8), NXY // 2)
        return rows[g][first].reshape(half, HALF), rows_p[g][first].reshape(half, HALF)

    def nt(a, b):
        return lax.dot_general(a, b, NT, preferred_element_type=jnp.float32)

    def near_own(pairs):
        return [(pair, nt(keys_of(pair[0])[0], own_half(pair[1])[0])) for pair in pairs]

    def near_finish(parts):
        for (kg, qg), part in parts:
            nk, nq = WIDTH[kg], WIDTH[qg] // 2
            scores = part + nt(keys_of(kg)[1], own_half(qg)[1])
            for h in range(-(-nq // 128)):
                cut = slice(128 * h, min(128 * h + 128, nq))
                size = cut.stop - cut.start
                same = idkey[kg][...][:, :size] == idq[qg, 0:1, cut]
                if kg == qg:
                    apart = (lax.broadcasted_iota(jnp.int32, (nk, size), 0)
                             - lax.broadcasted_iota(jnp.int32, (nk, size), 1))
                    same = same & (apart != nq * c + 128 * h)
                kept = jnp.where(same, scores[:, cut], -float(D))
                top[qg, :, cut] = jnp.maximum(top[qg, :, cut], jnp.max(kept.reshape(nk // 8, 8, size), axis=0))

    half_far = pl.ds(pl.multiple_of(ROOM // 2 * c, ROOM // 2), ROOM // 2)

    def side(g):
        if g < 3:
            return own_half(g)
        return z_far[g - 3, half_far, :], z_far_p[g - 3, half_far, :]

    def far_own(groups, planes):
        columns = z_far[planes[0]:planes[0] + len(planes)].reshape(ROOM * len(planes), HALF)
        return [(g, nt(side(g)[0], columns)) for g in groups]

    def far_finish(parts, planes):
        first = planes[0]
        columns = z_far_p[first:first + len(planes)].reshape(ROOM * len(planes), HALF)
        for g, part in parts:
            scores = part + nt(side(g)[1], columns)
            n = scores.shape[0]
            if g < 3:
                mine = idkey[g][pl.ds(pl.multiple_of(n * c, 8), n), :]
            else:
                mine = ik_far[g - 3, half_far, :]
            for kk in planes:
                line = min_[POS[FAR[kk]]][0:1, :]
                same = mine == line
                if g == 3 + kk:
                    apart = (lax.broadcasted_iota(jnp.int32, (n, ROOM), 1)
                             - lax.broadcasted_iota(jnp.int32, (n, ROOM), 0))
                    same = same & (apart != n * c)
                kept = jnp.where(same, scores[:, ROOM * (kk - first):ROOM * (kk - first) + ROOM], -float(D))
                top_far[kk] = jnp.maximum(top_far[kk], jnp.max(kept.reshape(n // 8, 8, ROOM), axis=0))
                if g < 3:
                    acc[g][...] = jnp.maximum(acc[g][...], kept)
                elif g - 3 < first:
                    acc_far[g - 3] = jnp.maximum(acc_far[g - 3], kept)

    def take_far(kk):
        arrived(min_.at[POS[FAR[kk]]], mr.at[1 + kk])
        line = min_[POS[FAR[kk]]][0:1, :]
        ik_far[kk] = jnp.broadcast_to(jnp.where(line < 0.5, -1.0, line), (128, 128)).T
        share_far(kk)

    counts, total = near_sums(OWN)
    sums[...] = total
    parts = near_own([(2, 2)])
    p_copies[OWN].wait_recv()
    near_finish(parts)
    share(0)
    parts = near_own([(0, 0), (0, 2), (2, 0)])
    more, total = near_sums(0)
    counts = counts + more
    sums[...] += total
    p_copies[0].wait_recv()
    near_finish(parts)
    share(1)
    parts = near_own([(1, 1), (0, 1), (1, 0), (2, 1), (1, 2)])
    take_far(0)
    take_far(1)
    p_copies[1].wait_recv()
    near_finish(parts)
    parts = far_own([2, 0, 1, 3, 4], (0, 1))
    p_copies[3].wait_recv()
    p_copies[4].wait_recv()
    far_finish(parts, (0, 1))
    take_far(2)
    parts = far_own([2, 0, 1, 3, 4, 5], (2,))
    p_copies[5].wait_recv()
    far_finish(parts, (2,))
    for kk in range(3):
        best = jnp.max(top_far[kk], axis=0, keepdims=True)
        if kk < 2:
            mine = jnp.broadcast_to(jnp.max(acc_far[kk], axis=1, keepdims=True), (ROOM // 2, 128))
            mine = jnp.concatenate([jnp.where(c == h, mine, -float(D)) for h in range(2)], axis=0)
            best = jnp.maximum(best, mine.T[0:1, :])
        far_out[kk, :, 0:128] = best * (1.0 / D)
        far_out[kk, :, 128:256] = over
    for kk, k in enumerate(FAR):
        there = FAR.index(NZ - k)
        for core in range(2):
            send(far_out.at[kk], far_z.at[c, there], us.at[core], ur.at[0], (at_z(k)[0], core))
    for g, (_, base, count) in enumerate(GROUPS):
        half = WIDTH[g] // 2
        pieces = []
        for h in range(-(-half // 128)):
            size = min(128, half - 128 * h)
            best = jnp.max(top[g, :, 128 * h:128 * h + size], axis=0, keepdims=True)
            pieces.append(jnp.broadcast_to(best, (128, size)).T)
        best = jnp.concatenate(pieces, axis=0)
        best = jnp.maximum(best, jnp.max(acc[g][...], axis=1, keepdims=True)) * (1.0 / D)
        for i in range(NXY // 2):
            column[i, base:base + count, :] = best[count * i:count * i + count, :]
    for i in range(NXY // 2):
        best_out[i] = jnp.where(last, over, column[i].T[0:1, :])

    def best_copy(i, other):
        jx, jy = 2 * c + i // 4, i % 4
        there = (z * 16 + ((x + jx) % 4) * 4 + (y + jy) % 4, 1 - c if other else c)
        return pltpu.make_async_remote_copy(
            best_out.at[i], ret1.at[8 * c + i], bs.at[int(other)], br.at[0],
            device_id=there, device_id_type=MESH)

    @pl.when(c == 0)
    def _():
        ret1[0] = best_out[0]

    @pl.when(c == 1)
    def _():
        best_copy(0, False).start()

    best_copy(0, True).start()
    for i in range(1, 8):
        best_copy(i, False).start()
        best_copy(i, True).start()

    more, total = near_sums(1)
    counts = counts + more
    for kk in range(3):
        more, part = member_sums(ik_far[kk], z_far[kk])
        counts = counts + more
        total = total + part
    cent_load.wait()
    mass_load.wait()
    number = jnp.sum(counts, axis=1, keepdims=True)
    mass = jnp.broadcast_to(mass_v[...], (128, CLUSTERS)).T[:, 0:1]
    cent[...] = (mass * cent[...] + (sums[...] + total)) / (mass + number)
    nc_copy = pltpu.make_async_copy(cent, nc_ref, local_sem.at[2])
    nc_copy.start()

    arrived(far_z, ur.at[0])
    lane16 = lax.broadcasted_iota(jnp.int32, (NXY, 128), 1)
    got = jnp.zeros((NXY, 128), jnp.float32)
    for kk in range(3):
        line = jnp.maximum(far_z[0, kk][:, 0:128], far_z[1, kk][:, 0:128])
        line = jnp.broadcast_to(line, (8, 128))
        found = jnp.concatenate(
            [jnp.take_along_axis(line, back_at[8 * h:8 * h + 8, :], axis=1, mode="promise_in_bounds") for h in range(2)],
            axis=0)
        got = jnp.where(lane16 >= kk * CAP, found, got)
    far_over = far_z[0, 0][:, 128:256]
    for h in range(2):
        for kk in range(3):
            far_over = jnp.maximum(far_over, far_z[h, kk][:, 128:256])
    got = jnp.where(lane16 == 127, far_over, got)
    for j in AROUND:
        if j == 0:
            far_ret[0] = got[0:1, :]
        else:
            back_out[j] = got[j:j + 1, :]
            send(back_out.at[j], far_ret.at[neg(j)], ts.at[0], tr.at[0], at_xy(j))
    @pl.when(c == 0)
    def _():
        arrived(ret1.at[others], br.at[0])

    @pl.when(c == 1)
    def _():
        arrived(ret1, br.at[0])

    back = {}
    for k in (2, 6, 1, 7):
        back[NZ - k] = send(
            ret1, ret2.at[POS[NZ - k]], fs.at[POS[k]], fr.at[POS[NZ - k]], at_z(k))
    tile_t = tiles_i[0]
    lane_t = tiles_i[1]
    result = jnp.zeros((8, 128), jnp.float32)
    flag = jnp.zeros((1, 128), jnp.float32)

    def pick(line, tile, result, flag):
        got = jnp.take_along_axis(jnp.broadcast_to(line, (8, 128)), lane_t, axis=1, mode="promise_in_bounds")
        return jnp.where(tile_t == tile, got, result), jnp.maximum(flag, jnp.where(last, line, 0.0))

    for j in range(NXY):
        result, flag = pick(ret1[j], j, result, flag)
    for k in NEAR:
        back[k].wait_recv()
        for j in range(NXY):
            result, flag = pick(ret2[POS[k], j], k * NXY + j, result, flag)
    arrived(far_ret.at[others], tr.at[0])
    for d in range(NXY):
        result, flag = pick(far_ret[d], NZ * NXY + d, result, flag)
    for b in range(ROWS // 128):
        best_ref[:, 128 * b:128 * b + 128] = result[b:b + 1, :]
    flag_ref[0, 0] = jnp.max(flag).astype(jnp.int32)

    @pl.when(c == 0)
    def _():
        sent(best_out.at[pl.ds(1, 7)], bs.at[0])

    @pl.when(c == 1)
    def _():
        sent(best_out, bs.at[0])

    sent(best_out, bs.at[1])
    for copy in list(back.values()) + list(p_copies.values()):
        copy.wait_send()
    sent(zout, zs.at[0])
    sent(mout, ms.at[0])
    for e in range(2):
        sent(xout[e].at[others], xs.at[e])
        sent(fout[e].at[others], ws.at[e])
        sent(far_out, us.at[e])
    sent(fid_out.at[others], vs.at[0])
    sent(idout.at[others], ids_s.at[0])
    sent(back_out.at[others], ts.at[0])
    nc_copy.wait()


def compact(embeddings, cluster_id, centroids, cluster_mass):
    vmem = pl.BlockSpec(memory_space=pltpu.VMEM)
    anywhere = pl.BlockSpec(memory_space=pl.ANY)
    f32, bf16, i32 = jnp.float32, jnp.bfloat16, jnp.int32
    dma = pltpu.SemaphoreType.DMA
    line = (1, 128)
    return pl.pallas_call(
        exchange_kernel,
        out_shape=(
            jax.ShapeDtypeStruct((1, ROWS), f32),
            jax.ShapeDtypeStruct((CLUSTERS, HALF), f32),
            jax.ShapeDtypeStruct((1, 1), i32),
        ),
        in_specs=[anywhere, anywhere, anywhere, anywhere],
        out_specs=(vmem, anywhere, pl.BlockSpec(memory_space=pltpu.SMEM)),
        scratch_shapes=[
            pltpu.VMEM((ROWS, HALF), f32),
            pltpu.VMEM((ROWS, HALF), bf16),
            pltpu.VMEM((1, ROWS), f32),
            pltpu.VMEM((1, ROWS), f32),
            pltpu.VMEM((NZ - 1, ROOM, HALF), bf16),
            pltpu.VMEM((len(NEAR), ROOM, HALF), bf16),
            pltpu.VMEM((3, ROOM, HALF), bf16),
            pltpu.VMEM((3, ROOM, HALF), bf16),
            pltpu.VMEM((NZ - 1, 8, 128), f32),
            pltpu.VMEM((NZ - 1, 8, 128), f32),
            *[pltpu.VMEM((NXY, count, HALF), bf16) for _, _, count in GROUPS[:OWN]],
            pltpu.VMEM((NXY, *line), f32),
            *[pltpu.VMEM((NXY, far[2], HALF), bf16) for far in FAR_SETS],
            *[pltpu.VMEM((NXY, far[2], HALF), bf16) for far in FAR_SETS],
            pltpu.VMEM((NXY, FAR_SETS[1][2], HALF), bf16),
            pltpu.VMEM((NXY, *line), f32),
            pltpu.VMEM((NXY, *line), f32),
            *[pltpu.VMEM((NXY, count, HALF), bf16) for _, _, count in GROUPS[:OWN]],
            *[pltpu.VMEM((NXY, count, HALF), bf16) for _, _, count in GROUPS[:OWN]],
            pltpu.VMEM((NXY, *line), f32),
            *[pltpu.VMEM((NXY * count, 128), f32) for _, _, count in GROUPS],
            pltpu.VMEM((3, 128, 128), f32),
            pltpu.VMEM((3, 8, 256), f32),
            pltpu.VMEM((3, 8, 256), f32),
            *[pltpu.VMEM((width // 2, 128), f32) for width in WIDTH],
            pltpu.VMEM((2, ROOM // 2, 128), f32),
            pltpu.VMEM((3, 8, 128), f32),
            pltpu.VMEM((CLUSTERS, HALF), f32),
            pltpu.VMEM((2, 8, 128), i32),
            pltpu.VMEM((8, 128, 128), f32),
            pltpu.VMEM((8, *line), f32),
            pltpu.VMEM((3, 1, 256), f32),
            pltpu.VMEM((NXY, *line), f32),
            pltpu.VMEM((len(NEAR), NXY, *line), f32),
            pltpu.VMEM((2, 3, 1, 256), f32),
            pltpu.VMEM((NXY, *line), f32),
            pltpu.VMEM((NXY, *line), f32),
            pltpu.VMEM((CLUSTERS, HALF), f32),
            pltpu.VMEM((ROWS,), i32),
            pltpu.VMEM((1, CLUSTERS), f32),
            dma((5,)), dma((2,)), dma((1,)), dma((5,)), dma((1,)), dma((4,)), dma((2,)), dma((2,)),
            dma((1,)), dma((1,)), dma((6,)), dma((6,)), dma((2,)), dma((1,)), dma((4,)), dma((4,)),
            dma((2,)), dma((2,)), dma((1,)), dma((1,)), dma((2,)), dma((1,)), dma((1,)), dma((1,)),
        ],
        compiler_params=pltpu.CompilerParams(
            collective_id=0, has_side_effects=True, vmem_limit_bytes=48 * 2**20),
    )(embeddings, cluster_id, centroids, cluster_mass.reshape(1, CLUSTERS))


def from_partner(value):
    return lax.ppermute(value, "mp", [(0, 1), (1, 0)])


def general(embeddings, cluster_id, centroids, cluster_mass):
    owners = lax.axis_size("dp")
    row_count = embeddings.shape[0]
    slot_count = 2 * row_count
    capacity = slot_count // owners
    cluster_count = centroids.shape[0]
    core = lax.axis_index("mp")
    squares = jnp.sum(embeddings * embeddings, axis=1)
    squares = squares + from_partner(squares)
    unit = (embeddings * lax.rsqrt(squares / D + 1e-06)[:, None]).astype(jnp.bfloat16)
    owner = cluster_id // cluster_count
    local = cluster_id - owner * cluster_count
    owner_hot = (owner[:, None] == jnp.arange(owners, dtype=jnp.int32)[None, :]).astype(jnp.bfloat16)
    row_index = jnp.arange(row_count, dtype=jnp.int32)
    lower = (row_index[:, None] >= row_index[None, :]).astype(jnp.bfloat16)
    running = jnp.dot(lower, owner_hot, preferred_element_type=jnp.float32)
    rank = jnp.sum(running * owner_hot.astype(jnp.float32), axis=1).astype(jnp.int32) - 1
    slot = owner * capacity + rank
    slot_index = jnp.arange(slot_count, dtype=jnp.int32)
    placed = slot_index[:, None] == slot[None, :]
    outgoing = jnp.dot(
        placed.astype(jnp.bfloat16), unit, preferred_element_type=jnp.float32
    ).astype(jnp.bfloat16)
    out_ids = jnp.max(jnp.where(placed, local[None, :] + 1, 0), axis=1) - 1
    incoming = lax.all_to_all(outgoing, "dp", split_axis=0, concat_axis=0, tiled=True)
    in_ids = lax.all_to_all(out_ids, "dp", split_axis=0, concat_axis=0, tiled=True)
    member = (jnp.arange(cluster_count, dtype=jnp.int32)[:, None] == in_ids[None, :]).astype(jnp.bfloat16)
    sums = jnp.dot(member, incoming, preferred_element_type=jnp.float32)
    counts = jnp.sum(member.astype(jnp.float32), axis=1)
    new_centroids = (cluster_mass[:, None] * centroids + sums) / (cluster_mass + counts)[:, None]
    half = slot_count // 2
    start = core * half
    contract = (((1,), (1,)), ((), ()))
    other = from_partner(incoming)
    scores = lax.dot_general(
        lax.dynamic_slice_in_dim(incoming, start, half, 0), incoming, contract, preferred_element_type=jnp.float32)
    scores = scores + lax.dot_general(
        lax.dynamic_slice_in_dim(other, start, half, 0), other, contract, preferred_element_type=jnp.float32)
    scores = scores / D
    query_ids = lax.dynamic_slice_in_dim(in_ids, start, half, 0)
    query_pos = start + jnp.arange(half, dtype=jnp.int32)
    same = (
        (query_ids[:, None] == in_ids[None, :])
        & (query_ids[:, None] >= 0)
        & (query_pos[:, None] != slot_index[None, :])
    )
    best = jnp.max(jnp.where(same, scores, -1.0), axis=1)
    best_p = from_partner(best)
    low, high = jnp.where(core == 0, best, best_p), jnp.where(core == 0, best_p, best)
    returned = lax.all_to_all(
        jnp.concatenate([low, high]), "dp", split_axis=0, concat_axis=0, tiled=True)
    return jnp.take(returned, slot), new_centroids


def shards(embeddings, cluster_id, centroids, cluster_mass):
    best, new_centroids, flag = compact(embeddings, cluster_id, centroids, cluster_mass)
    return lax.cond(
        flag[0, 0] > 0,
        lambda *args: general(*args),
        lambda *args: (best.reshape(ROWS), new_centroids),
        embeddings, cluster_id, centroids, cluster_mass,
    )


def solution(mesh):
    in_specs = (P("dp", "mp"), P("dp"), P("dp", "mp"), P("dp"))
    out_specs = (P("dp"), P("dp", "mp"))
    return jax.shard_map(shards, mesh=mesh, in_specs=in_specs, out_specs=out_specs, check_vma=False)
```
